8 devices in a mesh: data: 2 (over z, y), dap: 4 (over x, core).
Axes of the slice: x: 2, y: 2, z: 1, core: 2. Of those that a mesh axis runs over, the one named last changes fastest.
Arguments:
- msa_act: bfloat16 [32, 128, 64], P(('data', 'dap')), parts along dimension 0
- pair_act: bfloat16 [256, 128, 128], P(('data', 'dap')), parts along dimension 0
- msa_mask: int32 [32, 128], P('data'), parts along dimension 0
- res_mask: int32 [256], P('data'), parts along dimension 0
- w_row_bias: bfloat16 [2, 128, 8], replicated
- w_row_in: bfloat16 [2, 64, 4, 8, 8], replicated
- w_row_out: bfloat16 [2, 8, 8, 64], replicated
- w_col_in: bfloat16 [2, 64, 4, 8, 8], replicated
- w_col_out: bfloat16 [2, 8, 8, 64], replicated
- w_opm_in: bfloat16 [2, 64, 2, 32], replicated
- w_opm_out: bfloat16 [2, 32, 32, 128], replicated
- w_ts_bias: bfloat16 [2, 128, 4], replicated
- w_ts_in: bfloat16 [2, 128, 4, 4, 32], replicated
- w_ts_out: bfloat16 [2, 4, 32, 128], replicated
- w_te_bias: bfloat16 [2, 128, 4], replicated
- w_te_in: bfloat16 [2, 128, 4, 4, 32], replicated
- w_te_out: bfloat16 [2, 4, 32, 128], replicated
Outputs:
- output 1: bfloat16 [32, 128, 64], P(('data', 'dap')), parts along dimension 0
- output 2: bfloat16 [256, 128, 128], P(('data', 'dap')), parts along dimension 0
There are 2 independent parts. The reference program is written for one: setup_inputs(seed, part) draws one part's arguments, and reference() takes and returns one part's arrays. A program takes and returns all parts, laid end to end along the dimension named above; an argument that names none is the same for every part.
All inputs are finite; a program needn't handle non-finite values.
Results may differ from the reference program's by a relative error of at most 0.01828.
Values are sent between devices in bfloat16 or wider.
A program may use at most 1 GiB of HBM per device.

```python
import jax
import jax.numpy as jnp
from jax import lax

NR = 128
NS = 16
C_M = 64
C_Z = 128
HEADS_MSA = 8
HEAD_MSA = 8
HEADS_TRI = 4
HEAD_TRI = 32
OPM_DIM = 32


def draw_normal(key, shape, scale):
    return (jax.random.normal(key, shape, jnp.float32) * scale).astype(jnp.bfloat16)


def setup_inputs(seed: int = 0, part: int = 0) -> dict:
    base_key = jax.random.key(seed)
    part_keys = jax.random.split(jax.random.fold_in(base_key, part), 4)
    w_keys = jax.random.split(jax.random.fold_in(base_key, 1000), 13)
    width_msa = HEADS_MSA * HEAD_MSA
    width_tri = HEADS_TRI * HEAD_TRI
    return {
        'msa_act': draw_normal(part_keys[0], (NS, NR, C_M), 1.0),
        'pair_act': draw_normal(part_keys[1], (NR, NR, C_Z), 1.0),
        'msa_mask': (jax.random.randint(part_keys[2], (NS, NR), 0, 4) > 0).astype(jnp.int32),
        'res_mask': (jax.random.randint(part_keys[3], (NR,), 0, 4) > 0).astype(jnp.int32),
        'w_row_bias': draw_normal(w_keys[0], (2, C_Z, HEADS_MSA), 1.5 * C_Z ** -0.5),
        'w_row_in': draw_normal(w_keys[1], (2, C_M, 4, HEADS_MSA, HEAD_MSA), 1.25 * C_M ** -0.5),
        'w_row_out': draw_normal(w_keys[2], (2, HEADS_MSA, HEAD_MSA, C_M), 0.5 * width_msa ** -0.5),
        'w_col_in': draw_normal(w_keys[3], (2, C_M, 4, HEADS_MSA, HEAD_MSA), 1.25 * C_M ** -0.5),
        'w_col_out': draw_normal(w_keys[4], (2, HEADS_MSA, HEAD_MSA, C_M), 0.5 * width_msa ** -0.5),
        'w_opm_in': draw_normal(w_keys[5], (2, C_M, 2, OPM_DIM), C_M ** -0.5),
        'w_opm_out': draw_normal(w_keys[6], (2, OPM_DIM, OPM_DIM, C_Z), 0.25 * NS ** 0.5 / OPM_DIM),
        'w_ts_bias': draw_normal(w_keys[7], (2, C_Z, HEADS_TRI), 1.5 * C_Z ** -0.5),
        'w_ts_in': draw_normal(w_keys[8], (2, C_Z, 4, HEADS_TRI, HEAD_TRI), 1.25 * C_Z ** -0.5),
        'w_ts_out': draw_normal(w_keys[9], (2, HEADS_TRI, HEAD_TRI, C_Z), 0.5 * width_tri ** -0.5),
        'w_te_bias': draw_normal(w_keys[10], (2, C_Z, HEADS_TRI), 1.5 * C_Z ** -0.5),
        'w_te_in': draw_normal(w_keys[11], (2, C_Z, 4, HEADS_TRI, HEAD_TRI), 1.25 * C_Z ** -0.5),
        'w_te_out': draw_normal(w_keys[12], (2, HEADS_TRI, HEAD_TRI, C_Z), 0.5 * width_tri ** -0.5),
    }


def layer_norm(values):
    flat = values.astype(jnp.float32)
    row_mean = jnp.mean(flat, axis=-1, keepdims=True)
    centered = flat - row_mean
    row_var = jnp.mean(centered * centered, axis=-1, keepdims=True)
    return (centered * lax.rsqrt(row_var + 1e-5)).astype(jnp.bfloat16)


def add_residual(current, update):
    return (current.astype(jnp.float32) + update).astype(jnp.bfloat16)


def pair_bias(pair_ln, w_bias):
    num_res = pair_ln.shape[0]
    flat = jnp.dot(pair_ln.reshape(num_res * num_res, -1), w_bias, preferred_element_type=jnp.float32)
    return jnp.transpose(flat.astype(jnp.bfloat16).reshape(num_res, num_res, -1), (2, 0, 1))


def attend_one(x_ln, w_in, w_out, bias_hqk, key_mask):
    length = x_ln.shape[0]
    heads = w_in.shape[2]
    head_dim = w_in.shape[3]
    projected = jnp.dot(x_ln, w_in.reshape(w_in.shape[0], -1), preferred_element_type=jnp.float32)
    projected = projected.astype(jnp.bfloat16).astype(jnp.float32).reshape(length, 4, heads, head_dim)
    logits = jnp.einsum('qhd,khd->hqk', projected[:, 0], projected[:, 1]) * head_dim ** -0.5
    if bias_hqk is not None:
        logits = logits + bias_hqk.astype(jnp.float32)
    logits = jnp.where(key_mask[None, None, :] > 0, logits, -1e9)
    attn_probs = jax.nn.softmax(logits, axis=-1).astype(jnp.bfloat16).astype(jnp.float32)
    attended = jnp.einsum('hqk,khd->qhd', attn_probs, projected[:, 2])
    gated = (attended * jax.nn.sigmoid(projected[:, 3])).astype(jnp.bfloat16)
    return jnp.dot(gated.reshape(length, heads * head_dim), w_out.reshape(heads * head_dim, -1), preferred_element_type=jnp.float32)


def row_attention(msa_act, bias_hqk, msa_mask, w_in, w_out):
    def one_seq(inputs):
        seq_act, seq_mask = inputs
        return add_residual(seq_act, attend_one(layer_norm(seq_act), w_in, w_out, bias_hqk, seq_mask))
    return lax.map(one_seq, (msa_act, msa_mask))


def column_attention(msa_act, msa_mask, w_in, w_out):
    def one_col(inputs):
        col_act, col_mask = inputs
        return add_residual(col_act, attend_one(layer_norm(col_act), w_in, w_out, None, col_mask))
    result = lax.map(one_col, (jnp.swapaxes(msa_act, 0, 1), msa_mask.T))
    return jnp.swapaxes(result, 0, 1)


def outer_mean(msa_act, pair_act, msa_mask, w_in, w_out):
    num_seq, num_res, width = msa_act.shape
    mask_f32 = msa_mask.astype(jnp.float32)
    projected = jnp.dot(layer_norm(msa_act).reshape(num_seq * num_res, width), w_in.reshape(width, -1), preferred_element_type=jnp.float32)
    projected = projected.reshape(num_seq, num_res, 2, -1) * mask_f32[:, :, None, None]
    projected = projected.astype(jnp.bfloat16).astype(jnp.float32)
    left = jnp.swapaxes(projected[:, :, 0], 0, 1)
    right = projected[:, :, 1]
    pair_norm = jnp.dot(mask_f32.T, mask_f32)
    w_flat = w_out.reshape(-1, w_out.shape[-1])
    def one_row(inputs):
        left_row, norm_row = inputs
        outer = jnp.einsum('sp,sjq->jpq', left_row, right).astype(jnp.bfloat16)
        update = jnp.dot(outer.reshape(num_res, -1), w_flat, preferred_element_type=jnp.float32)
        return update / (1e-3 + norm_row[:, None])
    return add_residual(pair_act, lax.map(one_row, (left, pair_norm)))


def triangle_start(pair_act, res_mask, w_bias, w_in, w_out):
    pair_ln = layer_norm(pair_act)
    bias_hqk = pair_bias(pair_ln, w_bias)
    def one_row(row_ln):
        return attend_one(row_ln, w_in, w_out, bias_hqk, res_mask)
    return add_residual(pair_act, lax.map(one_row, pair_ln))


def triangle_end(pair_act, res_mask, w_bias, w_in, w_out):
    flipped = triangle_start(jnp.swapaxes(pair_act, 0, 1), res_mask, w_bias, w_in, w_out)
    return jnp.swapaxes(flipped, 0, 1)


def reference(msa_act, pair_act, msa_mask, res_mask, w_row_bias, w_row_in, w_row_out, w_col_in, w_col_out, w_opm_in, w_opm_out, w_ts_bias, w_ts_in, w_ts_out, w_te_bias, w_te_in, w_te_out):
    bias_first = pair_bias(layer_norm(pair_act), w_row_bias[0])
    msa_act = row_attention(msa_act, bias_first, msa_mask, w_row_in[0], w_row_out[0])
    msa_act = column_attention(msa_act, msa_mask, w_col_in[0], w_col_out[0])
    pair_act = outer_mean(msa_act, pair_act, msa_mask, w_opm_in[0], w_opm_out[0])
    pair_act = triangle_start(pair_act, res_mask, w_ts_bias[0], w_ts_in[0], w_ts_out[0])
    pair_act = triangle_end(pair_act, res_mask, w_te_bias[0], w_te_in[0], w_te_out[0])
    bias_second = pair_bias(layer_norm(pair_act), w_row_bias[1])
    msa_act = column_attention(msa_act, msa_mask, w_col_in[1], w_col_out[1])
    pair_act = outer_mean(msa_act, pair_act, msa_mask, w_opm_in[1], w_opm_out[1])
    msa_act = row_attention(msa_act, bias_second, msa_mask, w_row_in[1], w_row_out[1])
    pair_act = triangle_end(pair_act, res_mask, w_te_bias[1], w_te_in[1], w_te_out[1])
    pair_act = triangle_start(pair_act, res_mask, w_ts_bias[1], w_ts_in[1], w_ts_out[1])
    return msa_act, pair_act
```

```python
import functools

import jax
import jax.numpy as jnp
from jax import lax
from jax.experimental import pallas as pl
from jax.experimental.pallas import tpu as pltpu
from jax.sharding import PartitionSpec as P

F32 = jnp.float32
BF16 = jnp.bfloat16
LOG2E = 1.4426950408889634
NEG = -1e9 * LOG2E
N_DAP = 4
L = 128
R = 32
S = 16
C = 64
H = 8
L2 = 2 * L
MESH = pl.DeviceIdType.MESH


def mm(lhs, rhs):
    return jnp.dot(lhs, rhs, preferred_element_type=F32)


def mm_nt(lhs, rhs):
    return lax.dot_general(lhs, rhs, (((1,), (1,)), ((), ())), preferred_element_type=F32)


def lanes(parts):
    return jnp.concatenate(parts, axis=1)


def subl(parts):
    return jnp.concatenate(parts, axis=0)


def lo(x):
    return x[:, :L]


def hi(x):
    return x[:, L:]


def part(x, k, size):
    return x[k * size:(k + 1) * size]


def cols(k, size=L):
    return slice(k * size, (k + 1) * size)


def rows_at(n, size):
    return pl.ds(pl.multiple_of(n * size, size), size)


def pair(ref, n):
    return lanes([ref[n], ref[n + 1]])


def put_pair(ref, n, value):
    ref[n] = lo(value)
    ref[n + 1] = hi(value)


def only(value, k, size, count):
    zero = jnp.zeros((size, value.shape[1]), value.dtype)
    return subl([value if j == k else zero for j in range(count)])


def eye_bf16(n):
    rows = lax.broadcasted_iota(jnp.int32, (n, n), 0)
    columns = lax.broadcasted_iota(jnp.int32, (n, n), 1)
    return jnp.where(rows == columns, 1.0, 0.0).astype(BF16)


def layer_norm_t(x):
    x = x.astype(F32)
    inv_n = 1.0 / x.shape[0]
    centered = x - jnp.sum(x, axis=0, keepdims=True) * inv_n
    var = jnp.sum(centered * centered, axis=0, keepdims=True) * inv_n
    return (centered * lax.rsqrt(var + 1e-5)).astype(BF16)


def sigmoid(x):
    return 0.5 * jnp.tanh(0.5 * x) + 0.5


def round_bf16(x):
    return x.astype(BF16).astype(F32)


def pipeline(stages, trips):
    depth = len(stages)

    def run(t, first, last):
        for k in reversed(range(first, last)):
            stages[k](t - k)

    for t in range(depth - 1):
        run(t, 0, t + 1)

    def step(t, carry):
        run(t, 0, depth)
        return carry
    lax.fori_loop(depth - 1, trips, step, 0)
    for t in range(depth - 1):
        run(trips + t, t + 1, depth)


def body(
    m_in, z_in, msk, rmsk, w_bias, w_row_in, w_row_out, w_col_in, w_col_out, w_opm_in, w_opm_out,
    w_ts_in, w_ts_out, w_te_in, w_te_out,
    m_out, z_out,
    z_t, ln_t, p_q, p_kt, p_v, p_sg, k_s, bsc_row, bsc_tri, rb, tb, bt_row, bt_tri, m_all, ln_m, cp, og, cmask, kcols,
    mq, mkt, mv, acs, r_all, x_loc, o_scr, u_opm, z_snd, z_rcv, z_f, nrm, tmp, wro_t, wci_p, wco_t, woo_t, wtri_t,
    x_s, m_s, w_s, g_s,
    g_send, g_recv, a_send, a_recv,
):
    me = lax.axis_index('dap')
    data = lax.axis_index('data')
    my_rows = rows_at(me, R)

    def peer(o):
        return (data, lax.rem(me + o, N_DAP))

    barrier = pltpu.get_barrier_semaphore()
    for o in range(1, N_DAP):
        pl.semaphore_signal(barrier, inc=1, device_id=peer(o), device_id_type=MESH)
    pl.semaphore_wait(barrier, N_DAP - 1)

    def gather(stage, ref):
        return [
            pltpu.make_async_remote_copy(
                src_ref=ref, dst_ref=ref, send_sem=g_send.at[stage, o - 1], recv_sem=g_recv.at[stage, o - 1],
                device_id=peer(o), device_id_type=MESH)
            for o in range(1, N_DAP)
        ]

    def start(copies):
        for c in copies:
            c.start()

    def wait(copies):
        for c in copies:
            c.wait()

    def z_copy(stage, o, first, count):
        dest = lax.rem(me + o, N_DAP)
        return pltpu.make_async_remote_copy(
            src_ref=z_snd.at[stage, pl.ds(first, count), rows_at(dest, R), :],
            dst_ref=z_rcv.at[stage, pl.ds(me * R + first, count), :, :],
            send_sem=a_send.at[stage, o - 1], recv_sem=a_recv.at[stage, o - 1],
            device_id=(data, dest), device_id_type=MESH)

    e_c = eye_bf16(C)
    e_l = eye_bf16(L)

    def every(first, count, stride):
        return tmp[pl.ds(first, count, stride=stride), :]

    for b in range(2):
        wro_t[b] = mm_nt(e_c, w_row_out[b]).astype(BF16)
        tmp[:4 * C, :C] = w_col_in[b].astype(F32)
        wci_p[b] = subl([every(f * C + d, H, H) for f in range(4) for d in range(H)])[:, :C].astype(BF16)
        tmp[:C, :C] = w_col_out[b].astype(F32)
        wco_t[b] = mm_nt(e_c, subl([every(d, H, H) for d in range(H)])[:, :C].astype(BF16)).astype(BF16)
        wtri_t[0, b] = mm_nt(e_l, w_ts_out[b]).astype(BF16)
        wtri_t[1, b] = mm_nt(e_l, w_te_out[b]).astype(BF16)
    tmp[...] = w_opm_out[0].astype(F32)
    woo_t[0] = mm_nt(e_l, subl([every(q, R, R) for q in range(R)]).astype(BF16)).astype(BF16)
    woo_t[1] = mm_nt(e_l, w_opm_out[1]).astype(BF16)

    def down(row):
        return jnp.transpose(jnp.broadcast_to(row, (L, L)))

    mask_f = msk[...].astype(F32)
    for s in range(S):
        cmask[s] = jnp.broadcast_to(mask_f[s:s + 1, :], (H, L))
    mask_t = jnp.transpose(subl([mask_f] * H)).astype(BF16)[:, :S]
    nrm[...] = 1.0 / (1e-3 + mm(mask_t, mask_f.astype(BF16)))
    key_row = rmsk[...].astype(F32)
    key_col = down(key_row)
    key_row2 = lanes([key_row, key_row])
    for s in range(4):
        kcols[s] = down(msk[pl.ds(4 * me + s, 1), :].astype(F32))

    def bias_rows(bsc, ln_ref, b, group):
        def stage(t):
            n = t * 2
            rows = part(mm(w_bias[b], pair(ln_ref, n)), group, H)
            bsc[rows_at(n, H), :] = lo(rows)
            bsc[rows_at(n + 1, H), :] = hi(rows)
        return stage

    def pack_bias(bsc, ref, first, heads):
        for h in range(heads):
            ref[h, my_rows, :] = bsc[pl.ds(first + h, R, stride=H), :].astype(BF16)

    def normalise(t):
        for n in (t * 2, t * 2 + 1):
            ln_t[n] = layer_norm_t(z_t[n])

    def make_tri_bias(ref):
        for h in range(4):
            t = jnp.transpose(ref[h].astype(F32)) * LOG2E
            bt_tri[:, cols(h)] = jnp.where(key_col > 0, t, NEG)

    def tri_project(w_in_ref):
        def project(t):
            n = t * 2
            ln2 = pair(ln_t, n)
            put_pair(p_q, n, mm(part(w_in_ref, 0, L), ln2).astype(BF16))
            k_s[...] = round_bf16(mm(part(w_in_ref, 1, L), ln2)) * key_row2
            put_pair(p_v, n, mm(part(w_in_ref, 2, L), ln2).astype(BF16))
            put_pair(p_sg, n, round_bf16(mm(part(w_in_ref, 3, L), ln2)))

        def turn(t):
            for r in range(2):
                p_kt[t * 2 + r] = jnp.transpose(k_s[:, cols(r)]).astype(BF16)
                p_sg[t * 2 + r] = sigmoid(p_sg[t * 2 + r])

        pipeline([project, turn], R // 2)

    def weigh(t):
        for k in range(4):
            for half in (cols(0), cols(1)):
                e = jnp.exp2(x_s[k, :, half] - m_s[k, :, half])
                w_s[k, :, half] = (e * (1.0 / jnp.sum(e, axis=0, keepdims=True))).astype(BF16)

    def put_score(k, x):
        x_s[k] = x
        m_s[k] = jnp.max(x, axis=0, keepdims=True)

    def tri_attend(w_out_t, finish):
        scale = R ** -0.5 * LOG2E

        def score(t):
            for r in range(2):
                q = p_q[t * 2 + r]
                kt = p_kt[t * 2 + r]
                for hp in range(2):
                    blocks = [only(part(q, h, R), h, R, 4) for h in (2 * hp, 2 * hp + 1)]
                    put_score(2 * r + hp, mm(kt, lanes(blocks)) * scale + bt_tri[:, cols(hp, L2)])

        def gather_values(t):
            for r in range(2):
                v = p_v[t * 2 + r]
                outs = []
                for hp in range(2):
                    o2 = mm(part(v, hp, C), w_s[2 * r + hp])
                    outs += [lo(part(o2, 0, R)), hi(part(o2, 1, R))]
                g_s[:, cols(r)] = (subl(outs) * p_sg[t * 2 + r]).astype(BF16)

        def project_out(t):
            finish[0](t, pair(z_t, t * 2).astype(F32) + mm(w_out_t[...], g_s[...]))

        pipeline([score, weigh, gather_values, project_out] + finish[1:], R // 2)

    def row_attention(b, load, store):
        scale = H ** -0.5 * LOG2E
        for t in range(4):
            proj = round_bf16(mm(w_row_in[b], layer_norm_t(load(t))))
            q, k, v, g = [part(proj, f, C) for f in range(4)]
            mq[t] = q
            mkt[t] = jnp.transpose(subl([k, k]))[:, :C].astype(BF16)
            mv[t] = v.astype(BF16)
            p_sg[t, :C] = sigmoid(g)

        def score(t):
            kt = mkt[t]
            kcol = kcols[t]
            kcol2 = lanes([kcol, kcol])
            for hp in range(4):
                blocks = [only(mq[t, cols(h, H)], h, H, H) for h in (2 * hp, 2 * hp + 1)]
                x = mm(kt, lanes(blocks).astype(BF16)) * scale + bt_row[:, cols(hp, L2)]
                put_score(hp, jnp.where(kcol2 > 0, x, NEG))

        def gather_values(t):
            outs = []
            for hp in range(4):
                o2 = mm(mv[t, cols(hp, S)], w_s[hp])
                outs += [lo(part(o2, 0, H)), hi(part(o2, 1, H))]
            g_s[:C, :L] = (subl(outs) * p_sg[t, :C]).astype(BF16)

        def project_out(t):
            store(t, (load(t).astype(F32) + mm(wro_t[b], g_s[:C, :L])).astype(BF16))

        pipeline([score, weigh, gather_values, project_out], 4)

    def col_attention(b):
        scale = H ** -0.5 * LOG2E

        def normalise_m(t):
            for s in (2 * t, 2 * t + 1):
                ln_m[s] = layer_norm_t(m_all[s])

        def project(t):
            proj = round_bf16(mm(wci_p[b], pair(ln_m, 2 * t)))
            put_pair(cp, 2 * t, subl([proj[:3 * C], sigmoid(part(proj, 3, C))]))
        pipeline([normalise_m, project], S // 2)

        def attend(a, carry):
            def at(s, f, d):
                return cp[s, cols(f * H + d, H)]

            q = [at(a, 0, d) for d in range(H)]
            logits = []
            for t in range(S):
                acc = functools.reduce(jnp.add, [q[d] * at(t, 1, d) for d in range(H)])
                logits.append(jnp.where(cmask[t] > 0, acc * scale, NEG))
            top = functools.reduce(jnp.maximum, logits)
            e = [jnp.exp2(x - top) for x in logits]
            inv = 1.0 / functools.reduce(jnp.add, e)
            probs = [round_bf16(x * inv) for x in e]
            outs = [functools.reduce(jnp.add, [probs[t] * at(t, 2, d) for t in range(S)]) for d in range(H)]
            og[a] = (subl(outs) * cp[a, cols(3, C)]).astype(BF16)
            return carry
        lax.fori_loop(0, S, attend, 0)

        def update(t):
            new = pair(m_all, 2 * t).astype(F32) + mm(wco_t[b], pair(og, 2 * t))
            put_pair(m_all, 2 * t, new.astype(BF16))

        def halves(t):
            both = mm(w_opm_in[b], pair(ln_m, 2 * t))
            for s, x in ((2 * t, lo(both)), (2 * t + 1, hi(both))):
                acs[rows_at(s, C), :] = x * msk[pl.ds(s, 1), :].astype(F32)
        pipeline([update, normalise_m, halves], S // 2)

    row_id = lax.broadcasted_iota(jnp.int32, (S, L2), 0)
    lane_id = lax.broadcasted_iota(jnp.int32, (S, L2), 1)
    diag = row_id == lane_id // S

    def opm(b, finish):
        local, other = (0, R) if b == 0 else (R, 0)
        for q in range(R):
            r_all[q] = acs[pl.ds(other + q, S, stride=C), :].astype(BF16)
        for t in range(4):
            rows = subl([acs[pl.ds(local + H * t + p, S, stride=C), :] for p in range(H)])
            x_loc[:, cols(t)] = jnp.transpose(round_bf16(rows))

        def outer(t):
            left = []
            for k in range(4):
                row = x_loc[pl.ds(me * R + t * 4 + k, 1), :]
                for half in (cols(0, L2), cols(1, L2)):
                    left.append(jnp.where(diag, jnp.broadcast_to(row[:, half], (S, L2)), 0.0))
            left = subl(left).astype(BF16)
            for q in range(0, R, 2):
                put_pair(o_scr, q, mm(left, lanes([subl([r_all[q]] * S), subl([r_all[q + 1]] * S)])).astype(BF16))

        def contract(t):
            for k in range(2):
                blocks = [o_scr[:, cols(2 * k + j, R), :].reshape(R * R, L) for j in range(2)]
                n = t * 4 + 2 * k
                at = me * R + n
                norm = lanes([nrm[pl.ds(at, 1), :], nrm[pl.ds(at + 1, 1), :]])
                finish[0](n, mm(woo_t[b], lanes(blocks)) * norm)

        pipeline([outer, contract] + [
            lambda t, f=f: (f(2 * t), f(2 * t + 1)) for f in finish[1:]], R // 4)

    def put_z(t, z2):
        put_pair(z_t, 2 * t, z2.astype(BF16))

    def send_z(stage):
        def turn(t, z2):
            z2 = round_bf16(z2)
            for r, x in ((0, lo(z2)), (1, hi(z2))):
                z_snd[stage, 2 * t + r] = jnp.transpose(x).astype(BF16)

        def send(t):
            for o in range(1, N_DAP):
                z_copy(stage, o, 2 * t, 2).start()
            for n in (2 * t, 2 * t + 1):
                z_rcv[stage, me * R + n] = z_snd[stage, n, my_rows, :]
        return [turn, send]

    def receive_z(stage, b):
        for o in range(1, N_DAP):
            z_copy(stage, o, 0, R).wait()

        def widen(t):
            for r in range(4):
                n = t * 4 + r
                z_f[pl.ds(pl.multiple_of(n * (R + H), H), R), :] = z_rcv[stage, n].astype(F32)
        pipeline([widen], R)

        def turn(t):
            for n in (2 * t, 2 * t + 1):
                z_t[n] = jnp.transpose(z_f[pl.ds(n, L, stride=R + H), :]).astype(BF16)
        pipeline([turn, normalise, bias_rows(bsc_tri, ln_t, b, 1)], R // 2)

    def enter(t):
        for n in (2 * t, 2 * t + 1):
            z_t[n] = jnp.transpose(z_in[n].astype(F32)).astype(BF16)
    pipeline([enter, normalise, bias_rows(bsc_row, ln_t, 0, 0)], R // 2)
    pack_bias(bsc_row, rb.at[0], 0, H)
    g = gather(0, rb.at[0, :, my_rows, :])
    start(g)
    wait(g)
    for h in range(H):
        bt_row[:, cols(h)] = jnp.transpose(rb[0, h].astype(F32)) * LOG2E

    def store_m(s, value):
        m_all[4 * me + s] = value
    row_attention(0, lambda s: m_in[s], store_m)
    g = gather(1, m_all.at[pl.ds(4 * me, 4)])
    start(g)
    wait(g)
    col_attention(0)

    def add_first(n, update2):
        put_pair(z_t, n, (pair(z_t, n).astype(F32) + update2).astype(BF16))
    opm(0, [add_first, normalise, bias_rows(bsc_tri, ln_t, 0, 1)])
    pack_bias(bsc_tri, tb.at[0], 0, 4)
    g = gather(2, tb.at[0, :, my_rows, :])
    start(g)
    tri_project(w_ts_in.at[0])
    wait(g)
    make_tri_bias(tb.at[0])
    tri_attend(wtri_t.at[0, 0], send_z(0))

    col_attention(1)

    def keep_update(n, update2):
        put_pair(u_opm, n, update2)
    opm(1, [keep_update])

    receive_z(0, 0)
    pack_bias(bsc_tri, tb.at[1], 4, 4)
    g = gather(3, tb.at[1, :, my_rows, :])
    start(g)
    tri_project(w_te_in.at[0])
    wait(g)
    make_tri_bias(tb.at[1])
    tri_attend(wtri_t.at[1, 0], [put_z, normalise, bias_rows(bsc_row, ln_t, 1, 0)])

    pack_bias(bsc_row, rb.at[1], 0, H)
    g_row = gather(4, rb.at[1, :, my_rows, :])
    start(g_row)

    def add_second(t):
        put_z(t, pair(z_t, 2 * t).astype(F32) + pair(u_opm, 2 * t))
    pipeline([add_second, normalise, bias_rows(bsc_tri, ln_t, 1, 1)], R // 2)
    pack_bias(bsc_tri, tb.at[2], 4, 4)
    g = gather(5, tb.at[2, :, my_rows, :])
    start(g)
    tri_project(w_te_in.at[1])
    wait(g)
    make_tri_bias(tb.at[2])
    tri_attend(wtri_t.at[1, 1], send_z(1))

    wait(g_row)
    for h in range(H):
        bt_row[:, cols(h)] = rb[1, h].astype(F32) * LOG2E

    def emit_m(s, value):
        m_out[s] = value
    row_attention(1, lambda s: m_all[4 * me + s], emit_m)

    receive_z(1, 1)
    pack_bias(bsc_tri, tb.at[3], 0, 4)
    g = gather(6, tb.at[3, :, my_rows, :])
    start(g)
    tri_project(w_ts_in.at[1])
    wait(g)
    make_tri_bias(tb.at[3])

    def emit_z(t, z2):
        for n, x in ((2 * t, lo(z2)), (2 * t + 1, hi(z2))):
            z_out[n] = jnp.transpose(x).astype(BF16)
    tri_attend(wtri_t.at[0, 1], [emit_z])


def solution(mesh):
    def local_step(msa_act, pair_act, msa_mask, res_mask, w_row_bias, w_row_in, w_row_out, w_col_in, w_col_out, w_opm_in, w_opm_out, w_ts_bias, w_ts_in, w_ts_out, w_te_bias, w_te_in, w_te_out):
        def rows_first(w):
            w = jnp.moveaxis(w, 1, -1)
            return w.reshape(2, -1, w.shape[-1])

        def flat_out(w):
            return w.reshape(2, -1, w.shape[-1])

        w_bias = jnp.concatenate([jnp.swapaxes(w, 1, 2) for w in (w_row_bias, w_ts_bias, w_te_bias)], axis=1)
        vmem = pl.BlockSpec(memory_space=pltpu.VMEM)

        def wide(*shape):
            return pltpu.VMEM(shape, F32)

        def half(*shape):
            return pltpu.VMEM(shape, BF16)

        scratch = dict(
            z_t=half(R, L, L), ln_t=half(R, L, L), p_q=half(R, L, L), p_kt=half(R, L, L), p_v=half(R, L, L),
            p_sg=wide(R, L, L), k_s=wide(L, L2), bsc_row=wide(R * H, L), bsc_tri=wide(R * H, L),
            rb=half(2, H, L, L), tb=half(4, 4, L, L), bt_row=wide(L, H * L), bt_tri=wide(L, 4 * L),
            m_all=half(S, C, L), ln_m=half(S, C, L), cp=wide(S, 4 * C, L), og=half(S, C, L),
            cmask=wide(S, H, L), kcols=wide(4, L, L), mq=wide(4, C, L), mkt=half(4, L, C), mv=half(4, C, L),
            acs=wide(S * C, L), r_all=half(R, S, L), x_loc=wide(L, R * S),
            o_scr=half(R, L, L), u_opm=wide(R, L, L), z_snd=half(2, R, L, L), z_rcv=half(2, L, R, L),
            z_f=wide(L * (R + H), L), nrm=wide(L, L), tmp=wide(R * R, L),
            wro_t=half(2, C, C), wci_p=half(2, 4 * C, C), wco_t=half(2, C, C), woo_t=half(2, L, R * R),
            wtri_t=half(2, 2, L, L), x_s=wide(4, L, L2), m_s=wide(4, 1, L2), w_s=half(4, L, L2), g_s=half(L, L2),
        )
        sems = [pltpu.SemaphoreType.DMA((n, N_DAP - 1)) for n in (7, 7, 2, 2)]
        m_new, z_new = pl.pallas_call(
            body,
            out_shape=(jax.ShapeDtypeStruct((4, C, L), BF16), jax.ShapeDtypeStruct((R, L, L), BF16)),
            in_specs=[vmem] * 15,
            out_specs=(vmem, vmem),
            scratch_shapes=list(scratch.values()) + sems,
            compiler_params=pltpu.CompilerParams(collective_id=0, has_side_effects=True, vmem_limit_bytes=60 * 2 ** 20),
        )(
            jnp.swapaxes(msa_act, 1, 2), pair_act, msa_mask, res_mask.reshape(1, L), w_bias,
            rows_first(w_row_in), flat_out(w_row_out), rows_first(w_col_in), flat_out(w_col_out),
            rows_first(w_opm_in), flat_out(w_opm_out),
            rows_first(w_ts_in), flat_out(w_ts_out), rows_first(w_te_in), flat_out(w_te_out),
        )
        return jnp.swapaxes(m_new, 1, 2), z_new

    in_specs = (P(('data', 'dap')), P(('data', 'dap')), P('data'), P('data')) + (P(),) * 13
    out_specs = (P(('data', 'dap')), P(('data', 'dap')))
    return jax.shard_map(local_step, mesh=mesh, in_specs=in_specs, out_specs=out_specs, check_vma=False)
```

```python
import functools

import jax
import jax.numpy as jnp
from jax import lax
from jax.experimental import pallas as pl
from jax.experimental.pallas import tpu as pltpu
from jax.sharding import PartitionSpec as P

F32 = jnp.float32
BF16 = jnp.bfloat16
LOG2E = 1.4426950408889634
NEG = -1e9 * LOG2E
N_DAP = 4
N_IN = 15
L = 128
R = 32
S = 16
C = 64
H = 8
L2 = 2 * L
MESH = pl.DeviceIdType.MESH


def mm(lhs, rhs):
    return jnp.dot(lhs, rhs, preferred_element_type=F32)


def mm_nt(lhs, rhs):
    return lax.dot_general(lhs, rhs, (((1,), (1,)), ((), ())), preferred_element_type=F32)


def lanes(parts):
    return jnp.concatenate(parts, axis=1)


def subl(parts):
    return jnp.concatenate(parts, axis=0)


def lo(x):
    return x[:, :L]


def hi(x):
    return x[:, L:]


def part(x, k, size):
    return x[k * size:(k + 1) * size]


def cols(k, size=L):
    return slice(k * size, (k + 1) * size)


def rows_at(n, size):
    return pl.ds(pl.multiple_of(n * size, size), size)


def pair(ref, n):
    return lanes([ref[n], ref[n + 1]])


def put_pair(ref, n, value):
    ref[n] = lo(value)
    ref[n + 1] = hi(value)


def only(value, k, size, count):
    zero = jnp.zeros((size, value.shape[1]), value.dtype)
    return subl([value if j == k else zero for j in range(count)])


def eye_bf16(n):
    rows = lax.broadcasted_iota(jnp.int32, (n, n), 0)
    columns = lax.broadcasted_iota(jnp.int32, (n, n), 1)
    return jnp.where(rows == columns, 1.0, 0.0).astype(BF16)


def layer_norm_t(x):
    x = x.astype(F32)
    inv_n = 1.0 / x.shape[0]
    centered = x - jnp.sum(x, axis=0, keepdims=True) * inv_n
    var = jnp.sum(centered * centered, axis=0, keepdims=True) * inv_n
    return (centered * lax.rsqrt(var + 1e-5)).astype(BF16)


def sigmoid(x):
    return 0.5 * jnp.tanh(0.5 * x) + 0.5


def round_bf16(x):
    return x.astype(BF16).astype(F32)


def pipeline(stages, trips, pause=None, resume=None):
    depth = len(stages)

    def run(t, first, last):
        for k in reversed(range(first, last)):
            stages[k](t - k)

    def step(t, carry):
        run(t, 0, depth)
        return carry

    for t in range(depth - 1):
        run(t, 0, t + 1)
    if pause is not None:
        lax.fori_loop(depth - 1, pause, step, 0)
        resume()
    lax.fori_loop(depth - 1 if pause is None else pause, trips, step, 0)
    for t in range(depth - 1):
        run(trips + t, t + 1, depth)


def body(
    m_hbm, *refs,
):
    n = N_IN - 1
    given, (m_out, z_out), refs = refs[:n], refs[n:n + 2], refs[n + 2:]
    held, in_sems, refs = refs[:n], refs[n], refs[n + 1:]
    main(m_hbm, given, held, in_sems, m_out, z_out, *refs)


def main(
    m_hbm, given, held, in_sems, m_out, z_out,
    z_t, ln_t, p_q, p_kt, p_v, p_sg, k_s, bsc_row, bsc_tri, rb, tb, bt_row, bt_tri, m_all, m_dev, m_own, ln_m, cq, ckv, og,
    cmask, omask, kcols, mq, mkt, mv, pick, spread, join, acs, r_all, x_loc, o_scr, u_opm, z_snd, z_rcv, z_f, nrm, tmp, wro_t, wci_p, wco_t, woo_t, wtri_t,
    x_s, m_s, w_s, g_s,
    g_send, g_recv, a_send, a_recv,
):
    me = lax.axis_index('dap')
    data = lax.axis_index('data')
    my_rows = rows_at(me, R)

    def peer(o):
        return (data, lax.rem(me + o, N_DAP))

    z_in, msk, rmsk, w_bias, w_row_in, w_row_out, w_col_in, w_col_out, w_opm_in, w_opm_out = held[:10]
    w_ts_in, w_ts_out, w_te_in, w_te_out = held[10:]
    own_m = m_all.at[pl.ds(4 * me, 4)]
    copy_m = pltpu.make_async_copy(m_hbm, own_m, in_sems.at[N_IN - 1])
    copy_m.start()
    copies_in = [pltpu.make_async_copy(src, dst, in_sems.at[k]) for k, (src, dst) in enumerate(zip(given, held))]
    for c in copies_in:
        c.start()

    barrier = pltpu.get_barrier_semaphore()
    for o in range(1, N_DAP):
        pl.semaphore_signal(barrier, inc=1, device_id=peer(o), device_id_type=MESH)
    pl.semaphore_wait(barrier, N_DAP - 1)

    def gather(stage, ref):
        return [
            pltpu.make_async_remote_copy(
                src_ref=ref, dst_ref=ref, send_sem=g_send.at[stage, o - 1], recv_sem=g_recv.at[stage, o - 1],
                device_id=peer(o), device_id_type=MESH)
            for o in range(1, N_DAP)
        ]

    def start(copies):
        for c in copies:
            c.start()

    def wait(copies):
        for c in copies:
            c.wait()

    def z_copy(stage, o, first, count, at=0, size=R):
        dest = lax.rem(me + o, N_DAP)
        return pltpu.make_async_remote_copy(
            src_ref=z_snd.at[min(stage, 1), pl.ds(first, count), pl.ds(pl.multiple_of(dest * R + at, S), size), :],
            dst_ref=z_rcv.at[min(stage, 1), pl.ds(me * R + first, count), pl.ds(at, size), :],
            send_sem=a_send.at[stage, o - 1], recv_sem=a_recv.at[stage, o - 1],
            device_id=(data, dest), device_id_type=MESH)

    copy_m.wait()
    g_in = gather(0, own_m)
    start(g_in)
    for c in copies_in:
        c.wait()

    e_c = eye_bf16(C)
    e_l = eye_bf16(L)

    def every(first, count, stride):
        return tmp[pl.ds(first, count, stride=stride), :]

    for b in range(2):
        wro_t[b] = mm_nt(e_c, w_row_out[b]).astype(BF16)
        tmp[:4 * C, :C] = w_col_in[b].astype(F32)
        wci_p[b] = subl([every(f * C + d, H, H) for f in range(4) for d in range(H)])[:, :C].astype(BF16)
        tmp[:C, :C] = w_col_out[b].astype(F32)
        wco_t[b] = mm_nt(e_c, subl([every(d, H, H) for d in range(H)])[:, :C].astype(BF16)).astype(BF16)

    def late_weights():
        for b in range(2):
            wtri_t[0, b] = mm_nt(e_l, w_ts_out[b]).astype(BF16)
            wtri_t[1, b] = mm_nt(e_l, w_te_out[b]).astype(BF16)
        tmp[...] = w_opm_out[0].astype(F32)
        woo_t[0] = mm_nt(e_l, subl([every(q, R, R) for q in range(R)]).astype(BF16)).astype(BF16)
        woo_t[1] = mm_nt(e_l, w_opm_out[1]).astype(BF16)
        src, lane = iota((4 * L, 4 * L), 0), iota((4 * L, 4 * L), 1)
        join[...] = ones_at((src // L == lane % L // R) & (src % L == lane // L * R + lane % R))

    def down(row):
        return jnp.transpose(jnp.broadcast_to(row, (L, L)))

    mask_f = msk[...].astype(F32)
    for s in range(S):
        cmask[s] = jnp.broadcast_to(mask_f[s:s + 1, :], (H, L))
    mask_t = jnp.transpose(subl([mask_f] * H)).astype(BF16)[:, :S]
    nrm[...] = 1.0 / (1e-3 + mm(mask_t, mask_f.astype(BF16)))
    key_row = rmsk[...].astype(F32)
    key_col = down(key_row)
    key_row2 = lanes([key_row, key_row])
    turned = jnp.transpose(subl([mask_f] * H))
    for s in range(S):
        kcols[s] = jnp.broadcast_to(turned[:, s:s + 1], (L, L))

    def iota(shape, axis):
        return lax.broadcasted_iota(jnp.int32, shape, axis)

    def ones_at(where):
        return jnp.where(where, 1.0, 0.0).astype(BF16)

    src, lane = iota((4 * L, L), 0), iota((4 * L, L), 1)
    pick[...] = ones_at((src // L == lane // R) & (src % L == me * R + lane % R))
    src, lane = iota((L, 8 * L), 0), iota((L, 8 * L), 1)
    spread[...] = ones_at(src == lane // L2 * R + lane % R)
    src, lane = iota((L, L), 0), iota((L, L), 1)
    own_mask = mm(mask_f.astype(BF16), ones_at(src == me * R + lane % R))
    for s in range(S):
        omask[s] = jnp.broadcast_to(own_mask[s:s + 1, :], (H, L))

    def bias_rows(bsc, ln_ref, b, group):
        def stage(t):
            n = t * 2
            rows = part(mm(w_bias[b], pair(ln_ref, n)), group, H)
            bsc[rows_at(n, H), :] = lo(rows)
            bsc[rows_at(n + 1, H), :] = hi(rows)
        return stage

    def pack_bias(bsc, ref, first, heads):
        for h in range(heads):
            ref[h, my_rows, :] = bsc[pl.ds(first + h, R, stride=H), :].astype(BF16)

    def normalise(t):
        for n in (t * 2, t * 2 + 1):
            ln_t[n] = layer_norm_t(z_t[n])

    def make_tri_bias(ref, by_key):
        for h in range(4):
            t = ref[h].astype(F32) * LOG2E
            t = t if by_key else jnp.transpose(t)
            bt_tri[:, cols(h)] = jnp.where(key_col > 0, t, NEG)

    def project_stages(w_in_ref):
        def project(t):
            n = t * 2
            ln2 = pair(ln_t, n)
            put_pair(p_q, n, mm(part(w_in_ref, 0, L), ln2).astype(BF16))
            k_s[...] = round_bf16(mm(part(w_in_ref, 1, L), ln2)) * key_row2
            put_pair(p_v, n, mm(part(w_in_ref, 2, L), ln2).astype(BF16))
            put_pair(p_sg, n, round_bf16(mm(part(w_in_ref, 3, L), ln2)))

        def turn(t):
            for r in range(2):
                p_kt[t * 2 + r] = jnp.transpose(k_s[:, cols(r)]).astype(BF16)
                p_sg[t * 2 + r] = sigmoid(p_sg[t * 2 + r])

        return [project, turn]

    def weigh(t):
        for k in range(4):
            for half in (cols(0), cols(1)):
                e = jnp.exp2(x_s[k, :, half] - m_s[k, :, half])
                w_s[k, :, half] = (e * (1.0 / jnp.sum(e, axis=0, keepdims=True))).astype(BF16)

    def put_score(k, x):
        x_s[k] = x
        m_s[k] = jnp.max(x, axis=0, keepdims=True)

    def attend_stages(w_out_t, finish):
        scale = R ** -0.5 * LOG2E

        def score(t):
            for r in range(2):
                q = p_q[t * 2 + r]
                kt = p_kt[t * 2 + r]
                for hp in range(2):
                    blocks = [only(part(q, h, R), h, R, 4) for h in (2 * hp, 2 * hp + 1)]
                    put_score(2 * r + hp, mm(kt, lanes(blocks)) * scale + bt_tri[:, cols(hp, L2)])

        def gather_values(t):
            for r in range(2):
                v = p_v[t * 2 + r]
                outs = []
                for hp in range(2):
                    o2 = mm(part(v, hp, C), w_s[2 * r + hp])
                    outs += [lo(part(o2, 0, R)), hi(part(o2, 1, R))]
                g_s[:, cols(r)] = (subl(outs) * p_sg[t * 2 + r]).astype(BF16)

        def project_out(t):
            finish[0](t, pair(z_t, t * 2).astype(F32) + mm(w_out_t[...], g_s[...]))

        return [score, weigh, gather_values, project_out] + finish[1:]

    def row_attention(b, load, store):
        scale = H ** -0.5 * LOG2E
        for t in range(4):
            proj = round_bf16(mm(w_row_in[b], layer_norm_t(load(t))))
            q, k, v, g = [part(proj, f, C) for f in range(4)]
            p_sg[4 + t, :C] = q
            mkt[t] = jnp.transpose(subl([k, k]))[:, :C].astype(BF16)
            mv[t] = v.astype(BF16)
            p_sg[t, :C] = sigmoid(g)

        def score(t):
            kt = mkt[t]
            kcol = kcols[4 * me + t]
            kcol2 = lanes([kcol, kcol])
            for hp in range(4):
                blocks = [only(p_sg[4 + t, cols(h, H)], h, H, H) for h in (2 * hp, 2 * hp + 1)]
                x = mm(kt, lanes(blocks).astype(BF16)) * scale + bt_row[:, cols(hp, L2)]
                put_score(hp, jnp.where(kcol2 > 0, x, NEG))

        def gather_values(t):
            outs = []
            for hp in range(4):
                o2 = mm(mv[t, cols(hp, S)], w_s[hp])
                outs += [lo(part(o2, 0, H)), hi(part(o2, 1, H))]
            g_s[:C, :L] = (subl(outs) * p_sg[t, :C]).astype(BF16)

        def project_out(t):
            store(t, (load(t).astype(F32) + mm(wro_t[b], g_s[:C, :L])).astype(BF16))

        pipeline([score, weigh, gather_values, project_out], 4)

    same_head = iota((C, L2), 0) // H == iota((C, L2), 1) // R
    block = iota((C, L), 1) // R

    def row_attention_own():
        scale = H ** -0.5 * LOG2E
        rows = subl([bsc_row[pl.ds(h, R, stride=H), :] for h in range(H)])
        bias = jnp.transpose(round_bf16(rows)) * LOG2E
        bt_row[:, :L2] = bias
        w_qg = subl([part(w_row_in[0], 0, C), part(w_row_in[0], 3, C)])

        def keys(t):
            ln2 = lanes([layer_norm_t(m_all[2 * t]), layer_norm_t(m_all[2 * t + 1])])
            kv = round_bf16(mm(w_row_in[0, C:3 * C], ln2))
            for s, x in ((2 * t, lo(kv)), (2 * t + 1, hi(kv))):
                mkt[s] = jnp.transpose(x)[:, :C].astype(BF16)
                mv[s] = part(x, 1, C).astype(BF16)

        def queries(t):
            own = mm(lanes([m_all[4 * t + k] for k in range(4)]), pick[...])
            m_own[t] = own.astype(BF16)
            qg = round_bf16(mm(w_qg, layer_norm_t(own)))
            p_sg[t, :C] = sigmoid(part(qg, 1, C))
            q = mm(part(qg, 0, C).astype(BF16), spread[...])
            for k in range(4):
                mq[4 * t + k] = jnp.where(same_head, q[:, cols(k, L2)], 0.0).astype(BF16)

        def score(t):
            for k in range(4):
                s = 4 * t + k
                x = mm(mkt[s], mq[s]) * scale + bt_row[:, :L2]
                put_score(k, jnp.where(lanes([kcols[s], kcols[s]]) > 0, x, NEG))

        def gather_values(t):
            out = jnp.zeros((C, L), F32)
            for k in range(4):
                o2 = jnp.where(same_head, mm(mv[4 * t + k], w_s[k]), 0.0)
                o = lo(o2) + hi(o2)
                o = o + pltpu.roll(o, C, 1)
                o = o + pltpu.roll(o, R, 1)
                out = jnp.where(block == k, o, out)
            g_s[:C, :L] = (out * p_sg[t, :C]).astype(BF16)

        def project_out(t):
            m_own[t] = (m_own[t].astype(F32) + mm(wro_t[0], g_s[:C, :L])).astype(BF16)

        for t in range(4):
            queries(t)
        for t in range(S // 2):
            keys(t)
        pipeline([score, weigh, gather_values, project_out], 4)

    def attend_columns(steps, mask):
        scale = H ** -0.5 * LOG2E

        def attend(a, carry):
            def at(s, f, d):
                return ckv[s, cols(f * H + d, H)]

            q = [cq[a, cols(d, H)] for d in range(H)]
            logits = []
            for t in range(S):
                acc = functools.reduce(jnp.add, [q[d] * at(t, 0, d) for d in range(H)])
                logits.append(jnp.where(mask[t] > 0, acc * scale, NEG))
            top = functools.reduce(jnp.maximum, logits)
            e = [jnp.exp2(x - top) for x in logits]
            inv = 1.0 / functools.reduce(jnp.add, e)
            probs = [round_bf16(x * inv) for x in e]
            outs = [functools.reduce(jnp.add, [probs[t] * at(t, 1, d) for t in range(S)]) for d in range(H)]
            og[a] = (subl(outs) * part(cq[a], 1, C)).astype(BF16)
            return carry
        lax.fori_loop(0, steps, attend, 0)

    def col_attention_own():
        ln4 = lanes([layer_norm_t(m_own[t]) for t in range(4)])
        proj = round_bf16(mm(wci_p[0], ln4))
        for t in range(4):
            x = proj[:, cols(t)]
            cq[t] = subl([part(x, 0, C), sigmoid(part(x, 3, C))])
            kv = x[C:3 * C].astype(BF16)
            for k in range(4):
                ckv[4 * t + k] = mm(kv, spread[:, cols(2 * k)])
        attend_columns(4, omask)
        new = mm(wco_t[0], lanes([og[t] for t in range(4)]))
        for t in range(4):
            m_dev[me, t] = (m_own[t].astype(F32) + new[:, cols(t)]).astype(BF16)

    def col_attention():
        def normalise_m(t):
            for s in (2 * t, 2 * t + 1):
                ln_m[s] = layer_norm_t(m_all[s])

        def project(t):
            proj = round_bf16(mm(wci_p[1], pair(ln_m, 2 * t)))
            put_pair(cq, 2 * t, subl([part(proj, 0, C), sigmoid(part(proj, 3, C))]))
            put_pair(ckv, 2 * t, proj[C:3 * C])
        pipeline([normalise_m, project], S // 2)
        attend_columns(S, cmask)

        def update(t):
            new = pair(m_all, 2 * t).astype(F32) + mm(wco_t[1], pair(og, 2 * t))
            put_pair(m_all, 2 * t, new.astype(BF16))
        return update

    def opm_halves(b, first):
        def normalise_m(t):
            for s in (2 * t, 2 * t + 1):
                ln_m[s] = layer_norm_t(m_all[s])

        def halves(t):
            both = mm(w_opm_in[b], pair(ln_m, 2 * t))
            for s, x in ((2 * t, lo(both)), (2 * t + 1, hi(both))):
                acs[rows_at(s, C), :] = x * msk[pl.ds(s, 1), :].astype(F32)
        pipeline(first + [normalise_m, halves], S // 2)

    row_id = lax.broadcasted_iota(jnp.int32, (S, L2), 0)
    lane_id = lax.broadcasted_iota(jnp.int32, (S, L2), 1)
    diag = row_id == lane_id // S

    def opm(b, finish):
        local, other = (0, R) if b == 0 else (R, 0)
        for q in range(R):
            r_all[q] = acs[pl.ds(other + q, S, stride=C), :].astype(BF16)
        for t in range(4):
            rows = subl([acs[pl.ds(local + H * t + p, S, stride=C), :] for p in range(H)])
            x_loc[:, cols(t)] = jnp.transpose(round_bf16(rows))

        def outer(t):
            left = []
            for k in range(4):
                row = x_loc[pl.ds(me * R + t * 4 + k, 1), :]
                for half in (cols(0, L2), cols(1, L2)):
                    left.append(jnp.where(diag, jnp.broadcast_to(row[:, half], (S, L2)), 0.0))
            left = subl(left).astype(BF16)
            for q in range(0, R, 2):
                put_pair(o_scr, q, mm(left, lanes([subl([r_all[q]] * S), subl([r_all[q + 1]] * S)])).astype(BF16))

        def contract(t):
            for k in range(2):
                blocks = [o_scr[:, cols(2 * k + j, R), :].reshape(R * R, L) for j in range(2)]
                n = t * 4 + 2 * k
                at = me * R + n
                norm = lanes([nrm[pl.ds(at, 1), :], nrm[pl.ds(at + 1, 1), :]])
                finish[0](n, mm(woo_t[b], lanes(blocks)) * norm)

        pipeline([outer, contract] + [
            lambda t, f=f: (f(2 * t), f(2 * t + 1)) for f in finish[1:]], R // 4)

    def put_z(t, z2):
        put_pair(z_t, 2 * t, z2.astype(BF16))

    def send_z(stage, b, size):
        def turn(t, z2):
            put_z(t, z2)
            z2 = round_bf16(z2)
            for r, x in ((0, lo(z2)), (1, hi(z2))):
                z_snd[stage, 2 * t + r] = jnp.transpose(x).astype(BF16)

        def send(t):
            for o in range(1, N_DAP):
                z_copy(stage, o, 2 * t, 2, 0, size).start()
            for n in (2 * t, 2 * t + 1):
                z_rcv[stage, me * R + n] = z_snd[stage, n, my_rows, :]
        return [turn, normalise, bias_rows(bsc_tri, ln_t, b, 1), send]

    def widen_z(stage, at, size):
        def widen(t):
            for r in range(4):
                n = t * 4 + r
                z_f[pl.ds(pl.multiple_of(n * (R + H) + at, H), size), :] = z_rcv[stage, n, pl.ds(at, size), :].astype(F32)
        pipeline([widen], R)

    def wait_z(stage, at, size):
        for o in range(1, N_DAP):
            z_copy(stage, o, 0, R, at, size).wait()

    def turn_z(t):
        for n in (2 * t, 2 * t + 1):
            z_t[n] = jnp.transpose(z_f[pl.ds(n, L, stride=R + H), :]).astype(BF16)

    wait(g_in)

    def enter(t):
        for n in (2 * t, 2 * t + 1):
            z_t[n] = jnp.transpose(z_in[n].astype(F32)).astype(BF16)
    pipeline([enter, normalise, bias_rows(bsc_row, ln_t, 0, 0)], R // 2)
    row_attention_own()
    col_attention_own()
    g = gather(1, m_dev.at[me])
    start(g)
    late_weights()
    wait(g)
    for t in range(4):
        whole = mm(lanes([m_dev[d, t] for d in range(4)]), join[...]).astype(BF16)
        for k in range(4):
            m_all[4 * t + k] = whole[:, cols(k)]
    opm_halves(0, [])

    def add_first(n, update2):
        put_pair(z_t, n, (pair(z_t, n).astype(F32) + update2).astype(BF16))
    opm(0, [add_first, normalise, bias_rows(bsc_tri, ln_t, 0, 1)])
    pack_bias(bsc_tri, tb.at[0], 0, 4)
    g = gather(2, tb.at[0, :, my_rows, :])
    start(g)
    pipeline(project_stages(w_ts_in.at[0]), R // 2)
    wait(g)
    make_tri_bias(tb.at[0], False)
    pipeline(attend_stages(wtri_t.at[0, 0], send_z(0, 0, R)), R // 2)
    pack_bias(bsc_tri, tb.at[1], 4, 4)
    g = gather(3, tb.at[1, :, my_rows, :])
    start(g)

    opm_halves(1, [col_attention()])

    def keep_update(n, update2):
        put_pair(u_opm, n, update2)
    opm(1, [keep_update])

    wait(g)
    make_tri_bias(tb.at[1], True)
    wait_z(0, 0, R)
    widen_z(0, 0, R)
    pipeline(
        [turn_z, normalise] + project_stages(w_te_in.at[0])
        + attend_stages(wtri_t.at[1, 0], [put_z, normalise, bias_rows(bsc_row, ln_t, 1, 0)]), R // 2)

    pack_bias(bsc_row, rb, 0, H)
    g_row = gather(4, rb.at[:, my_rows, :])
    start(g_row)

    def add_second(t):
        put_z(t, pair(z_t, 2 * t).astype(F32) + pair(u_opm, 2 * t))
    pipeline([add_second, normalise, bias_rows(bsc_tri, ln_t, 1, 1)], R // 2)
    pack_bias(bsc_tri, tb.at[2], 4, 4)
    g = gather(5, tb.at[2, :, my_rows, :])
    start(g)
    pipeline(project_stages(w_te_in.at[1]), R // 2)
    wait(g)
    make_tri_bias(tb.at[2], False)
    pipeline(attend_stages(wtri_t.at[1, 1], send_z(1, 1, S)), R // 2)
    for o in range(1, N_DAP):
        z_copy(2, o, 0, R, S, S).start()
    pack_bias(bsc_tri, tb.at[3], 0, 4)
    g = gather(6, tb.at[3, :, my_rows, :])
    start(g)

    wait(g_row)
    for h in range(H):
        bt_row[:, cols(h)] = rb[h].astype(F32) * LOG2E

    def emit_m(s, value):
        m_own[s] = value
    row_attention(1, lambda s: m_all[4 * me + s], emit_m)
    m_done = pltpu.make_async_copy(m_own, m_out, in_sems.at[0])
    m_done.start()

    wait(g)
    make_tri_bias(tb.at[3], True)

    def emit_z(t, z2):
        for n, x in ((2 * t, lo(z2)), (2 * t + 1, hi(z2))):
            z_snd[0, n] = jnp.transpose(x).astype(BF16)

    def put_out(n, count):
        return pltpu.make_async_copy(z_snd.at[0, pl.ds(n, count)], z_out.at[pl.ds(n, count)], in_sems.at[1])

    def leave(t):
        put_out(2 * t, 2).start()

    def second_half():
        wait_z(2, S, S)
        widen_z(1, S, S)
    wait_z(1, 0, S)
    widen_z(1, 0, S)
    pipeline(
        [turn_z, normalise] + project_stages(w_ts_in.at[1]) + attend_stages(wtri_t.at[0, 1], [emit_z, leave]),
        R // 2, R // 4, second_half)
    m_done.wait()
    put_out(0, R).wait()


def hand_out(m_new, z_new, m_out, z_out):
    m_out[...] = m_new[...]
    z_out[...] = z_new[...]


def solution(mesh):
    def local_step(msa_act, pair_act, msa_mask, res_mask, w_row_bias, w_row_in, w_row_out, w_col_in, w_col_out, w_opm_in, w_opm_out, w_ts_bias, w_ts_in, w_ts_out, w_te_bias, w_te_in, w_te_out):
        def rows_first(w):
            w = jnp.moveaxis(w, 1, -1)
            return w.reshape(2, -1, w.shape[-1])

        def flat_out(w):
            return w.reshape(2, -1, w.shape[-1])

        w_bias = jnp.concatenate([jnp.swapaxes(w, 1, 2) for w in (w_row_bias, w_ts_bias, w_te_bias)], axis=1)
        hbm = pl.BlockSpec(memory_space=pltpu.HBM)

        def wide(*shape):
            return pltpu.VMEM(shape, F32)

        def half(*shape):
            return pltpu.VMEM(shape, BF16)

        scratch = dict(
            z_t=half(R, L, L), ln_t=half(R, L, L), p_q=half(R, L, L), p_kt=half(R, L, L), p_v=half(R, L, L),
            p_sg=wide(R, L, L), k_s=wide(L, L2), bsc_row=wide(R * H, L), bsc_tri=wide(R * H, L),
            rb=half(H, L, L), tb=half(4, 4, L, L), bt_row=wide(L, H * L), bt_tri=wide(L, 4 * L),
            m_all=half(S, C, L), m_dev=half(4, 4, C, L), m_own=half(4, C, L), ln_m=half(S, C, L),
            cq=wide(S, L, L), ckv=wide(S, L, L), og=half(S, C, L),
            cmask=wide(S, H, L), omask=wide(S, H, L), kcols=wide(S, L, L),
            mq=half(S, C, L2), mkt=half(S, L, C), mv=half(S, C, L),
            pick=half(4 * L, L), spread=half(L, 8 * L), join=half(4 * L, 4 * L),
            acs=wide(S * C, L), r_all=half(R, S, L), x_loc=wide(L, R * S),
            o_scr=half(R, L, L), u_opm=wide(R, L, L), z_snd=half(2, R, L, L), z_rcv=half(2, L, R, L),
            z_f=wide(L * (R + H), L), nrm=wide(L, L), tmp=wide(R * R, L),
            wro_t=half(2, C, C), wci_p=half(2, 4 * C, C), wco_t=half(2, C, C), woo_t=half(2, L, R * R),
            wtri_t=half(2, 2, L, L), x_s=wide(4, L, L2), m_s=wide(4, 1, L2), w_s=half(4, L, L2), g_s=half(L, L2),
        )
        sems = [pltpu.SemaphoreType.DMA((n, N_DAP - 1)) for n in (7, 7, 3, 3)]
        operands = (
            jnp.swapaxes(msa_act, 1, 2), pair_act, msa_mask, res_mask.reshape(1, L), w_bias,
            rows_first(w_row_in), flat_out(w_row_out), rows_first(w_col_in), flat_out(w_col_out),
            rows_first(w_opm_in), flat_out(w_opm_out),
            rows_first(w_ts_in), flat_out(w_ts_out), rows_first(w_te_in), flat_out(w_te_out),
        )
        held = [pltpu.VMEM(x.shape, x.dtype) for x in operands[1:]] + [pltpu.SemaphoreType.DMA((N_IN,))]
        m_new, z_new = pl.pallas_call(
            body,
            out_shape=(jax.ShapeDtypeStruct((4, C, L), BF16), jax.ShapeDtypeStruct((R, L, L), BF16)),
            in_specs=[hbm] * N_IN,
            out_specs=(hbm, hbm),
            scratch_shapes=held + list(scratch.values()) + sems,
            compiler_params=pltpu.CompilerParams(collective_id=0, has_side_effects=True, vmem_limit_bytes=60 * 2 ** 20),
        )(*operands)
        steps = 4

        def blocks(array):
            shape = (array.shape[0] // steps,) + array.shape[1:]
            return pl.BlockSpec(shape, lambda k: (k, 0, 0))

        specs = [blocks(m_new), blocks(z_new)]
        m_new, z_new = pl.pallas_call(
            hand_out, grid=(steps,), in_specs=specs, out_specs=specs,
            out_shape=[jax.ShapeDtypeStruct(x.shape, x.dtype) for x in (m_new, z_new)],
        )(m_new, z_new)
        return jnp.swapaxes(m_new, 1, 2), z_new

    in_specs = (P(('data', 'dap')), P(('data', 'dap')), P('data'), P('data')) + (P(),) * 13
    out_specs = (P(('data', 'dap')), P(('data', 'dap')))
    return jax.shard_map(local_step, mesh=mesh, in_specs=in_specs, out_specs=out_specs, check_vma=False)
```

```python
import functools

import jax
import jax.numpy as jnp
from jax import lax
from jax.experimental import pallas as pl
from jax.experimental.pallas import tpu as pltpu
from jax.sharding import PartitionSpec as P

F32 = jnp.float32
BF16 = jnp.bfloat16
LOG2E = 1.4426950408889634
NEG = -1e9 * LOG2E
N_DAP = 4
N_IN = 17
L = 128
R = 32
S = 16
C = 64
H = 8
L2 = 2 * L
FIRST = 24
MESH = pl.DeviceIdType.MESH


def mm(lhs, rhs):
    return jnp.dot(lhs, rhs, preferred_element_type=F32)


def mm_nt(lhs, rhs):
    return lax.dot_general(lhs, rhs, (((1,), (1,)), ((), ())), preferred_element_type=F32)


def lanes(parts):
    return jnp.concatenate(parts, axis=1)


def subl(parts):
    return jnp.concatenate(parts, axis=0)


def lo(x):
    return x[:, :L]


def hi(x):
    return x[:, L:]


def part(x, k, size):
    return x[k * size:(k + 1) * size]


def cols(k, size=L):
    return slice(k * size, (k + 1) * size)


def rows_at(n, size):
    return pl.ds(pl.multiple_of(n * size, size), size)


def pair(ref, n):
    return lanes([ref[n], ref[n + 1]])


def put_pair(ref, n, value):
    ref[n] = lo(value)
    ref[n + 1] = hi(value)


def only(value, k, size, count):
    zero = jnp.zeros((size, value.shape[1]), value.dtype)
    return subl([value if j == k else zero for j in range(count)])


def eye_bf16(n):
    rows = lax.broadcasted_iota(jnp.int32, (n, n), 0)
    columns = lax.broadcasted_iota(jnp.int32, (n, n), 1)
    return jnp.where(rows == columns, 1.0, 0.0).astype(BF16)


def layer_norm_t(x):
    x = x.astype(F32)
    inv_n = 1.0 / x.shape[0]
    centered = x - jnp.sum(x, axis=0, keepdims=True) * inv_n
    var = jnp.sum(centered * centered, axis=0, keepdims=True) * inv_n
    return (centered * lax.rsqrt(var + 1e-5)).astype(BF16)


def sigmoid(x):
    return 0.5 * jnp.tanh(0.5 * x) + 0.5


def round_bf16(x):
    return x.astype(BF16).astype(F32)


def pipeline(stages, trips, pause=None, resume=None):
    depth = len(stages)

    def run(t, first, last):
        for k in reversed(range(first, last)):
            stages[k](t - k)

    def step(t, carry):
        run(t, 0, depth)
        return carry

    for t in range(depth - 1):
        run(t, 0, t + 1)
    if pause is not None:
        lax.fori_loop(depth - 1, pause, step, 0)
        resume()
    lax.fori_loop(depth - 1 if pause is None else pause, trips, step, 0)
    for t in range(depth - 1):
        run(trips + t, t + 1, depth)


def body(
    m_hbm, *refs,
):
    n = N_IN - 1
    given, (m_out, z_out), refs = refs[:n], refs[n:n + 2], refs[n + 2:]
    held, in_sems, refs = refs[:n], refs[n], refs[n + 1:]
    main(m_hbm, given, held, in_sems, m_out, z_out, *refs)


def main(
    m_hbm, given, held, in_sems, m_out, z_out,
    z_t, ln_t, p_q, p_kt, p_v, p_sg, k_s, bsc_row, bsc_tri, rb, tb, bt_row, bt_tri, m_all, m_dev, m_own, ln_m, cq, ckv, og,
    cmask, omask, kcols, mq, mkt, mv, pick, spread, join, acs, r_all, x_loc, o_scr, u_opm, z_snd, z_rcv, z_f, nrm, tmp, wro_t, wci_p, wco_t, woo_t, wtri_t,
    x_s, m_s, w_s, g_s, w_bias,
    g_send, g_recv, a_send, a_recv,
):
    me = lax.axis_index('dap')
    data = lax.axis_index('data')
    my_rows = rows_at(me, R)

    def peer(o):
        return (data, lax.rem(me + o, N_DAP))

    z_in, msk, rmsk, w_row_bias, w_ts_bias, w_te_bias = held[:6]
    w_row_in, w_row_out, w_col_in, w_col_out, w_opm_in, w_opm_out, w_ts_in, w_ts_out, w_te_in, w_te_out = held[6:]
    own_m = m_all.at[pl.ds(4 * me, 4)]
    copy_m = pltpu.make_async_copy(m_hbm, own_m, in_sems.at[N_IN - 1])
    copy_m.start()
    copies_in = [pltpu.make_async_copy(src, dst, in_sems.at[k]) for k, (src, dst) in enumerate(zip(given, held))]
    for c in copies_in:
        c.start()

    barrier = pltpu.get_barrier_semaphore()
    for o in range(1, N_DAP):
        pl.semaphore_signal(barrier, inc=1, device_id=peer(o), device_id_type=MESH)
    pl.semaphore_wait(barrier, N_DAP - 1)

    def gather(stage, ref):
        return [
            pltpu.make_async_remote_copy(
                src_ref=ref, dst_ref=ref, send_sem=g_send.at[stage, o - 1], recv_sem=g_recv.at[stage, o - 1],
                device_id=peer(o), device_id_type=MESH)
            for o in range(1, N_DAP)
        ]

    def start(copies):
        for c in copies:
            c.start()

    def wait(copies):
        for c in copies:
            c.wait()

    def z_copy(stage, o, first, count, at=0, size=R):
        dest = lax.rem(me + o, N_DAP)
        return pltpu.make_async_remote_copy(
            src_ref=z_snd.at[min(stage, 1), pl.ds(first, count), pl.ds(pl.multiple_of(dest * R + at, H), size), :],
            dst_ref=z_rcv.at[min(stage, 1), pl.ds(me * R + first, count), pl.ds(at, size), :],
            send_sem=a_send.at[stage, o - 1], recv_sem=a_recv.at[stage, o - 1],
            device_id=(data, dest), device_id_type=MESH)

    copy_m.wait()
    g_in = gather(0, own_m)
    start(g_in)
    for c in copies_in:
        c.wait()

    e_c = eye_bf16(C)
    e_l = eye_bf16(L)

    def every(first, count, stride):
        return tmp[pl.ds(first, count, stride=stride), :]

    for b in range(2):
        tmp[:H, :] = w_row_bias[b].astype(F32)
        tmp[H:H + 4, :] = w_ts_bias[b].astype(F32)
        tmp[H + 4:S, :] = w_te_bias[b].astype(F32)
        w_bias[b] = tmp[:S, :].astype(BF16)
        wro_t[b] = mm_nt(e_c, w_row_out[b]).astype(BF16)
        tmp[:4 * C, :C] = w_col_in[b].astype(F32)
        wci_p[b] = subl([every(f * C + d, H, H) for f in range(4) for d in range(H)])[:, :C].astype(BF16)
        tmp[:C, :C] = w_col_out[b].astype(F32)
        wco_t[b] = mm_nt(e_c, subl([every(d, H, H) for d in range(H)])[:, :C].astype(BF16)).astype(BF16)

    def late_weights():
        for b in range(2):
            wtri_t[0, b] = mm_nt(e_l, w_ts_out[b]).astype(BF16)
            wtri_t[1, b] = mm_nt(e_l, w_te_out[b]).astype(BF16)
        tmp[...] = w_opm_out[0].astype(F32)
        woo_t[0] = mm_nt(e_l, subl([every(q, R, R) for q in range(R)]).astype(BF16)).astype(BF16)
        woo_t[1] = mm_nt(e_l, w_opm_out[1]).astype(BF16)
        src, lane = iota((4 * L, 4 * L), 0), iota((4 * L, 4 * L), 1)
        join[...] = ones_at((src // L == lane % L // R) & (src % L == lane // L * R + lane % R))

    def down(row):
        return jnp.transpose(jnp.broadcast_to(row, (L, L)))

    mask_f = msk[...].astype(F32)
    for s in range(S):
        cmask[s] = jnp.broadcast_to(mask_f[s:s + 1, :], (H, L))
    mask_t = jnp.transpose(subl([mask_f] * H)).astype(BF16)[:, :S]
    nrm[...] = 1.0 / (1e-3 + mm(mask_t, mask_f.astype(BF16)))
    key_row = rmsk[...].astype(F32)
    key_col = down(key_row)
    key_row2 = lanes([key_row, key_row])
    turned = jnp.transpose(subl([mask_f] * H))
    for s in range(S):
        kcols[s] = jnp.broadcast_to(turned[:, s:s + 1], (L, L))

    def iota(shape, axis):
        return lax.broadcasted_iota(jnp.int32, shape, axis)

    def ones_at(where):
        return jnp.where(where, 1.0, 0.0).astype(BF16)

    src, lane = iota((4 * L, L), 0), iota((4 * L, L), 1)
    pick[...] = ones_at((src // L == lane // R) & (src % L == me * R + lane % R))
    src, lane = iota((L, 8 * L), 0), iota((L, 8 * L), 1)
    spread[...] = ones_at(src == lane // L2 * R + lane % R)
    src, lane = iota((L, L), 0), iota((L, L), 1)
    own_mask = mm(mask_f.astype(BF16), ones_at(src == me * R + lane % R))
    for s in range(S):
        omask[s] = jnp.broadcast_to(own_mask[s:s + 1, :], (H, L))

    def bias_rows(bsc, ln_ref, b, group):
        def stage(t):
            n = t * 2
            rows = part(mm(w_bias[b], pair(ln_ref, n)), group, H)
            bsc[rows_at(n, H), :] = lo(rows)
            bsc[rows_at(n + 1, H), :] = hi(rows)
        return stage

    def pack_bias(bsc, ref, first, heads):
        for h in range(heads):
            ref[h, my_rows, :] = bsc[pl.ds(first + h, R, stride=H), :].astype(BF16)

    def normalise(t):
        for n in (t * 2, t * 2 + 1):
            ln_t[n] = layer_norm_t(z_t[n])

    def make_tri_bias(ref, by_key):
        for h in range(4):
            t = ref[h].astype(F32) * LOG2E
            t = t if by_key else jnp.transpose(t)
            bt_tri[:, cols(h)] = jnp.where(key_col > 0, t, NEG)

    def project_stages(w_in_ref):
        def project(t):
            n = t * 2
            ln2 = pair(ln_t, n)
            put_pair(p_q, n, mm(part(w_in_ref, 0, L), ln2).astype(BF16))
            k_s[...] = round_bf16(mm(part(w_in_ref, 1, L), ln2)) * key_row2
            put_pair(p_v, n, mm(part(w_in_ref, 2, L), ln2).astype(BF16))
            put_pair(p_sg, n, round_bf16(mm(part(w_in_ref, 3, L), ln2)))

        def turn(t):
            for r in range(2):
                p_kt[t * 2 + r] = jnp.transpose(k_s[:, cols(r)]).astype(BF16)
                p_sg[t * 2 + r] = sigmoid(p_sg[t * 2 + r])

        return [project, turn]

    def weigh(t):
        for k in range(4):
            for half in (cols(0), cols(1)):
                e = jnp.exp2(x_s[k, :, half] - m_s[k, :, half])
                w_s[k, :, half] = (e * (1.0 / jnp.sum(e, axis=0, keepdims=True))).astype(BF16)

    def put_score(k, x):
        x_s[k] = x
        m_s[k] = jnp.max(x, axis=0, keepdims=True)

    def attend_stages(w_out_t, finish):
        scale = R ** -0.5 * LOG2E

        def score(t):
            for r in range(2):
                q = p_q[t * 2 + r]
                kt = p_kt[t * 2 + r]
                for hp in range(2):
                    blocks = [only(part(q, h, R), h, R, 4) for h in (2 * hp, 2 * hp + 1)]
                    put_score(2 * r + hp, mm(kt, lanes(blocks)) * scale + bt_tri[:, cols(hp, L2)])

        def gather_values(t):
            for r in range(2):
                v = p_v[t * 2 + r]
                outs = []
                for hp in range(2):
                    o2 = mm(part(v, hp, C), w_s[2 * r + hp])
                    outs += [lo(part(o2, 0, R)), hi(part(o2, 1, R))]
                g_s[:, cols(r)] = (subl(outs) * p_sg[t * 2 + r]).astype(BF16)

        def project_out(t):
            finish[0](t, pair(z_t, t * 2).astype(F32) + mm(w_out_t[...], g_s[...]))

        return [score, weigh, gather_values, project_out] + finish[1:]

    def row_attention(b, load, store):
        scale = H ** -0.5 * LOG2E
        for t in range(4):
            proj = round_bf16(mm(w_row_in[b], layer_norm_t(load(t))))
            q, k, v, g = [part(proj, f, C) for f in range(4)]
            p_sg[4 + t, :C] = q
            mkt[t] = jnp.transpose(subl([k, k]))[:, :C].astype(BF16)
            mv[t] = v.astype(BF16)
            p_sg[t, :C] = sigmoid(g)

        def score(t):
            kt = mkt[t]
            kcol = kcols[4 * me + t]
            kcol2 = lanes([kcol, kcol])
            for hp in range(4):
                blocks = [only(p_sg[4 + t, cols(h, H)], h, H, H) for h in (2 * hp, 2 * hp + 1)]
                x = mm(kt, lanes(blocks).astype(BF16)) * scale + bt_row[:, cols(hp, L2)]
                put_score(hp, jnp.where(kcol2 > 0, x, NEG))

        def gather_values(t):
            outs = []
            for hp in range(4):
                o2 = mm(mv[t, cols(hp, S)], w_s[hp])
                outs += [lo(part(o2, 0, H)), hi(part(o2, 1, H))]
            g_s[:C, :L] = (subl(outs) * p_sg[t, :C]).astype(BF16)

        def project_out(t):
            store(t, (load(t).astype(F32) + mm(wro_t[b], g_s[:C, :L])).astype(BF16))

        pipeline([score, weigh, gather_values, project_out], 4)

    same_head = iota((C, L2), 0) // H == iota((C, L2), 1) // R
    block = iota((C, L), 1) // R

    def row_attention_own():
        scale = H ** -0.5 * LOG2E
        rows = subl([bsc_row[pl.ds(h, R, stride=H), :] for h in range(H)])
        bias = jnp.transpose(round_bf16(rows)) * LOG2E
        bt_row[:, :L2] = bias
        w_qg = subl([part(w_row_in[0], 0, C), part(w_row_in[0], 3, C)])

        def keys(t):
            ln2 = lanes([layer_norm_t(m_all[2 * t]), layer_norm_t(m_all[2 * t + 1])])
            kv = round_bf16(mm(w_row_in[0, C:3 * C], ln2))
            for s, x in ((2 * t, lo(kv)), (2 * t + 1, hi(kv))):
                mkt[s] = jnp.transpose(x)[:, :C].astype(BF16)
                mv[s] = part(x, 1, C).astype(BF16)

        def queries(t):
            own = mm(lanes([m_all[4 * t + k] for k in range(4)]), pick[...])
            m_own[t] = own.astype(BF16)
            qg = round_bf16(mm(w_qg, layer_norm_t(own)))
            p_sg[t, :C] = sigmoid(part(qg, 1, C))
            q = mm(part(qg, 0, C).astype(BF16), spread[...])
            for k in range(4):
                mq[4 * t + k] = jnp.where(same_head, q[:, cols(k, L2)], 0.0).astype(BF16)

        def score(t):
            for k in range(4):
                s = 4 * t + k
                x = mm(mkt[s], mq[s]) * scale + bt_row[:, :L2]
                put_score(k, jnp.where(lanes([kcols[s], kcols[s]]) > 0, x, NEG))

        def gather_values(t):
            out = jnp.zeros((C, L), F32)
            for k in range(4):
                o2 = jnp.where(same_head, mm(mv[4 * t + k], w_s[k]), 0.0)
                o = lo(o2) + hi(o2)
                o = o + pltpu.roll(o, C, 1)
                o = o + pltpu.roll(o, R, 1)
                out = jnp.where(block == k, o, out)
            g_s[:C, :L] = (out * p_sg[t, :C]).astype(BF16)

        def project_out(t):
            m_own[t] = (m_own[t].astype(F32) + mm(wro_t[0], g_s[:C, :L])).astype(BF16)

        for t in range(4):
            queries(t)
        for t in range(S // 2):
            keys(t)
        pipeline([score, weigh, gather_values, project_out], 4)

    def attend_columns(steps, mask):
        scale = H ** -0.5 * LOG2E

        def attend(a, carry):
            def at(s, f, d):
                return ckv[s, cols(f * H + d, H)]

            q = [cq[a, cols(d, H)] for d in range(H)]
            logits = []
            for t in range(S):
                acc = functools.reduce(jnp.add, [q[d] * at(t, 0, d) for d in range(H)])
                logits.append(jnp.where(mask[t] > 0, acc * scale, NEG))
            top = functools.reduce(jnp.maximum, logits)
            e = [jnp.exp2(x - top) for x in logits]
            inv = 1.0 / functools.reduce(jnp.add, e)
            probs = [round_bf16(x * inv) for x in e]
            outs = [functools.reduce(jnp.add, [probs[t] * at(t, 1, d) for t in range(S)]) for d in range(H)]
            og[a] = (subl(outs) * part(cq[a], 1, C)).astype(BF16)
            return carry
        lax.fori_loop(0, steps, attend, 0)

    def col_attention_own():
        ln4 = lanes([layer_norm_t(m_own[t]) for t in range(4)])
        proj = round_bf16(mm(wci_p[0], ln4))
        for t in range(4):
            x = proj[:, cols(t)]
            cq[t] = subl([part(x, 0, C), sigmoid(part(x, 3, C))])
            kv = x[C:3 * C].astype(BF16)
            for k in range(4):
                ckv[4 * t + k] = mm(kv, spread[:, cols(2 * k)])
        attend_columns(4, omask)
        new = mm(wco_t[0], lanes([og[t] for t in range(4)]))
        for t in range(4):
            m_dev[me, t] = (m_own[t].astype(F32) + new[:, cols(t)]).astype(BF16)

    def col_attention():
        def normalise_m(t):
            for s in (2 * t, 2 * t + 1):
                ln_m[s] = layer_norm_t(m_all[s])

        def project(t):
            proj = round_bf16(mm(wci_p[1], pair(ln_m, 2 * t)))
            put_pair(cq, 2 * t, subl([part(proj, 0, C), sigmoid(part(proj, 3, C))]))
            put_pair(ckv, 2 * t, proj[C:3 * C])
        pipeline([normalise_m, project], S // 2)
        attend_columns(S, cmask)

        def update(t):
            new = pair(m_all, 2 * t).astype(F32) + mm(wco_t[1], pair(og, 2 * t))
            put_pair(m_all, 2 * t, new.astype(BF16))
        return update

    def opm_halves(b, first):
        def normalise_m(t):
            for s in (2 * t, 2 * t + 1):
                ln_m[s] = layer_norm_t(m_all[s])

        def halves(t):
            both = mm(w_opm_in[b], pair(ln_m, 2 * t))
            for s, x in ((2 * t, lo(both)), (2 * t + 1, hi(both))):
                acs[rows_at(s, C), :] = x * msk[pl.ds(s, 1), :].astype(F32)
        pipeline(first + [normalise_m, halves], S // 2)

    row_id = lax.broadcasted_iota(jnp.int32, (S, L2), 0)
    lane_id = lax.broadcasted_iota(jnp.int32, (S, L2), 1)
    diag = row_id == lane_id // S

    def opm(b, finish):
        local, other = (0, R) if b == 0 else (R, 0)
        for q in range(R):
            r_all[q] = acs[pl.ds(other + q, S, stride=C), :].astype(BF16)
        for t in range(4):
            rows = subl([acs[pl.ds(local + H * t + p, S, stride=C), :] for p in range(H)])
            x_loc[:, cols(t)] = jnp.transpose(round_bf16(rows))

        def outer(t):
            left = []
            for k in range(4):
                row = x_loc[pl.ds(me * R + t * 4 + k, 1), :]
                for half in (cols(0, L2), cols(1, L2)):
                    left.append(jnp.where(diag, jnp.broadcast_to(row[:, half], (S, L2)), 0.0))
            left = subl(left).astype(BF16)
            for q in range(0, R, 2):
                put_pair(o_scr, q, mm(left, lanes([subl([r_all[q]] * S), subl([r_all[q + 1]] * S)])).astype(BF16))

        def contract(t):
            for k in range(2):
                blocks = [o_scr[:, cols(2 * k + j, R), :].reshape(R * R, L) for j in range(2)]
                n = t * 4 + 2 * k
                at = me * R + n
                norm = lanes([nrm[pl.ds(at, 1), :], nrm[pl.ds(at + 1, 1), :]])
                finish[0](n, mm(woo_t[b], lanes(blocks)) * norm)

        pipeline([outer, contract] + [
            lambda t, f=f: (f(2 * t), f(2 * t + 1)) for f in finish[1:]], R // 4)

    def put_z(t, z2):
        put_pair(z_t, 2 * t, z2.astype(BF16))

    def send_z(stage, b, size):
        def turn(t, z2):
            put_z(t, z2)
            z2 = round_bf16(z2)
            for r, x in ((0, lo(z2)), (1, hi(z2))):
                z_snd[stage, 2 * t + r] = jnp.transpose(x).astype(BF16)

        def send(t):
            for o in range(1, N_DAP):
                z_copy(stage, o, 2 * t, 2, 0, size).start()
            for n in (2 * t, 2 * t + 1):
                z_rcv[stage, me * R + n] = z_snd[stage, n, my_rows, :]
        return [turn, normalise, bias_rows(bsc_tri, ln_t, b, 1), send]

    def widen_z(stage, at, size):
        def widen(t):
            for r in range(4):
                n = t * 4 + r
                z_f[pl.ds(pl.multiple_of(n * (R + H) + at, H), size), :] = z_rcv[stage, n, pl.ds(at, size), :].astype(F32)
        pipeline([widen], R)

    def wait_z(stage, at, size):
        for o in range(1, N_DAP):
            z_copy(stage, o, 0, R, at, size).wait()

    def turn_z(t):
        for n in (2 * t, 2 * t + 1):
            z_t[n] = jnp.transpose(z_f[pl.ds(n, L, stride=R + H), :]).astype(BF16)

    wait(g_in)

    def enter(t):
        for n in (2 * t, 2 * t + 1):
            z_t[n] = jnp.transpose(z_in[n].astype(F32)).astype(BF16)
    pipeline([enter, normalise, bias_rows(bsc_row, ln_t, 0, 0)], R // 2)
    row_attention_own()
    col_attention_own()
    g = gather(1, m_dev.at[me])
    start(g)
    late_weights()
    wait(g)
    for t in range(4):
        whole = mm(lanes([m_dev[d, t] for d in range(4)]), join[...]).astype(BF16)
        for k in range(4):
            m_all[4 * t + k] = whole[:, cols(k)]
    opm_halves(0, [])

    def add_first(n, update2):
        put_pair(z_t, n, (pair(z_t, n).astype(F32) + update2).astype(BF16))
    opm(0, [add_first, normalise, bias_rows(bsc_tri, ln_t, 0, 1)])
    pack_bias(bsc_tri, tb.at[0], 0, 4)
    g = gather(2, tb.at[0, :, my_rows, :])
    start(g)
    pipeline(project_stages(w_ts_in.at[0]), R // 2)
    wait(g)
    make_tri_bias(tb.at[0], False)
    pipeline(attend_stages(wtri_t.at[0, 0], send_z(0, 0, R)), R // 2)
    pack_bias(bsc_tri, tb.at[1], 4, 4)
    g = gather(3, tb.at[1, :, my_rows, :])
    start(g)

    opm_halves(1, [col_attention()])

    def keep_update(n, update2):
        put_pair(u_opm, n, update2)
    opm(1, [keep_update])

    wait(g)
    make_tri_bias(tb.at[1], True)
    wait_z(0, 0, R)
    widen_z(0, 0, R)
    pipeline(
        [turn_z, normalise] + project_stages(w_te_in.at[0])
        + attend_stages(wtri_t.at[1, 0], [put_z, normalise, bias_rows(bsc_row, ln_t, 1, 0)]), R // 2)

    pack_bias(bsc_row, rb, 0, H)
    g_row = gather(4, rb.at[:, my_rows, :])
    start(g_row)

    def add_second(t):
        put_z(t, pair(z_t, 2 * t).astype(F32) + pair(u_opm, 2 * t))
    pipeline([add_second, normalise, bias_rows(bsc_tri, ln_t, 1, 1)], R // 2)
    pack_bias(bsc_tri, tb.at[2], 4, 4)
    g = gather(5, tb.at[2, :, my_rows, :])
    start(g)
    pipeline(project_stages(w_te_in.at[1]), R // 2)
    wait(g)
    make_tri_bias(tb.at[2], False)
    pipeline(attend_stages(wtri_t.at[1, 1], send_z(1, 1, FIRST)), R // 2)
    pack_bias(bsc_tri, tb.at[3], 0, 4)
    g = gather(6, tb.at[3, :, my_rows, :])
    start(g)
    for o in range(1, N_DAP):
        z_copy(2, o, 0, R, FIRST, R - FIRST).start()

    wait(g_row)
    for h in range(H):
        bt_row[:, cols(h)] = rb[h].astype(F32) * LOG2E

    def emit_m(s, value):
        m_own[s] = value
    row_attention(1, lambda s: m_all[4 * me + s], emit_m)
    m_done = pltpu.make_async_copy(m_own, m_out, in_sems.at[0])
    m_done.start()

    wait(g)
    make_tri_bias(tb.at[3], True)

    def emit_z(t, z2):
        for n, x in ((2 * t, lo(z2)), (2 * t + 1, hi(z2))):
            z_snd[0, n] = jnp.transpose(x).astype(BF16)

    def put_out(n, count):
        return pltpu.make_async_copy(z_snd.at[0, pl.ds(n, count)], z_out.at[pl.ds(n, count)], in_sems.at[1])

    def leave(t):
        put_out(2 * t, 2).start()

    def last_rows():
        wait_z(2, FIRST, R - FIRST)
        widen_z(1, FIRST, R - FIRST)
    wait_z(1, 0, FIRST)
    widen_z(1, 0, FIRST)
    pipeline(
        [turn_z, normalise] + project_stages(w_ts_in.at[1]) + attend_stages(wtri_t.at[0, 1], [emit_z, leave]),
        R // 2, FIRST // 2, last_rows)
    m_done.wait()
    put_out(0, R).wait()


def hand_out(m_new, z_new, m_out, z_out, m_v, z_v, sems):
    moves = [(m_new, m_v, m_out)]
    for k in range(4):
        moves.append([ref.at[pl.ds(k * H, H)] for ref in (z_new, z_v, z_out)])
    into = [pltpu.make_async_copy(src, mid, sems.at[0, k]) for k, (src, mid, _) in enumerate(moves)]
    out = [pltpu.make_async_copy(mid, dst, sems.at[1, k]) for k, (_, mid, dst) in enumerate(moves)]
    for c in into:
        c.start()
    for c, d in zip(into, out):
        c.wait()
        d.start()
    for d in out:
        d.wait()


def solution(mesh):
    def local_step(msa_act, pair_act, msa_mask, res_mask, w_row_bias, w_row_in, w_row_out, w_col_in, w_col_out, w_opm_in, w_opm_out, w_ts_bias, w_ts_in, w_ts_out, w_te_bias, w_te_in, w_te_out):
        def rows_first(w):
            w = jnp.moveaxis(w, 1, -1)
            return w.reshape(2, -1, w.shape[-1])

        def flat_out(w):
            return w.reshape(2, -1, w.shape[-1])

        w_bias = [jnp.swapaxes(w, 1, 2) for w in (w_row_bias, w_ts_bias, w_te_bias)]
        hbm = pl.BlockSpec(memory_space=pltpu.HBM)

        def wide(*shape):
            return pltpu.VMEM(shape, F32)

        def half(*shape):
            return pltpu.VMEM(shape, BF16)

        scratch = dict(
            z_t=half(R, L, L), ln_t=half(R, L, L), p_q=half(R, L, L), p_kt=half(R, L, L), p_v=half(R, L, L),
            p_sg=wide(R, L, L), k_s=wide(L, L2), bsc_row=wide(R * H, L), bsc_tri=wide(R * H, L),
            rb=half(H, L, L), tb=half(4, 4, L, L), bt_row=wide(L, H * L), bt_tri=wide(L, 4 * L),
            m_all=half(S, C, L), m_dev=half(4, 4, C, L), m_own=half(4, C, L), ln_m=half(S, C, L),
            cq=wide(S, L, L), ckv=wide(S, L, L), og=half(S, C, L),
            cmask=wide(S, H, L), omask=wide(S, H, L), kcols=wide(S, L, L),
            mq=half(S, C, L2), mkt=half(S, L, C), mv=half(S, C, L),
            pick=half(4 * L, L), spread=half(L, 8 * L), join=half(4 * L, 4 * L),
            acs=wide(S * C, L), r_all=half(R, S, L), x_loc=wide(L, R * S),
            o_scr=half(R, L, L), u_opm=wide(R, L, L), z_snd=half(2, R, L, L), z_rcv=half(2, L, R, L),
            z_f=wide(L * (R + H), L), nrm=wide(L, L), tmp=wide(R * R, L),
            wro_t=half(2, C, C), wci_p=half(2, 4 * C, C), wco_t=half(2, C, C), woo_t=half(2, L, R * R),
            wtri_t=half(2, 2, L, L), x_s=wide(4, L, L2), m_s=wide(4, 1, L2), w_s=half(4, L, L2), g_s=half(L, L2), w_bias=half(2, S, L),
        )
        sems = [pltpu.SemaphoreType.DMA((n, N_DAP - 1)) for n in (7, 7, 3, 3)]
        operands = (
            jnp.swapaxes(msa_act, 1, 2), pair_act, msa_mask, res_mask.reshape(1, L), *w_bias,
            rows_first(w_row_in), flat_out(w_row_out), rows_first(w_col_in), flat_out(w_col_out),
            rows_first(w_opm_in), flat_out(w_opm_out),
            rows_first(w_ts_in), flat_out(w_ts_out), rows_first(w_te_in), flat_out(w_te_out),
        )
        held = [pltpu.VMEM(x.shape, x.dtype) for x in operands[1:]] + [pltpu.SemaphoreType.DMA((N_IN,))]
        m_new, z_new = pl.pallas_call(
            body,
            out_shape=(jax.ShapeDtypeStruct((4, C, L), BF16), jax.ShapeDtypeStruct((R, L, L), BF16)),
            in_specs=[hbm] * N_IN,
            out_specs=(hbm, hbm),
            scratch_shapes=held + list(scratch.values()) + sems,
            compiler_params=pltpu.CompilerParams(collective_id=0, has_side_effects=True, vmem_limit_bytes=60 * 2 ** 20),
        )(*operands)
        m_new, z_new = pl.pallas_call(
            hand_out, in_specs=[hbm] * 2, out_specs=[hbm] * 2,
            out_shape=[jax.ShapeDtypeStruct(x.shape, x.dtype) for x in (m_new, z_new)],
            scratch_shapes=[half(4, C, L), half(R, L, L), pltpu.SemaphoreType.DMA((2, 5))],
        )(m_new, z_new)
        return jnp.swapaxes(m_new, 1, 2), z_new

    in_specs = (P(('data', 'dap')), P(('data', 'dap')), P('data'), P('data')) + (P(),) * 13
    out_specs = (P(('data', 'dap')), P(('data', 'dap')))
    return jax.shard_map(local_step, mesh=mesh, in_specs=in_specs, out_specs=out_specs, check_vma=False)
```

```python
import functools

import jax
import jax.numpy as jnp
from jax import lax
from jax.experimental import pallas as pl
from jax.experimental.pallas import tpu as pltpu
from jax.sharding import PartitionSpec as P

F32 = jnp.float32
BF16 = jnp.bfloat16
LOG2E = 1.4426950408889634
NEG = -1e9 * LOG2E
N_DAP = 4
N_IN = 17
L = 128
R = 32
S = 16
C = 64
H = 8
L2 = 2 * L
FIRST = 24
MESH = pl.DeviceIdType.MESH


def mm(lhs, rhs):
    return jnp.dot(lhs, rhs, preferred_element_type=F32)


def mm_nt(lhs, rhs):
    return lax.dot_general(lhs, rhs, (((1,), (1,)), ((), ())), preferred_element_type=F32)


def lanes(parts):
    return jnp.concatenate(parts, axis=1)


def subl(parts):
    return jnp.concatenate(parts, axis=0)


def lo(x):
    return x[:, :L]


def hi(x):
    return x[:, L:]


def part(x, k, size):
    return x[k * size:(k + 1) * size]


def cols(k, size=L):
    return slice(k * size, (k + 1) * size)


def rows_at(n, size):
    return pl.ds(pl.multiple_of(n * size, size), size)


def pair(ref, n):
    return lanes([ref[n], ref[n + 1]])


def put_pair(ref, n, value):
    ref[n] = lo(value)
    ref[n + 1] = hi(value)


def only(value, k, size, count):
    zero = jnp.zeros((size, value.shape[1]), value.dtype)
    return subl([value if j == k else zero for j in range(count)])


def eye_bf16(n):
    rows = lax.broadcasted_iota(jnp.int32, (n, n), 0)
    columns = lax.broadcasted_iota(jnp.int32, (n, n), 1)
    return jnp.where(rows == columns, 1.0, 0.0).astype(BF16)


def layer_norm_t(x):
    x = x.astype(F32)
    inv_n = 1.0 / x.shape[0]
    centered = x - jnp.sum(x, axis=0, keepdims=True) * inv_n
    var = jnp.sum(centered * centered, axis=0, keepdims=True) * inv_n
    return (centered * lax.rsqrt(var + 1e-5)).astype(BF16)


def sigmoid(x):
    return 0.5 * jnp.tanh(0.5 * x) + 0.5


def round_bf16(x):
    return x.astype(BF16).astype(F32)


def pipeline(stages, trips, pause=None, resume=None):
    depth = len(stages)

    def run(t, first, last):
        for k in reversed(range(first, last)):
            stages[k](t - k)

    def step(t, carry):
        run(t, 0, depth)
        return carry

    for t in range(depth - 1):
        run(t, 0, t + 1)
    if pause is not None:
        lax.fori_loop(depth - 1, pause, step, 0)
        resume()
    lax.fori_loop(depth - 1 if pause is None else pause, trips, step, 0)
    for t in range(depth - 1):
        run(trips + t, t + 1, depth)


def body(
    m_hbm, *refs,
):
    n = N_IN - 1
    given, (m_out, z_out), refs = refs[:n], refs[n:n + 2], refs[n + 2:]
    held, in_sems, refs = refs[:n], refs[n], refs[n + 1:]
    main(m_hbm, given, held, in_sems, m_out, z_out, *refs)


def main(
    m_hbm, given, held, in_sems, m_out, z_out,
    z_t, ln_t, p_q, p_kt, p_v, p_sg, k_s, bsc_row, bsc_tri, rb, tb, bt_row, bt_tri, m_all, m_dev, c_dev, m_own, ln_m, cq, ckv, og,
    cmask, omask, kcols, mq, mkt, mv, pick, spread, join, acs, r_all, x_loc, o_scr, u_opm, z_snd, z_rcv, z_f, nrm, tmp, wro_t, wci_p, wco_t, woo_t, wtri_t,
    x_s, m_s, w_s, g_s, w_bias,
    g_send, g_recv, a_send, a_recv,
):
    me = lax.axis_index('dap')
    data = lax.axis_index('data')
    my_rows = rows_at(me, R)

    def peer(o):
        return (data, lax.rem(me + o, N_DAP))

    z_in, msk, rmsk, w_row_bias, w_ts_bias, w_te_bias = held[:6]
    w_row_in, w_row_out, w_col_in, w_col_out, w_opm_in, w_opm_out, w_ts_in, w_ts_out, w_te_in, w_te_out = held[6:]
    own_m = m_all.at[pl.ds(4 * me, 4)]
    copy_m = pltpu.make_async_copy(m_hbm, own_m, in_sems.at[N_IN - 1])
    copy_m.start()
    copies_in = [pltpu.make_async_copy(src, dst, in_sems.at[k]) for k, (src, dst) in enumerate(zip(given, held))]
    for c in copies_in:
        c.start()

    barrier = pltpu.get_barrier_semaphore()
    for o in range(1, N_DAP):
        pl.semaphore_signal(barrier, inc=1, device_id=peer(o), device_id_type=MESH)
    pl.semaphore_wait(barrier, N_DAP - 1)

    def gather(stage, ref):
        return [
            pltpu.make_async_remote_copy(
                src_ref=ref, dst_ref=ref, send_sem=g_send.at[stage, o - 1], recv_sem=g_recv.at[stage, o - 1],
                device_id=peer(o), device_id_type=MESH)
            for o in range(1, N_DAP)
        ]

    def start(copies):
        for c in copies:
            c.start()

    def wait(copies):
        for c in copies:
            c.wait()

    def z_copy(stage, o, first, count, at=0, size=R):
        dest = lax.rem(me + o, N_DAP)
        return pltpu.make_async_remote_copy(
            src_ref=z_snd.at[min(stage, 1), pl.ds(first, count), pl.ds(pl.multiple_of(dest * R + at, H), size), :],
            dst_ref=z_rcv.at[min(stage, 1), pl.ds(me * R + first, count), pl.ds(at, size), :],
            send_sem=a_send.at[stage, o - 1], recv_sem=a_recv.at[stage, o - 1],
            device_id=(data, dest), device_id_type=MESH)

    copy_m.wait()
    g_in = gather(0, own_m)
    start(g_in)
    for c in copies_in:
        c.wait()

    e_c = eye_bf16(C)
    e_l = eye_bf16(L)

    def every(first, count, stride):
        return tmp[pl.ds(first, count, stride=stride), :]

    for b in range(2):
        tmp[:H, :] = w_row_bias[b].astype(F32)
        tmp[H:H + 4, :] = w_ts_bias[b].astype(F32)
        tmp[H + 4:S, :] = w_te_bias[b].astype(F32)
        w_bias[b] = tmp[:S, :].astype(BF16)
        wro_t[b] = mm_nt(e_c, w_row_out[b]).astype(BF16)
        tmp[:4 * C, :C] = w_col_in[b].astype(F32)
        wci_p[b] = subl([every(f * C + d, H, H) for f in range(4) for d in range(H)])[:, :C].astype(BF16)
        tmp[:C, :C] = w_col_out[b].astype(F32)
        wco_t[b] = mm_nt(e_c, subl([every(d, H, H) for d in range(H)])[:, :C].astype(BF16)).astype(BF16)

    def late_weights():
        for b in range(2):
            wtri_t[0, b] = mm_nt(e_l, w_ts_out[b]).astype(BF16)
            wtri_t[1, b] = mm_nt(e_l, w_te_out[b]).astype(BF16)
        tmp[...] = w_opm_out[0].astype(F32)
        woo_t[0] = mm_nt(e_l, subl([every(q, R, R) for q in range(R)]).astype(BF16)).astype(BF16)
        woo_t[1] = mm_nt(e_l, w_opm_out[1]).astype(BF16)
        src, lane = iota((4 * L, 4 * L), 0), iota((4 * L, 4 * L), 1)
        join[...] = ones_at((src // L == lane % L // R) & (src % L == lane // L * R + lane % R))

    def down(row):
        return jnp.transpose(jnp.broadcast_to(row, (L, L)))

    mask_f = msk[...].astype(F32)
    for s in range(S):
        cmask[s] = jnp.broadcast_to(mask_f[s:s + 1, :], (H, L))
    mask_t = jnp.transpose(subl([mask_f] * H)).astype(BF16)[:, :S]
    nrm[...] = 1.0 / (1e-3 + mm(mask_t, mask_f.astype(BF16)))
    key_row = rmsk[...].astype(F32)
    key_col = down(key_row)
    key_row2 = lanes([key_row, key_row])
    turned = jnp.transpose(subl([mask_f] * H))
    for s in range(S):
        kcols[s] = jnp.broadcast_to(turned[:, s:s + 1], (L, L))

    def iota(shape, axis):
        return lax.broadcasted_iota(jnp.int32, shape, axis)

    def ones_at(where):
        return jnp.where(where, 1.0, 0.0).astype(BF16)

    src, lane = iota((4 * L, L), 0), iota((4 * L, L), 1)
    pick[...] = ones_at((src // L == lane // R) & (src % L == me * R + lane % R))
    src, lane = iota((L, 8 * L), 0), iota((L, 8 * L), 1)
    spread[...] = ones_at(src == lane // L2 * R + lane % R)
    src, lane = iota((L, L), 0), iota((L, L), 1)
    own_mask = mm(mask_f.astype(BF16), ones_at(src == me * R + lane % R))
    for s in range(S):
        omask[s] = jnp.broadcast_to(own_mask[s:s + 1, :], (H, L))

    def bias_rows(bsc, ln_ref, b, group):
        def stage(t):
            n = t * 2
            rows = part(mm(w_bias[b], pair(ln_ref, n)), group, H)
            bsc[rows_at(n, H), :] = lo(rows)
            bsc[rows_at(n + 1, H), :] = hi(rows)
        return stage

    def pack_bias(bsc, ref, first, heads):
        for h in range(heads):
            ref[h, my_rows, :] = bsc[pl.ds(first + h, R, stride=H), :].astype(BF16)

    def normalise(t):
        for n in (t * 2, t * 2 + 1):
            ln_t[n] = layer_norm_t(z_t[n])

    def make_tri_bias(ref, by_key):
        for h in range(4):
            t = ref[h].astype(F32) * LOG2E
            t = t if by_key else jnp.transpose(t)
            bt_tri[:, cols(h)] = jnp.where(key_col > 0, t, NEG)

    def project_stages(w_in_ref):
        def project(t):
            n = t * 2
            ln2 = pair(ln_t, n)
            put_pair(p_q, n, mm(part(w_in_ref, 0, L), ln2).astype(BF16))
            k_s[...] = round_bf16(mm(part(w_in_ref, 1, L), ln2)) * key_row2
            put_pair(p_v, n, mm(part(w_in_ref, 2, L), ln2).astype(BF16))
            put_pair(p_sg, n, round_bf16(mm(part(w_in_ref, 3, L), ln2)))

        def turn(t):
            for r in range(2):
                p_kt[t * 2 + r] = jnp.transpose(k_s[:, cols(r)]).astype(BF16)
                p_sg[t * 2 + r] = sigmoid(p_sg[t * 2 + r])

        return [project, turn]

    def weigh(t):
        for k in range(4):
            for half in (cols(0), cols(1)):
                e = jnp.exp2(x_s[k, :, half] - m_s[k, :, half])
                w_s[k, :, half] = (e * (1.0 / jnp.sum(e, axis=0, keepdims=True))).astype(BF16)

    def put_score(k, x):
        x_s[k] = x
        m_s[k] = jnp.max(x, axis=0, keepdims=True)

    def attend_stages(w_out_t, finish):
        scale = R ** -0.5 * LOG2E

        def score(t):
            for r in range(2):
                q = p_q[t * 2 + r]
                kt = p_kt[t * 2 + r]
                for hp in range(2):
                    blocks = [only(part(q, h, R), h, R, 4) for h in (2 * hp, 2 * hp + 1)]
                    put_score(2 * r + hp, mm(kt, lanes(blocks)) * scale + bt_tri[:, cols(hp, L2)])

        def gather_values(t):
            for r in range(2):
                v = p_v[t * 2 + r]
                outs = []
                for hp in range(2):
                    o2 = mm(part(v, hp, C), w_s[2 * r + hp])
                    outs += [lo(part(o2, 0, R)), hi(part(o2, 1, R))]
                g_s[:, cols(r)] = (subl(outs) * p_sg[t * 2 + r]).astype(BF16)

        def project_out(t):
            finish[0](t, pair(z_t, t * 2).astype(F32) + mm(w_out_t[...], g_s[...]))

        return [score, weigh, gather_values, project_out] + finish[1:]

    def row_attention(b, load, store):
        scale = H ** -0.5 * LOG2E
        for t in range(4):
            proj = round_bf16(mm(w_row_in[b], layer_norm_t(load(t))))
            q, k, v, g = [part(proj, f, C) for f in range(4)]
            p_sg[4 + t, :C] = q
            mkt[t] = jnp.transpose(subl([k, k]))[:, :C].astype(BF16)
            mv[t] = v.astype(BF16)
            p_sg[t, :C] = sigmoid(g)

        def score(t):
            kt = mkt[t]
            kcol = kcols[4 * me + t]
            kcol2 = lanes([kcol, kcol])
            for hp in range(4):
                blocks = [only(p_sg[4 + t, cols(h, H)], h, H, H) for h in (2 * hp, 2 * hp + 1)]
                x = mm(kt, lanes(blocks).astype(BF16)) * scale + bt_row[:, cols(hp, L2)]
                put_score(hp, jnp.where(kcol2 > 0, x, NEG))

        def gather_values(t):
            outs = []
            for hp in range(4):
                o2 = mm(mv[t, cols(hp, S)], w_s[hp])
                outs += [lo(part(o2, 0, H)), hi(part(o2, 1, H))]
            g_s[:C, :L] = (subl(outs) * p_sg[t, :C]).astype(BF16)

        def project_out(t):
            store(t, (load(t).astype(F32) + mm(wro_t[b], g_s[:C, :L])).astype(BF16))

        pipeline([score, weigh, gather_values, project_out], 4)

    same_head = iota((C, L2), 0) // H == iota((C, L2), 1) // R
    block = iota((C, L), 1) // R

    def row_attention_own():
        scale = H ** -0.5 * LOG2E
        rows = subl([bsc_row[pl.ds(h, R, stride=H), :] for h in range(H)])
        bias = jnp.transpose(round_bf16(rows)) * LOG2E
        bt_row[:, :L2] = bias
        w_qg = subl([part(w_row_in[0], 0, C), part(w_row_in[0], 3, C)])

        def keys(t):
            ln2 = lanes([layer_norm_t(m_all[2 * t]), layer_norm_t(m_all[2 * t + 1])])
            kv = round_bf16(mm(w_row_in[0, C:3 * C], ln2))
            for s, x in ((2 * t, lo(kv)), (2 * t + 1, hi(kv))):
                mkt[s] = jnp.transpose(x)[:, :C].astype(BF16)
                mv[s] = part(x, 1, C).astype(BF16)

        def queries(t):
            own = mm(lanes([m_all[4 * t + k] for k in range(4)]), pick[...])
            m_own[t] = own.astype(BF16)
            qg = round_bf16(mm(w_qg, layer_norm_t(own)))
            p_sg[t, :C] = sigmoid(part(qg, 1, C))
            q = mm(part(qg, 0, C).astype(BF16), spread[...])
            for k in range(4):
                mq[4 * t + k] = jnp.where(same_head, q[:, cols(k, L2)], 0.0).astype(BF16)

        def score(t):
            for k in range(4):
                s = 4 * t + k
                x = mm(mkt[s], mq[s]) * scale + bt_row[:, :L2]
                put_score(k, jnp.where(lanes([kcols[s], kcols[s]]) > 0, x, NEG))

        def gather_values(t):
            out = jnp.zeros((C, L), F32)
            for k in range(4):
                o2 = jnp.where(same_head, mm(mv[4 * t + k], w_s[k]), 0.0)
                o = lo(o2) + hi(o2)
                o = o + pltpu.roll(o, C, 1)
                o = o + pltpu.roll(o, R, 1)
                out = jnp.where(block == k, o, out)
            g_s[:C, :L] = (out * p_sg[t, :C]).astype(BF16)

        def project_out(t):
            m_own[t] = (m_own[t].astype(F32) + mm(wro_t[0], g_s[:C, :L])).astype(BF16)

        for t in range(4):
            queries(t)
        for t in range(S // 2):
            keys(t)
        pipeline([score, weigh, gather_values, project_out], 4)

    def attend_columns(steps, mask):
        scale = H ** -0.5 * LOG2E

        def attend(a, carry):
            def at(s, f, d):
                return ckv[s, cols(f * H + d, H)]

            q = [cq[a, cols(d, H)] for d in range(H)]
            logits = []
            for t in range(S):
                acc = functools.reduce(jnp.add, [q[d] * at(t, 0, d) for d in range(H)])
                logits.append(jnp.where(mask[t] > 0, acc * scale, NEG))
            top = functools.reduce(jnp.maximum, logits)
            e = [jnp.exp2(x - top) for x in logits]
            inv = 1.0 / functools.reduce(jnp.add, e)
            probs = [round_bf16(x * inv) for x in e]
            outs = [functools.reduce(jnp.add, [probs[t] * at(t, 1, d) for t in range(S)]) for d in range(H)]
            og[a] = (subl(outs) * part(cq[a], 1, C)).astype(BF16)
            return carry
        lax.fori_loop(0, steps, attend, 0)

    def col_attention_own():
        ln4 = lanes([layer_norm_t(m_own[t]) for t in range(4)])
        proj = round_bf16(mm(wci_p[0], ln4))
        for t in range(4):
            x = proj[:, cols(t)]
            cq[t] = subl([part(x, 0, C), sigmoid(part(x, 3, C))])
            kv = x[C:3 * C].astype(BF16)
            for k in range(4):
                ckv[4 * t + k] = mm(kv, spread[:, cols(2 * k)])
        attend_columns(4, omask)
        new = mm(wco_t[0], lanes([og[t] for t in range(4)]))
        for t in range(4):
            m_dev[me, t] = (m_own[t].astype(F32) + new[:, cols(t)]).astype(BF16)
        both = mm(w_opm_in[0], lanes([layer_norm_t(m_dev[me, t]) for t in range(4)]))
        for t in range(4):
            mask = omask[4 * t, :1]
            for k in range(1, 4):
                mask = jnp.where(block[:1] == k, omask[4 * t + k, :1], mask)
            x = (both[:, cols(t)] * mask).astype(BF16)
            c_dev[me, t] = part(x, 1, R)
            for k in range(4):
                acs[pl.ds((4 * t + k) * C, R), :] = mm(part(x, 0, R), spread[:, cols(2 * k)])

    def col_attention():
        def normalise_m(t):
            for s in (2 * t, 2 * t + 1):
                ln_m[s] = layer_norm_t(m_all[s])

        def project(t):
            proj = round_bf16(mm(wci_p[1], pair(ln_m, 2 * t)))
            put_pair(cq, 2 * t, subl([part(proj, 0, C), sigmoid(part(proj, 3, C))]))
            put_pair(ckv, 2 * t, proj[C:3 * C])
        pipeline([normalise_m, project], S // 2)
        attend_columns(S, cmask)

        def update(t):
            new = pair(m_all, 2 * t).astype(F32) + mm(wco_t[1], pair(og, 2 * t))
            put_pair(m_all, 2 * t, new.astype(BF16))
        return update

    def opm_halves(b, first):
        def normalise_m(t):
            for s in (2 * t, 2 * t + 1):
                ln_m[s] = layer_norm_t(m_all[s])

        def halves(t):
            both = mm(w_opm_in[b], pair(ln_m, 2 * t))
            for s, x in ((2 * t, lo(both)), (2 * t + 1, hi(both))):
                acs[rows_at(s, C), :] = x * msk[pl.ds(s, 1), :].astype(F32)
        pipeline(first + [normalise_m, halves], S // 2)

    row_id = lax.broadcasted_iota(jnp.int32, (S, L2), 0)
    lane_id = lax.broadcasted_iota(jnp.int32, (S, L2), 1)
    diag = row_id == lane_id // S

    def opm(b, finish):
        local, other = (0, R) if b == 0 else (R, 0)
        for q in range(R):
            r_all[q] = acs[pl.ds(other + q, S, stride=C), :].astype(BF16)
        for t in range(4):
            rows = subl([acs[pl.ds(local + H * t + p, S, stride=C), :] for p in range(H)])
            x_loc[:, cols(t)] = jnp.transpose(round_bf16(rows))

        def outer(t):
            left = []
            for k in range(4):
                row = x_loc[pl.ds(b * me * R + t * 4 + k, 1), :]
                for half in (cols(0, L2), cols(1, L2)):
                    left.append(jnp.where(diag, jnp.broadcast_to(row[:, half], (S, L2)), 0.0))
            left = subl(left).astype(BF16)
            for q in range(0, R, 2):
                put_pair(o_scr, q, mm(left, lanes([subl([r_all[q]] * S), subl([r_all[q + 1]] * S)])).astype(BF16))

        def contract(t):
            for k in range(2):
                blocks = [o_scr[:, cols(2 * k + j, R), :].reshape(R * R, L) for j in range(2)]
                n = t * 4 + 2 * k
                at = me * R + n
                norm = lanes([nrm[pl.ds(at, 1), :], nrm[pl.ds(at + 1, 1), :]])
                finish[0](n, mm(woo_t[b], lanes(blocks)) * norm)

        pipeline([outer, contract] + [
            lambda t, f=f: (f(2 * t), f(2 * t + 1)) for f in finish[1:]], R // 4)

    def put_z(t, z2):
        put_pair(z_t, 2 * t, z2.astype(BF16))

    def send_z(stage, b, size):
        def turn(t, z2):
            put_z(t, z2)
            z2 = round_bf16(z2)
            for r, x in ((0, lo(z2)), (1, hi(z2))):
                z_snd[stage, 2 * t + r] = jnp.transpose(x).astype(BF16)

        def send(t):
            for o in range(1, N_DAP):
                z_copy(stage, o, 2 * t, 2, 0, size).start()
            for n in (2 * t, 2 * t + 1):
                z_rcv[stage, me * R + n] = z_snd[stage, n, my_rows, :]
        return [turn, normalise, bias_rows(bsc_tri, ln_t, b, 1), send]

    def widen_z(stage, at, size):
        def widen(t):
            for r in range(4):
                n = t * 4 + r
                z_f[pl.ds(pl.multiple_of(n * (R + H) + at, H), size), :] = z_rcv[stage, n, pl.ds(at, size), :].astype(F32)
        pipeline([widen], R)

    def wait_z(stage, at, size):
        for o in range(1, N_DAP):
            z_copy(stage, o, 0, R, at, size).wait()

    def turn_z(t):
        for n in (2 * t, 2 * t + 1):
            z_t[n] = jnp.transpose(z_f[pl.ds(n, L, stride=R + H), :]).astype(BF16)

    def enter(t):
        for n in (2 * t, 2 * t + 1):
            z_t[n] = jnp.transpose(z_in[n].astype(F32)).astype(BF16)
    pipeline([enter, normalise, bias_rows(bsc_row, ln_t, 0, 0)], R // 2)
    wait(g_in)
    row_attention_own()
    col_attention_own()
    g = gather(7, c_dev.at[me])
    start(g)
    g_m = gather(1, m_dev.at[me])
    start(g_m)
    late_weights()
    wait(g)
    for t in range(4):
        whole = mm(lanes([c_dev[d, t] for d in range(4)]), join[...])
        for k in range(4):
            acs[pl.ds((4 * t + k) * C + R, R), :] = whole[:, cols(k)]

    def add_first(n, update2):
        put_pair(z_t, n, (pair(z_t, n).astype(F32) + update2).astype(BF16))
    opm(0, [add_first, normalise, bias_rows(bsc_tri, ln_t, 0, 1)])
    pack_bias(bsc_tri, tb.at[0], 0, 4)
    g = gather(2, tb.at[0, :, my_rows, :])
    start(g)
    pipeline(project_stages(w_ts_in.at[0]), R // 2)
    wait(g)
    make_tri_bias(tb.at[0], False)
    pipeline(attend_stages(wtri_t.at[0, 0], send_z(0, 0, R)), R // 2)
    pack_bias(bsc_tri, tb.at[1], 4, 4)
    g = gather(3, tb.at[1, :, my_rows, :])
    start(g)

    wait(g_m)
    for t in range(4):
        whole = mm(lanes([m_dev[d, t] for d in range(4)]), join[...]).astype(BF16)
        for k in range(4):
            m_all[4 * t + k] = whole[:, cols(k)]
    opm_halves(1, [col_attention()])

    def keep_update(n, update2):
        put_pair(u_opm, n, update2)
    opm(1, [keep_update])

    wait(g)
    make_tri_bias(tb.at[1], True)
    wait_z(0, 0, R)
    widen_z(0, 0, R)
    pipeline(
        [turn_z, normalise] + project_stages(w_te_in.at[0])
        + attend_stages(wtri_t.at[1, 0], [put_z, normalise, bias_rows(bsc_row, ln_t, 1, 0)]), R // 2)

    pack_bias(bsc_row, rb, 0, H)
    g_row = gather(4, rb.at[:, my_rows, :])
    start(g_row)

    def add_second(t):
        put_z(t, pair(z_t, 2 * t).astype(F32) + pair(u_opm, 2 * t))
    pipeline([add_second, normalise, bias_rows(bsc_tri, ln_t, 1, 1)], R // 2)
    pack_bias(bsc_tri, tb.at[2], 4, 4)
    g = gather(5, tb.at[2, :, my_rows, :])
    start(g)
    pipeline(project_stages(w_te_in.at[1]), R // 2)
    wait(g)
    make_tri_bias(tb.at[2], False)
    pipeline(attend_stages(wtri_t.at[1, 1], send_z(1, 1, FIRST)), R // 2)
    pack_bias(bsc_tri, tb.at[3], 0, 4)
    g = gather(6, tb.at[3, :, my_rows, :])
    start(g)
    for o in range(1, N_DAP):
        z_copy(2, o, 0, R, FIRST, R - FIRST).start()

    wait(g_row)
    for h in range(H):
        bt_row[:, cols(h)] = rb[h].astype(F32) * LOG2E

    def emit_m(s, value):
        m_own[s] = value
    row_attention(1, lambda s: m_all[4 * me + s], emit_m)
    m_done = pltpu.make_async_copy(m_own, m_out, in_sems.at[0])
    m_done.start()

    wait(g)
    make_tri_bias(tb.at[3], True)

    def emit_z(t, z2):
        for n, x in ((2 * t, lo(z2)), (2 * t + 1, hi(z2))):
            z_snd[0, n] = jnp.transpose(x).astype(BF16)

    def put_out(n, count):
        return pltpu.make_async_copy(z_snd.at[0, pl.ds(n, count)], z_out.at[pl.ds(n, count)], in_sems.at[1])

    def leave(t):
        put_out(2 * t, 2).start()

    def last_rows():
        wait_z(2, FIRST, R - FIRST)
        widen_z(1, FIRST, R - FIRST)
    wait_z(1, 0, FIRST)
    widen_z(1, 0, FIRST)
    pipeline(
        [turn_z, normalise] + project_stages(w_ts_in.at[1]) + attend_stages(wtri_t.at[0, 1], [emit_z, leave]),
        R // 2, FIRST // 2, last_rows)
    m_done.wait()
    put_out(0, R).wait()


def hand_out(m_new, z_new, m_out, z_out, m_v, z_v, sems):
    moves = [(m_new, m_v, m_out)]
    for k in range(4):
        moves.append([ref.at[pl.ds(k * H, H)] for ref in (z_new, z_v, z_out)])
    into = [pltpu.make_async_copy(src, mid, sems.at[0, k]) for k, (src, mid, _) in enumerate(moves)]
    out = [pltpu.make_async_copy(mid, dst, sems.at[1, k]) for k, (_, mid, dst) in enumerate(moves)]
    for c in into:
        c.start()
    for c, d in zip(into, out):
        c.wait()
        d.start()
    for d in out:
        d.wait()


def solution(mesh):
    def local_step(msa_act, pair_act, msa_mask, res_mask, w_row_bias, w_row_in, w_row_out, w_col_in, w_col_out, w_opm_in, w_opm_out, w_ts_bias, w_ts_in, w_ts_out, w_te_bias, w_te_in, w_te_out):
        def rows_first(w):
            w = jnp.moveaxis(w, 1, -1)
            return w.reshape(2, -1, w.shape[-1])

        def flat_out(w):
            return w.reshape(2, -1, w.shape[-1])

        w_bias = [jnp.swapaxes(w, 1, 2) for w in (w_row_bias, w_ts_bias, w_te_bias)]
        hbm = pl.BlockSpec(memory_space=pltpu.HBM)

        def wide(*shape):
            return pltpu.VMEM(shape, F32)

        def half(*shape):
            return pltpu.VMEM(shape, BF16)

        scratch = dict(
            z_t=half(R, L, L), ln_t=half(R, L, L), p_q=half(R, L, L), p_kt=half(R, L, L), p_v=half(R, L, L),
            p_sg=wide(R, L, L), k_s=wide(L, L2), bsc_row=wide(R * H, L), bsc_tri=wide(R * H, L),
            rb=half(H, L, L), tb=half(4, 4, L, L), bt_row=wide(L, H * L), bt_tri=wide(L, 4 * L),
            m_all=half(S, C, L), m_dev=half(4, 4, C, L), c_dev=half(4, 4, R, L), m_own=half(4, C, L), ln_m=half(S, C, L),
            cq=wide(S, L, L), ckv=wide(S, L, L), og=half(S, C, L),
            cmask=wide(S, H, L), omask=wide(S, H, L), kcols=wide(S, L, L),
            mq=half(S, C, L2), mkt=half(S, L, C), mv=half(S, C, L),
            pick=half(4 * L, L), spread=half(L, 8 * L), join=half(4 * L, 4 * L),
            acs=wide(S * C, L), r_all=half(R, S, L), x_loc=wide(L, R * S),
            o_scr=half(R, L, L), u_opm=wide(R, L, L), z_snd=half(2, R, L, L), z_rcv=half(2, L, R, L),
            z_f=wide(L * (R + H), L), nrm=wide(L, L), tmp=wide(R * R, L),
            wro_t=half(2, C, C), wci_p=half(2, 4 * C, C), wco_t=half(2, C, C), woo_t=half(2, L, R * R),
            wtri_t=half(2, 2, L, L), x_s=wide(4, L, L2), m_s=wide(4, 1, L2), w_s=half(4, L, L2), g_s=half(L, L2), w_bias=half(2, S, L),
        )
        sems = [pltpu.SemaphoreType.DMA((n, N_DAP - 1)) for n in (8, 8, 3, 3)]
        operands = (
            jnp.swapaxes(msa_act, 1, 2), pair_act, msa_mask, res_mask.reshape(1, L), *w_bias,
            rows_first(w_row_in), flat_out(w_row_out), rows_first(w_col_in), flat_out(w_col_out),
            rows_first(w_opm_in), flat_out(w_opm_out),
            rows_first(w_ts_in), flat_out(w_ts_out), rows_first(w_te_in), flat_out(w_te_out),
        )
        held = [pltpu.VMEM(x.shape, x.dtype) for x in operands[1:]] + [pltpu.SemaphoreType.DMA((N_IN,))]
        m_new, z_new = pl.pallas_call(
            body,
            out_shape=(jax.ShapeDtypeStruct((4, C, L), BF16), jax.ShapeDtypeStruct((R, L, L), BF16)),
            in_specs=[hbm] * N_IN,
            out_specs=(hbm, hbm),
            scratch_shapes=held + list(scratch.values()) + sems,
            compiler_params=pltpu.CompilerParams(collective_id=0, has_side_effects=True, vmem_limit_bytes=60 * 2 ** 20),
        )(*operands)
        m_new, z_new = pl.pallas_call(
            hand_out, in_specs=[hbm] * 2, out_specs=[hbm] * 2,
            out_shape=[jax.ShapeDtypeStruct(x.shape, x.dtype) for x in (m_new, z_new)],
            scratch_shapes=[half(4, C, L), half(R, L, L), pltpu.SemaphoreType.DMA((2, 5))],
        )(m_new, z_new)
        return jnp.swapaxes(m_new, 1, 2), z_new

    in_specs = (P(('data', 'dap')), P(('data', 'dap')), P('data'), P('data')) + (P(),) * 13
    out_specs = (P(('data', 'dap')), P(('data', 'dap')))
    return jax.shard_map(local_step, mesh=mesh, in_specs=in_specs, out_specs=out_specs, check_vma=False)
```

```python
import functools

import jax
import jax.numpy as jnp
from jax import lax
from jax.experimental import pallas as pl
from jax.experimental.pallas import tpu as pltpu
from jax.sharding import PartitionSpec as P

F32 = jnp.float32
BF16 = jnp.bfloat16
LOG2E = 1.4426950408889634
NEG = -1e9 * LOG2E
N_DAP = 4
N_IN = 17
L = 128
R = 32
S = 16
C = 64
H = 8
L2 = 2 * L
FIRST = 24
MESH = pl.DeviceIdType.MESH


def mm(lhs, rhs):
    return jnp.dot(lhs, rhs, preferred_element_type=F32)


def mm_nt(lhs, rhs):
    return lax.dot_general(lhs, rhs, (((1,), (1,)), ((), ())), preferred_element_type=F32)


def lanes(parts):
    return jnp.concatenate(parts, axis=1)


def subl(parts):
    return jnp.concatenate(parts, axis=0)


def lo(x):
    return x[:, :L]


def hi(x):
    return x[:, L:]


def part(x, k, size):
    return x[k * size:(k + 1) * size]


def cols(k, size=L):
    return slice(k * size, (k + 1) * size)


def rows_at(n, size):
    return pl.ds(pl.multiple_of(n * size, size), size)


def pair(ref, n):
    return lanes([ref[n], ref[n + 1]])


def put_pair(ref, n, value):
    ref[n] = lo(value)
    ref[n + 1] = hi(value)


def only(value, k, size, count):
    zero = jnp.zeros((size, value.shape[1]), value.dtype)
    return subl([value if j == k else zero for j in range(count)])


def eye_bf16(n):
    rows = lax.broadcasted_iota(jnp.int32, (n, n), 0)
    columns = lax.broadcasted_iota(jnp.int32, (n, n), 1)
    return jnp.where(rows == columns, 1.0, 0.0).astype(BF16)


def layer_norm_t(x):
    x = x.astype(F32)
    inv_n = 1.0 / x.shape[0]
    centered = x - jnp.sum(x, axis=0, keepdims=True) * inv_n
    var = jnp.sum(centered * centered, axis=0, keepdims=True) * inv_n
    return (centered * lax.rsqrt(var + 1e-5)).astype(BF16)


def sigmoid(x):
    return 0.5 * jnp.tanh(0.5 * x) + 0.5


def round_bf16(x):
    return x.astype(BF16).astype(F32)


def pipeline(stages, trips, hooks=None):
    depth = len(stages)
    hooks = hooks or {}

    def run(t, first, last):
        for k in reversed(range(first, last)):
            stages[k](t - k)

    def step(t, carry):
        run(t, 0, depth)
        return carry

    begin = depth - 1
    for t in range(begin):
        if t in hooks:
            hooks[t]()
        run(t, 0, t + 1)
    for t in sorted(t for t in hooks if t >= begin):
        lax.fori_loop(begin, t, step, 0)
        hooks[t]()
        begin = t
    lax.fori_loop(begin, trips, step, 0)
    for t in range(depth - 1):
        run(trips + t, t + 1, depth)


def body(
    m_hbm, *refs,
):
    n = N_IN - 1
    given, (m_out, z_out), refs = refs[:n], refs[n:n + 2], refs[n + 2:]
    held, in_sems, refs = refs[:n], refs[n], refs[n + 1:]
    main(m_hbm, given, held, in_sems, m_out, z_out, *refs)


def main(
    m_hbm, given, held, in_sems, m_out, z_out,
    z_t, ln_t, p_q, p_kt, p_v, p_sg, k_s, bsc_row, bsc_tri, rb, tb, bt_row, bt_tri, m_all, m_dev, c_dev, m_own, ln_m, cq, ckv, og,
    cmask, omask, kcols, mq, mkt, mv, pick, spread, join, acs, r_all, x_loc, o_scr, u_opm, z_snd, z_rcv, z_f, nrm, tmp, wro_t, wci_p, wco_t, woo_t, wtri_t,
    x_s, m_s, w_s, g_s, w_bias,
    g_send, g_recv, a_send, a_recv,
):
    me = lax.axis_index('dap')
    data = lax.axis_index('data')
    my_rows = rows_at(me, R)

    def peer(o):
        return (data, lax.rem(me + o, N_DAP))

    z_in, msk, rmsk, w_row_bias, w_ts_bias, w_te_bias = held[:6]
    w_row_in, w_row_out, w_col_in, w_col_out, w_opm_in, w_opm_out, w_ts_in, w_ts_out, w_te_in, w_te_out = held[6:]
    own_m = m_all.at[pl.ds(4 * me, 4)]
    copy_m = pltpu.make_async_copy(m_hbm, own_m, in_sems.at[N_IN - 1])
    copy_m.start()
    copies_in = [pltpu.make_async_copy(src, dst, in_sems.at[k]) for k, (src, dst) in enumerate(zip(given, held))]
    for c in copies_in:
        c.start()

    barrier = pltpu.get_barrier_semaphore()
    for o in range(1, N_DAP):
        pl.semaphore_signal(barrier, inc=1, device_id=peer(o), device_id_type=MESH)
    pl.semaphore_wait(barrier, N_DAP - 1)

    def gather(stage, ref):
        return [
            pltpu.make_async_remote_copy(
                src_ref=ref, dst_ref=ref, send_sem=g_send.at[stage, o - 1], recv_sem=g_recv.at[stage, o - 1],
                device_id=peer(o), device_id_type=MESH)
            for o in range(1, N_DAP)
        ]

    def start(copies):
        for c in copies:
            c.start()

    def wait(copies):
        for c in copies:
            c.wait()

    def z_copy(stage, o, first, count, at=0, size=R):
        dest = lax.rem(me + o, N_DAP)
        return pltpu.make_async_remote_copy(
            src_ref=z_snd.at[min(stage, 1), pl.ds(first, count), pl.ds(pl.multiple_of(dest * R + at, H), size), :],
            dst_ref=z_rcv.at[min(stage, 1), pl.ds(me * R + first, count), pl.ds(at, size), :],
            send_sem=a_send.at[stage, o - 1], recv_sem=a_recv.at[stage, o - 1],
            device_id=(data, dest), device_id_type=MESH)

    copy_m.wait()
    g_in = gather(0, own_m)
    start(g_in)
    for c in copies_in:
        c.wait()

    e_c = eye_bf16(C)
    e_l = eye_bf16(L)

    def every(first, count, stride):
        return tmp[pl.ds(first, count, stride=stride), :]

    for b in range(2):
        tmp[:H, :] = w_row_bias[b].astype(F32)
        tmp[H:H + 4, :] = w_ts_bias[b].astype(F32)
        tmp[H + 4:S, :] = w_te_bias[b].astype(F32)
        w_bias[b] = tmp[:S, :].astype(BF16)
        wro_t[b] = mm_nt(e_c, w_row_out[b]).astype(BF16)
        tmp[:4 * C, :C] = w_col_in[b].astype(F32)
        wci_p[b] = subl([every(f * C + d, H, H) for f in range(4) for d in range(H)])[:, :C].astype(BF16)
        tmp[:C, :C] = w_col_out[b].astype(F32)
        wco_t[b] = mm_nt(e_c, subl([every(d, H, H) for d in range(H)])[:, :C].astype(BF16)).astype(BF16)

    def late_weights():
        for b in range(2):
            wtri_t[0, b] = mm_nt(e_l, w_ts_out[b]).astype(BF16)
            wtri_t[1, b] = mm_nt(e_l, w_te_out[b]).astype(BF16)
        tmp[...] = w_opm_out[0].astype(F32)
        woo_t[0] = mm_nt(e_l, subl([every(q, R, R) for q in range(R)]).astype(BF16)).astype(BF16)
        woo_t[1] = mm_nt(e_l, w_opm_out[1]).astype(BF16)
        src, lane = iota((4 * L, 4 * L), 0), iota((4 * L, 4 * L), 1)
        join[...] = ones_at((src // L == lane % L // R) & (src % L == lane // L * R + lane % R))

    def down(row):
        return jnp.transpose(jnp.broadcast_to(row, (L, L)))

    mask_f = msk[...].astype(F32)
    for s in range(S):
        cmask[s] = jnp.broadcast_to(mask_f[s:s + 1, :], (H, L))
    mask_t = jnp.transpose(subl([mask_f] * H)).astype(BF16)[:, :S]
    nrm[...] = 1.0 / (1e-3 + mm(mask_t, mask_f.astype(BF16)))
    key_row = rmsk[...].astype(F32)
    key_col = down(key_row)
    key_row2 = lanes([key_row, key_row])
    turned = jnp.transpose(subl([mask_f] * H))
    for s in range(S):
        kcols[s] = jnp.broadcast_to(turned[:, s:s + 1], (L, L))

    def iota(shape, axis):
        return lax.broadcasted_iota(jnp.int32, shape, axis)

    def ones_at(where):
        return jnp.where(where, 1.0, 0.0).astype(BF16)

    src, lane = iota((4 * L, L), 0), iota((4 * L, L), 1)
    pick[...] = ones_at((src // L == lane // R) & (src % L == me * R + lane % R))
    src, lane = iota((L, 8 * L), 0), iota((L, 8 * L), 1)
    spread[...] = ones_at(src == lane // L2 * R + lane % R)
    src, lane = iota((L, L), 0), iota((L, L), 1)
    own_mask = mm(mask_f.astype(BF16), ones_at(src == me * R + lane % R))
    for s in range(S):
        omask[s] = jnp.broadcast_to(own_mask[s:s + 1, :], (H, L))

    def bias_rows(bsc, ln_ref, b, group):
        def stage(t):
            n = t * 2
            rows = part(mm(w_bias[b], pair(ln_ref, n)), group, H)
            bsc[rows_at(n, H), :] = lo(rows)
            bsc[rows_at(n + 1, H), :] = hi(rows)
        return stage

    def pack_bias(bsc, ref, first, heads):
        for h in range(heads):
            ref[h, my_rows, :] = bsc[pl.ds(first + h, R, stride=H), :].astype(BF16)

    def normalise(t):
        for n in (t * 2, t * 2 + 1):
            ln_t[n] = layer_norm_t(z_t[n])

    def make_tri_bias(ref, by_key):
        for h in range(4):
            t = ref[h].astype(F32) * LOG2E
            t = t if by_key else jnp.transpose(t)
            bt_tri[:, cols(h)] = jnp.where(key_col > 0, t, NEG)

    def project_stages(w_in_ref):
        def project(t):
            n = t * 2
            ln2 = pair(ln_t, n)
            put_pair(p_q, n, mm(part(w_in_ref, 0, L), ln2).astype(BF16))
            k_s[...] = round_bf16(mm(part(w_in_ref, 1, L), ln2)) * key_row2
            put_pair(p_v, n, mm(part(w_in_ref, 2, L), ln2).astype(BF16))
            put_pair(p_sg, n, round_bf16(mm(part(w_in_ref, 3, L), ln2)))

        def turn(t):
            for r in range(2):
                p_kt[t * 2 + r] = jnp.transpose(k_s[:, cols(r)]).astype(BF16)
                p_sg[t * 2 + r] = sigmoid(p_sg[t * 2 + r])

        return [project, turn]

    def weigh(t):
        for k in range(4):
            for half in (cols(0), cols(1)):
                e = jnp.exp2(x_s[k, :, half] - m_s[k, :, half])
                w_s[k, :, half] = (e * (1.0 / jnp.sum(e, axis=0, keepdims=True))).astype(BF16)

    def put_score(k, x):
        x_s[k] = x
        m_s[k] = jnp.max(x, axis=0, keepdims=True)

    def attend_stages(w_out_t, finish):
        scale = R ** -0.5 * LOG2E

        def score(t):
            for r in range(2):
                q = p_q[t * 2 + r]
                kt = p_kt[t * 2 + r]
                for hp in range(2):
                    blocks = [only(part(q, h, R), h, R, 4) for h in (2 * hp, 2 * hp + 1)]
                    put_score(2 * r + hp, mm(kt, lanes(blocks)) * scale + bt_tri[:, cols(hp, L2)])

        def gather_values(t):
            for r in range(2):
                v = p_v[t * 2 + r]
                outs = []
                for hp in range(2):
                    o2 = mm(part(v, hp, C), w_s[2 * r + hp])
                    outs += [lo(part(o2, 0, R)), hi(part(o2, 1, R))]
                g_s[:, cols(r)] = (subl(outs) * p_sg[t * 2 + r]).astype(BF16)

        def project_out(t):
            finish[0](t, pair(z_t, t * 2).astype(F32) + mm(w_out_t[...], g_s[...]))

        return [score, weigh, gather_values, project_out] + finish[1:]

    def row_attention(b, load, store):
        scale = H ** -0.5 * LOG2E
        for t in range(4):
            proj = round_bf16(mm(w_row_in[b], layer_norm_t(load(t))))
            q, k, v, g = [part(proj, f, C) for f in range(4)]
            p_sg[4 + t, :C] = q
            mkt[t] = jnp.transpose(subl([k, k]))[:, :C].astype(BF16)
            mv[t] = v.astype(BF16)
            p_sg[t, :C] = sigmoid(g)

        def score(t):
            kt = mkt[t]
            kcol = kcols[4 * me + t]
            kcol2 = lanes([kcol, kcol])
            for hp in range(4):
                blocks = [only(p_sg[4 + t, cols(h, H)], h, H, H) for h in (2 * hp, 2 * hp + 1)]
                x = mm(kt, lanes(blocks).astype(BF16)) * scale + bt_row[:, cols(hp, L2)]
                put_score(hp, jnp.where(kcol2 > 0, x, NEG))

        def gather_values(t):
            outs = []
            for hp in range(4):
                o2 = mm(mv[t, cols(hp, S)], w_s[hp])
                outs += [lo(part(o2, 0, H)), hi(part(o2, 1, H))]
            g_s[:C, :L] = (subl(outs) * p_sg[t, :C]).astype(BF16)

        def project_out(t):
            store(t, (load(t).astype(F32) + mm(wro_t[b], g_s[:C, :L])).astype(BF16))

        pipeline([score, weigh, gather_values, project_out], 4)

    same_head = iota((C, L2), 0) // H == iota((C, L2), 1) // R
    block = iota((C, L), 1) // R

    def row_attention_own():
        scale = H ** -0.5 * LOG2E
        rows = subl([bsc_row[pl.ds(h, R, stride=H), :] for h in range(H)])
        bias = jnp.transpose(round_bf16(rows)) * LOG2E
        bt_row[:, :L2] = bias
        w_qg = subl([part(w_row_in[0], 0, C), part(w_row_in[0], 3, C)])

        def keys(t):
            ln2 = lanes([layer_norm_t(m_all[2 * t]), layer_norm_t(m_all[2 * t + 1])])
            kv = round_bf16(mm(w_row_in[0, C:3 * C], ln2))
            for s, x in ((2 * t, lo(kv)), (2 * t + 1, hi(kv))):
                mkt[s] = jnp.transpose(x)[:, :C].astype(BF16)
                mv[s] = part(x, 1, C).astype(BF16)

        def queries(t):
            own = mm(lanes([m_all[4 * t + k] for k in range(4)]), pick[...])
            m_own[t] = own.astype(BF16)
            qg = round_bf16(mm(w_qg, layer_norm_t(own)))
            p_sg[t, :C] = sigmoid(part(qg, 1, C))
            q = mm(part(qg, 0, C).astype(BF16), spread[...])
            for k in range(4):
                mq[4 * t + k] = jnp.where(same_head, q[:, cols(k, L2)], 0.0).astype(BF16)

        def score(t):
            for k in range(4):
                s = 4 * t + k
                x = mm(mkt[s], mq[s]) * scale + bt_row[:, :L2]
                put_score(k, jnp.where(lanes([kcols[s], kcols[s]]) > 0, x, NEG))

        def gather_values(t):
            out = jnp.zeros((C, L), F32)
            for k in range(4):
                o2 = jnp.where(same_head, mm(mv[4 * t + k], w_s[k]), 0.0)
                o = lo(o2) + hi(o2)
                o = o + pltpu.roll(o, C, 1)
                o = o + pltpu.roll(o, R, 1)
                out = jnp.where(block == k, o, out)
            g_s[:C, :L] = (out * p_sg[t, :C]).astype(BF16)

        def project_out(t):
            m_own[t] = (m_own[t].astype(F32) + mm(wro_t[0], g_s[:C, :L])).astype(BF16)

        wait(g_in)
        for t in range(4):
            queries(t)
        for t in range(S // 2):
            keys(t)
        pipeline([score, weigh, gather_values, project_out], 4)

    def attend_columns(steps, mask):
        scale = H ** -0.5 * LOG2E

        def attend(a, carry):
            def at(s, f, d):
                return ckv[s, cols(f * H + d, H)]

            q = [cq[a, cols(d, H)] for d in range(H)]
            logits = []
            for t in range(S):
                acc = functools.reduce(jnp.add, [q[d] * at(t, 0, d) for d in range(H)])
                logits.append(jnp.where(mask[t] > 0, acc * scale, NEG))
            top = functools.reduce(jnp.maximum, logits)
            e = [jnp.exp2(x - top) for x in logits]
            inv = 1.0 / functools.reduce(jnp.add, e)
            probs = [round_bf16(x * inv) for x in e]
            outs = [functools.reduce(jnp.add, [probs[t] * at(t, 1, d) for t in range(S)]) for d in range(H)]
            og[a] = (subl(outs) * part(cq[a], 1, C)).astype(BF16)
            return carry
        lax.fori_loop(0, steps, attend, 0)

    def col_attention_own():
        ln4 = lanes([layer_norm_t(m_own[t]) for t in range(4)])
        proj = round_bf16(mm(wci_p[0], ln4))
        for t in range(4):
            x = proj[:, cols(t)]
            cq[t] = subl([part(x, 0, C), sigmoid(part(x, 3, C))])
            kv = x[C:3 * C].astype(BF16)
            for k in range(4):
                ckv[4 * t + k] = mm(kv, spread[:, cols(2 * k)])
        attend_columns(4, omask)
        new = mm(wco_t[0], lanes([og[t] for t in range(4)]))
        for t in range(4):
            m_dev[me, t] = (m_own[t].astype(F32) + new[:, cols(t)]).astype(BF16)
        both = mm(w_opm_in[0], lanes([layer_norm_t(m_dev[me, t]) for t in range(4)]))
        for t in range(4):
            mask = omask[4 * t, :1]
            for k in range(1, 4):
                mask = jnp.where(block[:1] == k, omask[4 * t + k, :1], mask)
            x = (both[:, cols(t)] * mask).astype(BF16)
            c_dev[me, t] = part(x, 1, R)
            for k in range(4):
                acs[pl.ds((4 * t + k) * C, R), :] = mm(part(x, 0, R), spread[:, cols(2 * k)])

    def col_attention():
        def normalise_m(t):
            for s in (2 * t, 2 * t + 1):
                ln_m[s] = layer_norm_t(m_all[s])

        def project(t):
            proj = round_bf16(mm(wci_p[1], pair(ln_m, 2 * t)))
            put_pair(cq, 2 * t, subl([part(proj, 0, C), sigmoid(part(proj, 3, C))]))
            put_pair(ckv, 2 * t, proj[C:3 * C])
        pipeline([normalise_m, project], S // 2)
        attend_columns(S, cmask)

        def update(t):
            new = pair(m_all, 2 * t).astype(F32) + mm(wco_t[1], pair(og, 2 * t))
            put_pair(m_all, 2 * t, new.astype(BF16))
        return update

    def opm_halves(b, first):
        def normalise_m(t):
            for s in (2 * t, 2 * t + 1):
                ln_m[s] = layer_norm_t(m_all[s])

        def halves(t):
            both = mm(w_opm_in[b], pair(ln_m, 2 * t))
            for s, x in ((2 * t, lo(both)), (2 * t + 1, hi(both))):
                acs[rows_at(s, C), :] = x * msk[pl.ds(s, 1), :].astype(F32)
        pipeline(first + [normalise_m, halves], S // 2)

    row_id = lax.broadcasted_iota(jnp.int32, (S, L2), 0)
    lane_id = lax.broadcasted_iota(jnp.int32, (S, L2), 1)
    diag = row_id == lane_id // S

    def opm(b, finish):
        local, other = (0, R) if b == 0 else (R, 0)
        for q in range(R):
            r_all[q] = acs[pl.ds(other + q, S, stride=C), :].astype(BF16)
        for t in range(4):
            rows = subl([acs[pl.ds(local + H * t + p, S, stride=C), :] for p in range(H)])
            x_loc[:, cols(t)] = jnp.transpose(round_bf16(rows))

        def outer(t):
            left = []
            for k in range(4):
                row = x_loc[pl.ds(b * me * R + t * 4 + k, 1), :]
                for half in (cols(0, L2), cols(1, L2)):
                    left.append(jnp.where(diag, jnp.broadcast_to(row[:, half], (S, L2)), 0.0))
            left = subl(left).astype(BF16)
            for q in range(0, R, 2):
                put_pair(o_scr, q, mm(left, lanes([subl([r_all[q]] * S), subl([r_all[q + 1]] * S)])).astype(BF16))

        def contract(t):
            for k in range(2):
                blocks = [o_scr[:, cols(2 * k + j, R), :].reshape(R * R, L) for j in range(2)]
                n = t * 4 + 2 * k
                at = me * R + n
                norm = lanes([nrm[pl.ds(at, 1), :], nrm[pl.ds(at + 1, 1), :]])
                finish[0](n, mm(woo_t[b], lanes(blocks)) * norm)

        pipeline([outer, contract] + [
            lambda t, f=f: (f(2 * t), f(2 * t + 1)) for f in finish[1:]], R // 4)

    def put_z(t, z2):
        put_pair(z_t, 2 * t, z2.astype(BF16))

    def send_z(stage, b, size):
        def turn(t, z2):
            put_z(t, z2)
            z2 = round_bf16(z2)
            for r, x in ((0, lo(z2)), (1, hi(z2))):
                z_snd[stage, 2 * t + r] = jnp.transpose(x).astype(BF16)

        def send(t):
            for o in range(1, N_DAP):
                z_copy(stage, o, 2 * t, 2, 0, size).start()
            for n in (2 * t, 2 * t + 1):
                z_rcv[stage, me * R + n] = z_snd[stage, n, my_rows, :]
        return [turn, normalise, bias_rows(bsc_tri, ln_t, b, 1), send]

    def widen_z(stage, at, size):
        def widen(t):
            for r in range(4):
                n = t * 4 + r
                z_f[pl.ds(pl.multiple_of(n * (R + H) + at, H), size), :] = z_rcv[stage, n, pl.ds(at, size), :].astype(F32)
        pipeline([widen], R)

    def wait_z(stage, at, size):
        for o in range(1, N_DAP):
            z_copy(stage, o, 0, R, at, size).wait()

    def turn_z(t):
        for n in (2 * t, 2 * t + 1):
            z_t[n] = jnp.transpose(z_f[pl.ds(n, L, stride=R + H), :]).astype(BF16)

    def enter(t):
        for n in (2 * t, 2 * t + 1):
            z_t[n] = jnp.transpose(z_in[n].astype(F32)).astype(BF16)
    pipeline([enter, normalise, bias_rows(bsc_row, ln_t, 0, 0)], R // 2)
    row_attention_own()
    col_attention_own()
    g = gather(7, c_dev.at[me])
    start(g)
    g_m = gather(1, m_dev.at[me])
    start(g_m)
    late_weights()
    wait(g)
    for t in range(4):
        whole = mm(lanes([c_dev[d, t] for d in range(4)]), join[...])
        for k in range(4):
            acs[pl.ds((4 * t + k) * C + R, R), :] = whole[:, cols(k)]

    def add_first(n, update2):
        put_pair(z_t, n, (pair(z_t, n).astype(F32) + update2).astype(BF16))
    opm(0, [add_first, normalise, bias_rows(bsc_tri, ln_t, 0, 1)])
    pack_bias(bsc_tri, tb.at[0], 0, 4)
    g = gather(2, tb.at[0, :, my_rows, :])
    start(g)
    pipeline(project_stages(w_ts_in.at[0]), R // 2)
    wait(g)
    make_tri_bias(tb.at[0], False)
    pipeline(attend_stages(wtri_t.at[0, 0], send_z(0, 0, R)), R // 2)
    pack_bias(bsc_tri, tb.at[1], 4, 4)
    g = gather(3, tb.at[1, :, my_rows, :])
    start(g)

    wait(g_m)
    for t in range(4):
        whole = mm(lanes([m_dev[d, t] for d in range(4)]), join[...]).astype(BF16)
        for k in range(4):
            m_all[4 * t + k] = whole[:, cols(k)]
    opm_halves(1, [col_attention()])

    def keep_update(n, update2):
        put_pair(u_opm, n, update2)
    opm(1, [keep_update])

    wait(g)
    make_tri_bias(tb.at[1], True)
    wait_z(0, 0, R)
    widen_z(0, 0, R)
    pipeline(
        [turn_z, normalise] + project_stages(w_te_in.at[0])
        + attend_stages(wtri_t.at[1, 0], [put_z, normalise, bias_rows(bsc_row, ln_t, 1, 0)]), R // 2)

    pack_bias(bsc_row, rb, 0, H)

    def add_second(t):
        put_z(t, pair(z_t, 2 * t).astype(F32) + pair(u_opm, 2 * t))
    pipeline([add_second, normalise, bias_rows(bsc_tri, ln_t, 1, 1)], R // 2)
    pack_bias(bsc_tri, tb.at[2], 4, 4)
    g = gather(5, tb.at[2, :, my_rows, :])
    start(g)
    g_row = gather(4, rb.at[:, my_rows, :])
    start(g_row)
    pipeline(project_stages(w_te_in.at[1]), R // 2)
    wait(g)
    make_tri_bias(tb.at[2], False)
    pipeline(attend_stages(wtri_t.at[1, 1], send_z(1, 1, FIRST)), R // 2)
    pack_bias(bsc_tri, tb.at[3], 0, 4)
    g = gather(6, tb.at[3, :, my_rows, :])
    start(g)
    for o in range(1, N_DAP):
        z_copy(2, o, 0, R, FIRST, R - FIRST).start()

    wait(g_row)
    for h in range(H):
        bt_row[:, cols(h)] = rb[h].astype(F32) * LOG2E

    def emit_m(s, value):
        m_own[s] = value
    row_attention(1, lambda s: m_all[4 * me + s], emit_m)
    m_done = pltpu.make_async_copy(m_own, m_out, in_sems.at[0])
    m_done.start()

    def last_bias():
        wait(g)
        make_tri_bias(tb.at[3], True)

    def emit_z(t, z2):
        for n, x in ((2 * t, lo(z2)), (2 * t + 1, hi(z2))):
            z_snd[0, n] = jnp.transpose(x).astype(BF16)

    def put_out(n, count):
        return pltpu.make_async_copy(z_snd.at[0, pl.ds(n, count)], z_out.at[pl.ds(n, count)], in_sems.at[1])

    def leave(t):
        put_out(2 * t, 2).start()

    def last_rows():
        wait_z(2, FIRST, R - FIRST)
        widen_z(1, FIRST, R - FIRST)
    wait_z(1, 0, FIRST)
    widen_z(1, 0, FIRST)
    pipeline(
        [turn_z, normalise] + project_stages(w_ts_in.at[1]) + attend_stages(wtri_t.at[0, 1], [emit_z, leave]),
        R // 2, {4: last_bias, FIRST // 2: last_rows})
    m_done.wait()
    put_out(0, R).wait()


def hand_out(m_new, z_new, m_out, z_out, m_v, z_v, sems):
    moves = [(m_new, m_v, m_out)]
    for k in range(4):
        moves.append([ref.at[pl.ds(k * H, H)] for ref in (z_new, z_v, z_out)])
    into = [pltpu.make_async_copy(src, mid, sems.at[0, k]) for k, (src, mid, _) in enumerate(moves)]
    out = [pltpu.make_async_copy(mid, dst, sems.at[1, k]) for k, (_, mid, dst) in enumerate(moves)]
    for c in into:
        c.start()
    for c, d in zip(into, out):
        c.wait()
        d.start()
    for d in out:
        d.wait()


def solution(mesh):
    def local_step(msa_act, pair_act, msa_mask, res_mask, w_row_bias, w_row_in, w_row_out, w_col_in, w_col_out, w_opm_in, w_opm_out, w_ts_bias, w_ts_in, w_ts_out, w_te_bias, w_te_in, w_te_out):
        def rows_first(w):
            w = jnp.moveaxis(w, 1, -1)
            return w.reshape(2, -1, w.shape[-1])

        def flat_out(w):
            return w.reshape(2, -1, w.shape[-1])

        w_bias = [jnp.swapaxes(w, 1, 2) for w in (w_row_bias, w_ts_bias, w_te_bias)]
        hbm = pl.BlockSpec(memory_space=pltpu.HBM)

        def wide(*shape):
            return pltpu.VMEM(shape, F32)

        def half(*shape):
            return pltpu.VMEM(shape, BF16)

        scratch = dict(
            z_t=half(R, L, L), ln_t=half(R, L, L), p_q=half(R, L, L), p_kt=half(R, L, L), p_v=half(R, L, L),
            p_sg=wide(R, L, L), k_s=wide(L, L2), bsc_row=wide(R * H, L), bsc_tri=wide(R * H, L),
            rb=half(H, L, L), tb=half(4, 4, L, L), bt_row=wide(L, H * L), bt_tri=wide(L, 4 * L),
            m_all=half(S, C, L), m_dev=half(4, 4, C, L), c_dev=half(4, 4, R, L), m_own=half(4, C, L), ln_m=half(S, C, L),
            cq=wide(S, L, L), ckv=wide(S, L, L), og=half(S, C, L),
            cmask=wide(S, H, L), omask=wide(S, H, L), kcols=wide(S, L, L),
            mq=half(S, C, L2), mkt=half(S, L, C), mv=half(S, C, L),
            pick=half(4 * L, L), spread=half(L, 8 * L), join=half(4 * L, 4 * L),
            acs=wide(S * C, L), r_all=half(R, S, L), x_loc=wide(L, R * S),
            o_scr=half(R, L, L), u_opm=wide(R, L, L), z_snd=half(2, R, L, L), z_rcv=half(2, L, R, L),
            z_f=wide(L * (R + H), L), nrm=wide(L, L), tmp=wide(R * R, L),
            wro_t=half(2, C, C), wci_p=half(2, 4 * C, C), wco_t=half(2, C, C), woo_t=half(2, L, R * R),
            wtri_t=half(2, 2, L, L), x_s=wide(4, L, L2), m_s=wide(4, 1, L2), w_s=half(4, L, L2), g_s=half(L, L2), w_bias=half(2, S, L),
        )
        sems = [pltpu.SemaphoreType.DMA((n, N_DAP - 1)) for n in (8, 8, 3, 3)]
        operands = (
            jnp.swapaxes(msa_act, 1, 2), pair_act, msa_mask, res_mask.reshape(1, L), *w_bias,
            rows_first(w_row_in), flat_out(w_row_out), rows_first(w_col_in), flat_out(w_col_out),
            rows_first(w_opm_in), flat_out(w_opm_out),
            rows_first(w_ts_in), flat_out(w_ts_out), rows_first(w_te_in), flat_out(w_te_out),
        )
        held = [pltpu.VMEM(x.shape, x.dtype) for x in operands[1:]] + [pltpu.SemaphoreType.DMA((N_IN,))]
        m_new, z_new = pl.pallas_call(
            body,
            out_shape=(jax.ShapeDtypeStruct((4, C, L), BF16), jax.ShapeDtypeStruct((R, L, L), BF16)),
            in_specs=[hbm] * N_IN,
            out_specs=(hbm, hbm),
            scratch_shapes=held + list(scratch.values()) + sems,
            compiler_params=pltpu.CompilerParams(collective_id=0, has_side_effects=True, vmem_limit_bytes=60 * 2 ** 20),
        )(*operands)
        m_new, z_new = pl.pallas_call(
            hand_out, in_specs=[hbm] * 2, out_specs=[hbm] * 2,
            out_shape=[jax.ShapeDtypeStruct(x.shape, x.dtype) for x in (m_new, z_new)],
            scratch_shapes=[half(4, C, L), half(R, L, L), pltpu.SemaphoreType.DMA((2, 5))],
        )(m_new, z_new)
        return jnp.swapaxes(m_new, 1, 2), z_new

    in_specs = (P(('data', 'dap')), P(('data', 'dap')), P('data'), P('data')) + (P(),) * 13
    out_specs = (P(('data', 'dap')), P(('data', 'dap')))
    return jax.shard_map(local_step, mesh=mesh, in_specs=in_specs, out_specs=out_specs, check_vma=False)
```

```python
import functools

import jax
import jax.numpy as jnp
from jax import lax
from jax.experimental import pallas as pl
from jax.experimental.pallas import tpu as pltpu
from jax.sharding import PartitionSpec as P

F32 = jnp.float32
BF16 = jnp.bfloat16
LOG2E = 1.4426950408889634
NEG = -1e9 * LOG2E
N_DAP = 4
N_IN = 17
L = 128
R = 32
S = 16
C = 64
H = 8
L2 = 2 * L
FIRST = 24
MESH = pl.DeviceIdType.MESH


def mm(lhs, rhs):
    return jnp.dot(lhs, rhs, preferred_element_type=F32)


def mm_nt(lhs, rhs):
    return lax.dot_general(lhs, rhs, (((1,), (1,)), ((), ())), preferred_element_type=F32)


def lanes(parts):
    return jnp.concatenate(parts, axis=1)


def subl(parts):
    return jnp.concatenate(parts, axis=0)


def lo(x):
    return x[:, :L]


def hi(x):
    return x[:, L:]


def part(x, k, size):
    return x[k * size:(k + 1) * size]


def cols(k, size=L):
    return slice(k * size, (k + 1) * size)


def rows_at(n, size):
    return pl.ds(pl.multiple_of(n * size, size), size)


def pair(ref, n):
    return lanes([ref[n], ref[n + 1]])


def put_pair(ref, n, value):
    ref[n] = lo(value)
    ref[n + 1] = hi(value)


def only(value, k, size, count):
    zero = jnp.zeros((size, value.shape[1]), value.dtype)
    return subl([value if j == k else zero for j in range(count)])


def eye_bf16(n):
    rows = lax.broadcasted_iota(jnp.int32, (n, n), 0)
    columns = lax.broadcasted_iota(jnp.int32, (n, n), 1)
    return jnp.where(rows == columns, 1.0, 0.0).astype(BF16)


def layer_norm_t(x):
    x = x.astype(F32)
    inv_n = 1.0 / x.shape[0]
    centered = x - jnp.sum(x, axis=0, keepdims=True) * inv_n
    var = jnp.sum(centered * centered, axis=0, keepdims=True) * inv_n
    return (centered * lax.rsqrt(var + 1e-5)).astype(BF16)


def sigmoid(x):
    return 0.5 * jnp.tanh(0.5 * x) + 0.5


def round_bf16(x):
    return x.astype(BF16).astype(F32)


def pipeline(stages, trips, hooks=None):
    depth = len(stages)
    hooks = hooks or {}

    def run(t, first, last):
        for k in reversed(range(first, last)):
            stages[k](t - k)

    def step(t, carry):
        run(t, 0, depth)
        return carry

    begin = depth - 1
    for t in range(begin):
        if t in hooks:
            hooks[t]()
        run(t, 0, t + 1)
    for t in sorted(t for t in hooks if t >= begin):
        lax.fori_loop(begin, t, step, 0)
        hooks[t]()
        begin = t
    lax.fori_loop(begin, trips, step, 0)
    for t in range(depth - 1):
        run(trips + t, t + 1, depth)


def body(
    m_hbm, *refs,
):
    n = N_IN - 1
    given, (m_out, z_out), refs = refs[:n], refs[n:n + 2], refs[n + 2:]
    held, in_sems, refs = refs[:n], refs[n], refs[n + 1:]
    main(m_hbm, given, held, in_sems, m_out, z_out, *refs)


def main(
    m_hbm, given, held, in_sems, m_out, z_out,
    z_t, ln_t, p_q, p_kt, p_v, p_sg, k_s, bsc_row, bsc_tri, rb, tb, bt_row, bt_tri, m_all, m_dev, c_dev, m_own, ln_m, cq, ckv, og,
    cmask, omask, kcols, mq, mkt, mv, pick, spread, join, acs, r_all, x_loc, o_scr, u_opm, z_snd, z_rcv, z_f, nrm, tmp, wro_t, wci_p, wco_t, woo_t, wtri_t,
    x_s, m_s, w_s, g_s, w_bias,
    g_send, g_recv, a_send, a_recv,
):
    me = lax.axis_index('dap')
    data = lax.axis_index('data')
    my_rows = rows_at(me, R)

    def peer(o):
        return (data, lax.rem(me + o, N_DAP))

    z_in, msk, rmsk, w_row_bias, w_ts_bias, w_te_bias = held[:6]
    w_row_in, w_row_out, w_col_in, w_col_out, w_opm_in, w_opm_out, w_ts_in, w_ts_out, w_te_in, w_te_out = held[6:]
    own_m = m_all.at[pl.ds(4 * me, 4)]
    copy_m = pltpu.make_async_copy(m_hbm, own_m, in_sems.at[N_IN - 1])
    copy_m.start()
    copies_in = [pltpu.make_async_copy(src, dst, in_sems.at[k]) for k, (src, dst) in enumerate(zip(given, held))]
    for c in copies_in:
        c.start()

    barrier = pltpu.get_barrier_semaphore()
    for o in range(1, N_DAP):
        pl.semaphore_signal(barrier, inc=1, device_id=peer(o), device_id_type=MESH)
    pl.semaphore_wait(barrier, N_DAP - 1)

    def gather(stage, ref):
        return [
            pltpu.make_async_remote_copy(
                src_ref=ref, dst_ref=ref, send_sem=g_send.at[stage, o - 1], recv_sem=g_recv.at[stage, o - 1],
                device_id=peer(o), device_id_type=MESH)
            for o in range(1, N_DAP)
        ]

    def start(copies):
        for c in copies:
            c.start()

    def wait(copies):
        for c in copies:
            c.wait()

    def z_copy(stage, o, first, count, at=0, size=R):
        dest = lax.rem(me + o, N_DAP)
        return pltpu.make_async_remote_copy(
            src_ref=z_snd.at[min(stage, 1), pl.ds(first, count), pl.ds(pl.multiple_of(dest * R + at, H), size), :],
            dst_ref=z_rcv.at[min(stage, 1), pl.ds(me * R + first, count), pl.ds(at, size), :],
            send_sem=a_send.at[stage, o - 1], recv_sem=a_recv.at[stage, o - 1],
            device_id=(data, dest), device_id_type=MESH)

    copy_m.wait()
    g_in = gather(0, own_m)
    start(g_in)
    for c in copies_in:
        c.wait()

    e_c = eye_bf16(C)
    e_l = eye_bf16(L)

    def every(first, count, stride):
        return tmp[pl.ds(first, count, stride=stride), :]

    for b in range(2):
        tmp[:H, :] = w_row_bias[b].astype(F32)
        tmp[H:H + 4, :] = w_ts_bias[b].astype(F32)
        tmp[H + 4:S, :] = w_te_bias[b].astype(F32)
        w_bias[b] = tmp[:S, :].astype(BF16)
        wro_t[b] = mm_nt(e_c, w_row_out[b]).astype(BF16)
        tmp[:4 * C, :C] = w_col_in[b].astype(F32)
        wci_p[b] = subl([every(f * C + d, H, H) for f in range(4) for d in range(H)])[:, :C].astype(BF16)
        tmp[:C, :C] = w_col_out[b].astype(F32)
        wco_t[b] = mm_nt(e_c, subl([every(d, H, H) for d in range(H)])[:, :C].astype(BF16)).astype(BF16)

    def late_weights():
        for b in range(2):
            wtri_t[0, b] = mm_nt(e_l, w_ts_out[b]).astype(BF16)
            wtri_t[1, b] = mm_nt(e_l, w_te_out[b]).astype(BF16)
        tmp[...] = w_opm_out[0].astype(F32)
        woo_t[0] = mm_nt(e_l, subl([every(q, R, R) for q in range(R)]).astype(BF16)).astype(BF16)
        woo_t[1] = mm_nt(e_l, w_opm_out[1]).astype(BF16)
        src, lane = iota((4 * L, 4 * L), 0), iota((4 * L, 4 * L), 1)
        join[...] = ones_at((src // L == lane % L // R) & (src % L == lane // L * R + lane % R))

    def down(row):
        return jnp.transpose(jnp.broadcast_to(row, (L, L)))

    mask_f = msk[...].astype(F32)
    for s in range(S):
        cmask[s] = jnp.broadcast_to(mask_f[s:s + 1, :], (H, L))
    mask_t = jnp.transpose(subl([mask_f] * H)).astype(BF16)[:, :S]
    nrm[...] = 1.0 / (1e-3 + mm(mask_t, mask_f.astype(BF16)))
    key_row = rmsk[...].astype(F32)
    key_col = down(key_row)
    key_row2 = lanes([key_row, key_row])
    turned = jnp.transpose(subl([mask_f] * H))
    for s in range(S):
        kcols[s] = jnp.broadcast_to(turned[:, s:s + 1], (L, L))

    def iota(shape, axis):
        return lax.broadcasted_iota(jnp.int32, shape, axis)

    def ones_at(where):
        return jnp.where(where, 1.0, 0.0).astype(BF16)

    src, lane = iota((4 * L, L), 0), iota((4 * L, L), 1)
    pick[...] = ones_at((src // L == lane // R) & (src % L == me * R + lane % R))
    src, lane = iota((L, 8 * L), 0), iota((L, 8 * L), 1)
    spread[...] = ones_at(src == lane // L2 * R + lane % R)
    src, lane = iota((L, L), 0), iota((L, L), 1)
    own_mask = mm(mask_f.astype(BF16), ones_at(src == me * R + lane % R))
    for s in range(S):
        omask[s] = jnp.broadcast_to(own_mask[s:s + 1, :], (H, L))

    def bias_rows(bsc, ln_ref, b, group):
        def stage(t):
            n = t * 2
            rows = part(mm(w_bias[b], pair(ln_ref, n)), group, H)
            bsc[rows_at(n, H), :] = lo(rows)
            bsc[rows_at(n + 1, H), :] = hi(rows)
        return stage

    def pack_bias(bsc, ref, first, heads):
        for h in range(heads):
            ref[h, my_rows, :] = bsc[pl.ds(first + h, R, stride=H), :].astype(BF16)

    def normalise(t):
        for n in (t * 2, t * 2 + 1):
            ln_t[n] = layer_norm_t(z_t[n])

    def make_tri_bias(ref, by_key):
        for h in range(4):
            t = ref[h].astype(F32) * LOG2E
            t = t if by_key else jnp.transpose(t)
            bt_tri[:, cols(h)] = jnp.where(key_col > 0, t, NEG)

    def project_stages(w_in_ref):
        def project(t):
            n = t * 2
            ln2 = pair(ln_t, n)
            put_pair(p_q, n, mm(part(w_in_ref, 0, L), ln2).astype(BF16))
            k_s[...] = round_bf16(mm(part(w_in_ref, 1, L), ln2)) * key_row2
            put_pair(p_v, n, mm(part(w_in_ref, 2, L), ln2).astype(BF16))
            put_pair(p_sg, n, round_bf16(mm(part(w_in_ref, 3, L), ln2)))

        def turn(t):
            for r in range(2):
                p_kt[t * 2 + r] = jnp.transpose(k_s[:, cols(r)]).astype(BF16)
                p_sg[t * 2 + r] = sigmoid(p_sg[t * 2 + r])

        return [project, turn]

    def weigh(t):
        for k in range(4):
            for half in (cols(0), cols(1)):
                e = jnp.exp2(x_s[k, :, half] - m_s[k, :, half])
                w_s[k, :, half] = (e * (1.0 / jnp.sum(e, axis=0, keepdims=True))).astype(BF16)

    def put_score(k, x):
        x_s[k] = x
        m_s[k] = jnp.max(x, axis=0, keepdims=True)

    def attend_stages(w_out_t, finish):
        scale = R ** -0.5 * LOG2E

        def score(t):
            for r in range(2):
                q = p_q[t * 2 + r]
                kt = p_kt[t * 2 + r]
                for hp in range(2):
                    blocks = [only(part(q, h, R), h, R, 4) for h in (2 * hp, 2 * hp + 1)]
                    put_score(2 * r + hp, mm(kt, lanes(blocks)) * scale + bt_tri[:, cols(hp, L2)])

        def gather_values(t):
            for r in range(2):
                v = p_v[t * 2 + r]
                outs = []
                for hp in range(2):
                    o2 = mm(part(v, hp, C), w_s[2 * r + hp])
                    outs += [lo(part(o2, 0, R)), hi(part(o2, 1, R))]
                g_s[:, cols(r)] = (subl(outs) * p_sg[t * 2 + r]).astype(BF16)

        def project_out(t):
            finish[0](t, pair(z_t, t * 2).astype(F32) + mm(w_out_t[...], g_s[...]))

        return [score, weigh, gather_values, project_out] + finish[1:]

    def row_attention(b, load, store):
        scale = H ** -0.5 * LOG2E
        for t in range(4):
            proj = round_bf16(mm(w_row_in[b], layer_norm_t(load(t))))
            q, k, v, g = [part(proj, f, C) for f in range(4)]
            p_sg[4 + t, :C] = q
            mkt[t] = jnp.transpose(subl([k, k]))[:, :C].astype(BF16)
            mv[t] = v.astype(BF16)
            p_sg[t, :C] = sigmoid(g)

        def score(t):
            kt = mkt[t]
            kcol = kcols[4 * me + t]
            kcol2 = lanes([kcol, kcol])
            for hp in range(4):
                blocks = [only(p_sg[4 + t, cols(h, H)], h, H, H) for h in (2 * hp, 2 * hp + 1)]
                x = mm(kt, lanes(blocks).astype(BF16)) * scale + bt_row[:, cols(hp, L2)]
                put_score(hp, jnp.where(kcol2 > 0, x, NEG))

        def gather_values(t):
            outs = []
            for hp in range(4):
                o2 = mm(mv[t, cols(hp, S)], w_s[hp])
                outs += [lo(part(o2, 0, H)), hi(part(o2, 1, H))]
            g_s[:C, :L] = (subl(outs) * p_sg[t, :C]).astype(BF16)

        def project_out(t):
            store(t, (load(t).astype(F32) + mm(wro_t[b], g_s[:C, :L])).astype(BF16))

        pipeline([score, weigh, gather_values, project_out], 4)

    same_head = iota((C, L2), 0) // H == iota((C, L2), 1) // R
    block = iota((C, L), 1) // R

    def row_attention_own():
        scale = H ** -0.5 * LOG2E
        rows = subl([bsc_row[pl.ds(h, R, stride=H), :] for h in range(H)])
        bias = jnp.transpose(round_bf16(rows)) * LOG2E
        bt_row[:, :L2] = bias
        w_qg = subl([part(w_row_in[0], 0, C), part(w_row_in[0], 3, C)])

        def keys(t):
            ln2 = lanes([layer_norm_t(m_all[2 * t]), layer_norm_t(m_all[2 * t + 1])])
            kv = round_bf16(mm(w_row_in[0, C:3 * C], ln2))
            for s, x in ((2 * t, lo(kv)), (2 * t + 1, hi(kv))):
                mkt[s] = jnp.transpose(x)[:, :C].astype(BF16)
                mv[s] = part(x, 1, C).astype(BF16)

        def queries(t):
            own = mm(lanes([m_all[4 * t + k] for k in range(4)]), pick[...])
            m_own[t] = own.astype(BF16)
            qg = round_bf16(mm(w_qg, layer_norm_t(own)))
            p_sg[t, :C] = sigmoid(part(qg, 1, C))
            q = mm(part(qg, 0, C).astype(BF16), spread[...])
            for k in range(4):
                mq[4 * t + k] = jnp.where(same_head, q[:, cols(k, L2)], 0.0).astype(BF16)

        def score(t):
            for k in range(4):
                s = 4 * t + k
                x = mm(mkt[s], mq[s]) * scale + bt_row[:, :L2]
                put_score(k, jnp.where(lanes([kcols[s], kcols[s]]) > 0, x, NEG))

        def gather_values(t):
            out = jnp.zeros((C, L), F32)
            for k in range(4):
                o2 = jnp.where(same_head, mm(mv[4 * t + k], w_s[k]), 0.0)
                o = lo(o2) + hi(o2)
                o = o + pltpu.roll(o, C, 1)
                o = o + pltpu.roll(o, R, 1)
                out = jnp.where(block == k, o, out)
            g_s[:C, :L] = (out * p_sg[t, :C]).astype(BF16)

        def project_out(t):
            m_own[t] = (m_own[t].astype(F32) + mm(wro_t[0], g_s[:C, :L])).astype(BF16)

        wait(g_in)
        for t in range(4):
            queries(t)
        for t in range(S // 2):
            keys(t)
        pipeline([score, weigh, gather_values, project_out], 4)

    def attend_columns(steps, mask):
        scale = H ** -0.5 * LOG2E

        def attend(a, carry):
            def at(s, f, d):
                return ckv[s, cols(f * H + d, H)]

            q = [cq[a, cols(d, H)] for d in range(H)]
            logits = []
            for t in range(S):
                acc = functools.reduce(jnp.add, [q[d] * at(t, 0, d) for d in range(H)])
                logits.append(jnp.where(mask[t] > 0, acc * scale, NEG))
            top = functools.reduce(jnp.maximum, logits)
            e = [jnp.exp2(x - top) for x in logits]
            inv = 1.0 / functools.reduce(jnp.add, e)
            probs = [round_bf16(x * inv) for x in e]
            outs = [functools.reduce(jnp.add, [probs[t] * at(t, 1, d) for t in range(S)]) for d in range(H)]
            og[a] = (subl(outs) * part(cq[a], 1, C)).astype(BF16)
            return carry
        lax.fori_loop(0, steps, attend, 0)

    def col_attention_own():
        ln4 = lanes([layer_norm_t(m_own[t]) for t in range(4)])
        proj = round_bf16(mm(wci_p[0], ln4))
        for t in range(4):
            x = proj[:, cols(t)]
            cq[t] = subl([part(x, 0, C), sigmoid(part(x, 3, C))])
            kv = x[C:3 * C].astype(BF16)
            for k in range(4):
                ckv[4 * t + k] = mm(kv, spread[:, cols(2 * k)])
        attend_columns(4, omask)
        new = mm(wco_t[0], lanes([og[t] for t in range(4)]))
        for t in range(4):
            m_dev[me, t] = (m_own[t].astype(F32) + new[:, cols(t)]).astype(BF16)
        both = mm(w_opm_in[0], lanes([layer_norm_t(m_dev[me, t]) for t in range(4)]))
        for t in range(4):
            mask = omask[4 * t, :1]
            for k in range(1, 4):
                mask = jnp.where(block[:1] == k, omask[4 * t + k, :1], mask)
            x = (both[:, cols(t)] * mask).astype(BF16)
            c_dev[me, t] = part(x, 1, R)
            for k in range(4):
                acs[pl.ds((4 * t + k) * C, R), :] = mm(part(x, 0, R), spread[:, cols(2 * k)])

    def col_attention():
        def normalise_m(t):
            for s in (2 * t, 2 * t + 1):
                ln_m[s] = layer_norm_t(m_all[s])

        def project(t):
            proj = round_bf16(mm(wci_p[1], pair(ln_m, 2 * t)))
            put_pair(cq, 2 * t, subl([part(proj, 0, C), sigmoid(part(proj, 3, C))]))
            put_pair(ckv, 2 * t, proj[C:3 * C])
        pipeline([normalise_m, project], S // 2)
        attend_columns(S, cmask)

        def update(t):
            new = pair(m_all, 2 * t).astype(F32) + mm(wco_t[1], pair(og, 2 * t))
            put_pair(m_all, 2 * t, new.astype(BF16))
        return update

    def opm_halves(b, first):
        def normalise_m(t):
            for s in (2 * t, 2 * t + 1):
                ln_m[s] = layer_norm_t(m_all[s])

        def halves(t):
            both = mm(w_opm_in[b], pair(ln_m, 2 * t))
            for s, x in ((2 * t, lo(both)), (2 * t + 1, hi(both))):
                acs[rows_at(s, C), :] = x * msk[pl.ds(s, 1), :].astype(F32)
        pipeline(first + [normalise_m, halves], S // 2)

    row_id = lax.broadcasted_iota(jnp.int32, (S, L2), 0)
    lane_id = lax.broadcasted_iota(jnp.int32, (S, L2), 1)
    diag = row_id == lane_id // S

    def opm(b, finish):
        local, other = (0, R) if b == 0 else (R, 0)
        for q in range(R):
            r_all[q] = acs[pl.ds(other + q, S, stride=C), :].astype(BF16)
        for t in range(4):
            rows = subl([acs[pl.ds(local + H * t + p, S, stride=C), :] for p in range(H)])
            x_loc[:, cols(t)] = jnp.transpose(round_bf16(rows))

        def outer(t):
            left = []
            for k in range(4):
                row = x_loc[pl.ds(b * me * R + t * 4 + k, 1), :]
                for half in (cols(0, L2), cols(1, L2)):
                    left.append(jnp.where(diag, jnp.broadcast_to(row[:, half], (S, L2)), 0.0))
            left = subl(left).astype(BF16)
            for q in range(0, R, 2):
                put_pair(o_scr, q, mm(left, lanes([subl([r_all[q]] * S), subl([r_all[q + 1]] * S)])).astype(BF16))

        def contract(t):
            for k in range(2):
                blocks = [o_scr[:, cols(2 * k + j, R), :].reshape(R * R, L) for j in range(2)]
                n = t * 4 + 2 * k
                at = me * R + n
                norm = lanes([nrm[pl.ds(at, 1), :], nrm[pl.ds(at + 1, 1), :]])
                finish[0](n, mm(woo_t[b], lanes(blocks)) * norm)

        pipeline([outer, contract] + [
            lambda t, f=f: (f(2 * t), f(2 * t + 1)) for f in finish[1:]], R // 4)

    def put_z(t, z2):
        put_pair(z_t, 2 * t, z2.astype(BF16))

    def send_z(stage, b, size):
        def turn(t, z2):
            put_z(t, z2)
            z2 = round_bf16(z2)
            for r, x in ((0, lo(z2)), (1, hi(z2))):
                z_snd[stage, 2 * t + r] = jnp.transpose(x).astype(BF16)

        def send(t):
            for o in range(1, N_DAP):
                z_copy(stage, o, 2 * t, 2, 0, size).start()
            for n in (2 * t, 2 * t + 1):
                z_rcv[stage, me * R + n] = z_snd[stage, n, my_rows, :]
        return [turn, normalise, bias_rows(bsc_tri, ln_t, b, 1), send]

    def widen_z(stage, at, size):
        def widen(t):
            for r in range(4):
                n = t * 4 + r
                z_f[pl.ds(pl.multiple_of(n * (R + H) + at, H), size), :] = z_rcv[stage, n, pl.ds(at, size), :].astype(F32)
        pipeline([widen], R)

    def wait_z(stage, at, size):
        for o in range(1, N_DAP):
            z_copy(stage, o, 0, R, at, size).wait()

    def turn_z(t):
        for n in (2 * t, 2 * t + 1):
            z_t[n] = jnp.transpose(z_f[pl.ds(n, L, stride=R + H), :]).astype(BF16)

    def enter(t):
        for n in (2 * t, 2 * t + 1):
            z_t[n] = jnp.transpose(z_in[n].astype(F32)).astype(BF16)
    pipeline([enter, normalise, bias_rows(bsc_row, ln_t, 0, 0)], R // 2)
    row_attention_own()
    col_attention_own()
    g = gather(7, c_dev.at[me])
    start(g)
    g_m = gather(1, m_dev.at[me])
    start(g_m)
    late_weights()
    wait(g)
    for t in range(4):
        whole = mm(lanes([c_dev[d, t] for d in range(4)]), join[...])
        for k in range(4):
            acs[pl.ds((4 * t + k) * C + R, R), :] = whole[:, cols(k)]

    def add_first(n, update2):
        put_pair(z_t, n, (pair(z_t, n).astype(F32) + update2).astype(BF16))
    opm(0, [add_first, normalise, bias_rows(bsc_tri, ln_t, 0, 1)])
    pack_bias(bsc_tri, tb.at[0], 0, 4)
    g = gather(2, tb.at[0, :, my_rows, :])
    start(g)
    pipeline(project_stages(w_ts_in.at[0]), R // 2)
    wait(g)
    make_tri_bias(tb.at[0], False)
    pipeline(attend_stages(wtri_t.at[0, 0], send_z(0, 0, R)), R // 2)
    pack_bias(bsc_tri, tb.at[1], 4, 4)
    g = gather(3, tb.at[1, :, my_rows, :])
    start(g)

    wait(g_m)
    for t in range(4):
        whole = mm(lanes([m_dev[d, t] for d in range(4)]), join[...]).astype(BF16)
        for k in range(4):
            m_all[4 * t + k] = whole[:, cols(k)]
    opm_halves(1, [col_attention()])

    def keep_update(n, update2):
        put_pair(u_opm, n, update2)
    opm(1, [keep_update])

    def add_second(t):
        put_z(t, pair(z_t, 2 * t).astype(F32) + pair(u_opm, 2 * t))

    wait(g)
    make_tri_bias(tb.at[1], True)
    wait_z(0, 0, R)
    widen_z(0, 0, R)
    pipeline(
        [turn_z, normalise] + project_stages(w_te_in.at[0])
        + attend_stages(wtri_t.at[1, 0], [
            put_z, normalise, bias_rows(bsc_row, ln_t, 1, 0), add_second, normalise, bias_rows(bsc_tri, ln_t, 1, 1)]),
        R // 2)

    pack_bias(bsc_row, rb, 0, H)

    pack_bias(bsc_tri, tb.at[2], 4, 4)
    g = gather(5, tb.at[2, :, my_rows, :])
    start(g)
    g_row = gather(4, rb.at[:, my_rows, :])
    start(g_row)
    pipeline(project_stages(w_te_in.at[1]), R // 2)
    wait(g)
    make_tri_bias(tb.at[2], False)
    pipeline(attend_stages(wtri_t.at[1, 1], send_z(1, 1, FIRST)), R // 2)
    pack_bias(bsc_tri, tb.at[3], 0, 4)
    g = gather(6, tb.at[3, :, my_rows, :])
    start(g)
    for o in range(1, N_DAP):
        z_copy(2, o, 0, R, FIRST, R - FIRST).start()

    wait(g_row)
    for h in range(H):
        bt_row[:, cols(h)] = rb[h].astype(F32) * LOG2E

    def emit_m(s, value):
        m_own[s] = value
    row_attention(1, lambda s: m_all[4 * me + s], emit_m)
    m_done = pltpu.make_async_copy(m_own, m_out, in_sems.at[0])
    m_done.start()

    def last_bias():
        wait(g)
        make_tri_bias(tb.at[3], True)

    def emit_z(t, z2):
        for n, x in ((2 * t, lo(z2)), (2 * t + 1, hi(z2))):
            z_snd[0, n] = jnp.transpose(x).astype(BF16)

    def put_out(n, count):
        return pltpu.make_async_copy(z_snd.at[0, pl.ds(n, count)], z_out.at[pl.ds(n, count)], in_sems.at[1])

    def leave(t):
        put_out(2 * t, 2).start()

    def last_rows():
        wait_z(2, FIRST, R - FIRST)
        widen_z(1, FIRST, R - FIRST)
    wait_z(1, 0, FIRST)
    widen_z(1, 0, FIRST)
    pipeline(
        [turn_z, normalise] + project_stages(w_ts_in.at[1]) + attend_stages(wtri_t.at[0, 1], [emit_z, leave]),
        R // 2, {4: last_bias, FIRST // 2: last_rows})
    m_done.wait()
    put_out(0, R).wait()


def hand_out(m_new, z_new, m_out, z_out, m_v, z_v, sems):
    moves = [(m_new, m_v, m_out)]
    for k in range(4):
        moves.append([ref.at[pl.ds(k * H, H)] for ref in (z_new, z_v, z_out)])
    into = [pltpu.make_async_copy(src, mid, sems.at[0, k]) for k, (src, mid, _) in enumerate(moves)]
    out = [pltpu.make_async_copy(mid, dst, sems.at[1, k]) for k, (_, mid, dst) in enumerate(moves)]
    for c in into:
        c.start()
    for c, d in zip(into, out):
        c.wait()
        d.start()
    for d in out:
        d.wait()


def solution(mesh):
    def local_step(msa_act, pair_act, msa_mask, res_mask, w_row_bias, w_row_in, w_row_out, w_col_in, w_col_out, w_opm_in, w_opm_out, w_ts_bias, w_ts_in, w_ts_out, w_te_bias, w_te_in, w_te_out):
        def rows_first(w):
            w = jnp.moveaxis(w, 1, -1)
            return w.reshape(2, -1, w.shape[-1])

        def flat_out(w):
            return w.reshape(2, -1, w.shape[-1])

        w_bias = [jnp.swapaxes(w, 1, 2) for w in (w_row_bias, w_ts_bias, w_te_bias)]
        hbm = pl.BlockSpec(memory_space=pltpu.HBM)

        def wide(*shape):
            return pltpu.VMEM(shape, F32)

        def half(*shape):
            return pltpu.VMEM(shape, BF16)

        scratch = dict(
            z_t=half(R, L, L), ln_t=half(R, L, L), p_q=half(R, L, L), p_kt=half(R, L, L), p_v=half(R, L, L),
            p_sg=wide(R, L, L), k_s=wide(L, L2), bsc_row=wide(R * H, L), bsc_tri=wide(R * H, L),
            rb=half(H, L, L), tb=half(4, 4, L, L), bt_row=wide(L, H * L), bt_tri=wide(L, 4 * L),
            m_all=half(S, C, L), m_dev=half(4, 4, C, L), c_dev=half(4, 4, R, L), m_own=half(4, C, L), ln_m=half(S, C, L),
            cq=wide(S, L, L), ckv=wide(S, L, L), og=half(S, C, L),
            cmask=wide(S, H, L), omask=wide(S, H, L), kcols=wide(S, L, L),
            mq=half(S, C, L2), mkt=half(S, L, C), mv=half(S, C, L),
            pick=half(4 * L, L), spread=half(L, 8 * L), join=half(4 * L, 4 * L),
            acs=wide(S * C, L), r_all=half(R, S, L), x_loc=wide(L, R * S),
            o_scr=half(R, L, L), u_opm=wide(R, L, L), z_snd=half(2, R, L, L), z_rcv=half(2, L, R, L),
            z_f=wide(L * (R + H), L), nrm=wide(L, L), tmp=wide(R * R, L),
            wro_t=half(2, C, C), wci_p=half(2, 4 * C, C), wco_t=half(2, C, C), woo_t=half(2, L, R * R),
            wtri_t=half(2, 2, L, L), x_s=wide(4, L, L2), m_s=wide(4, 1, L2), w_s=half(4, L, L2), g_s=half(L, L2), w_bias=half(2, S, L),
        )
        sems = [pltpu.SemaphoreType.DMA((n, N_DAP - 1)) for n in (8, 8, 3, 3)]
        operands = (
            jnp.swapaxes(msa_act, 1, 2), pair_act, msa_mask, res_mask.reshape(1, L), *w_bias,
            rows_first(w_row_in), flat_out(w_row_out), rows_first(w_col_in), flat_out(w_col_out),
            rows_first(w_opm_in), flat_out(w_opm_out),
            rows_first(w_ts_in), flat_out(w_ts_out), rows_first(w_te_in), flat_out(w_te_out),
        )
        held = [pltpu.VMEM(x.shape, x.dtype) for x in operands[1:]] + [pltpu.SemaphoreType.DMA((N_IN,))]
        m_new, z_new = pl.pallas_call(
            body,
            out_shape=(jax.ShapeDtypeStruct((4, C, L), BF16), jax.ShapeDtypeStruct((R, L, L), BF16)),
            in_specs=[hbm] * N_IN,
            out_specs=(hbm, hbm),
            scratch_shapes=held + list(scratch.values()) + sems,
            compiler_params=pltpu.CompilerParams(collective_id=0, has_side_effects=True, vmem_limit_bytes=60 * 2 ** 20),
        )(*operands)
        m_new, z_new = pl.pallas_call(
            hand_out, in_specs=[hbm] * 2, out_specs=[hbm] * 2,
            out_shape=[jax.ShapeDtypeStruct(x.shape, x.dtype) for x in (m_new, z_new)],
            scratch_shapes=[half(4, C, L), half(R, L, L), pltpu.SemaphoreType.DMA((2, 5))],
        )(m_new, z_new)
        return jnp.swapaxes(m_new, 1, 2), z_new

    in_specs = (P(('data', 'dap')), P(('data', 'dap')), P('data'), P('data')) + (P(),) * 13
    out_specs = (P(('data', 'dap')), P(('data', 'dap')))
    return jax.shard_map(local_step, mesh=mesh, in_specs=in_specs, out_specs=out_specs, check_vma=False)
```

```python
import functools

import jax
import jax.numpy as jnp
from jax import lax
from jax.experimental import pallas as pl
from jax.experimental.pallas import tpu as pltpu
from jax.sharding import PartitionSpec as P

F32 = jnp.float32
BF16 = jnp.bfloat16
LOG2E = 1.4426950408889634
NEG = -1e9 * LOG2E
N_DAP = 4
N_IN = 17
L = 128
R = 32
S = 16
C = 64
H = 8
L2 = 2 * L
FIRST = 24
MESH = pl.DeviceIdType.MESH


def mm(lhs, rhs):
    return jnp.dot(lhs, rhs, preferred_element_type=F32)


def mm_nt(lhs, rhs):
    return lax.dot_general(lhs, rhs, (((1,), (1,)), ((), ())), preferred_element_type=F32)


def lanes(parts):
    return jnp.concatenate(parts, axis=1)


def subl(parts):
    return jnp.concatenate(parts, axis=0)


def lo(x):
    return x[:, :L]


def hi(x):
    return x[:, L:]


def part(x, k, size):
    return x[k * size:(k + 1) * size]


def cols(k, size=L):
    return slice(k * size, (k + 1) * size)


def rows_at(n, size):
    return pl.ds(pl.multiple_of(n * size, size), size)


def pair(ref, n):
    return lanes([ref[n], ref[n + 1]])


def put_pair(ref, n, value):
    ref[n] = lo(value)
    ref[n + 1] = hi(value)


def only(value, k, size, count):
    zero = jnp.zeros((size, value.shape[1]), value.dtype)
    return subl([value if j == k else zero for j in range(count)])


def eye_bf16(n):
    rows = lax.broadcasted_iota(jnp.int32, (n, n), 0)
    columns = lax.broadcasted_iota(jnp.int32, (n, n), 1)
    return jnp.where(rows == columns, 1.0, 0.0).astype(BF16)


def layer_norm_t(x):
    x = x.astype(F32)
    inv_n = 1.0 / x.shape[0]
    centered = x - jnp.sum(x, axis=0, keepdims=True) * inv_n
    var = jnp.sum(centered * centered, axis=0, keepdims=True) * inv_n
    return (centered * lax.rsqrt(var + 1e-5)).astype(BF16)


def sigmoid(x):
    return 0.5 * jnp.tanh(0.5 * x) + 0.5


def round_bf16(x):
    return x.astype(BF16).astype(F32)


def pipeline(stages, trips, hooks=None):
    depth = len(stages)
    hooks = hooks or {}

    def run(t, first, last):
        for k in sorted(range(first, last), key=lambda k: (not hasattr(stages[k], 'early'), -k)):
            stages[k](t - k)

    def step(t, carry):
        run(t, 0, depth)
        return carry

    begin = depth - 1
    for t in range(begin):
        if t in hooks:
            hooks[t]()
        run(t, 0, t + 1)
    for t in sorted(t for t in hooks if t >= begin):
        lax.fori_loop(begin, t, step, 0)
        hooks[t]()
        begin = t
    lax.fori_loop(begin, trips, step, 0)
    for t in range(depth - 1):
        run(trips + t, t + 1, depth)


def body(
    m_hbm, *refs,
):
    n = N_IN - 1
    given, (m_out, z_out), refs = refs[:n], refs[n:n + 2], refs[n + 2:]
    held, in_sems, refs = refs[:n], refs[n], refs[n + 1:]
    main(m_hbm, given, held, in_sems, m_out, z_out, *refs)


def main(
    m_hbm, given, held, in_sems, m_out, z_out,
    z_t, ln_t, p_q, p_kt, p_v, p_sg, k_s, bsc_row, bsc_tri, rb, tb, bt_row, bt_tri, m_all, m_dev, c_dev, m_own, ln_m, cq, ckv, og,
    cmask, omask, kcols, mq, mkt, mv, pick, spread, join, acs, r_all, x_loc, o_scr, u_opm, z_snd, z_rcv, z_f, nrm, tmp, wro_t, wci_p, wco_t, woo_t, wtri_t,
    x_s, m_s, w_s, g_s, w_bias,
    g_send, g_recv, a_send, a_recv,
):
    me = lax.axis_index('dap')
    data = lax.axis_index('data')
    my_rows = rows_at(me, R)

    def peer(o):
        return (data, lax.rem(me + o, N_DAP))

    z_in, msk, rmsk, w_row_bias, w_ts_bias, w_te_bias = held[:6]
    w_row_in, w_row_out, w_col_in, w_col_out, w_opm_in, w_opm_out, w_ts_in, w_ts_out, w_te_in, w_te_out = held[6:]
    own_m = m_all.at[pl.ds(4 * me, 4)]
    copy_m = pltpu.make_async_copy(m_hbm, own_m, in_sems.at[N_IN - 1])
    copy_m.start()
    copies_in = [pltpu.make_async_copy(src, dst, in_sems.at[k]) for k, (src, dst) in enumerate(zip(given, held))]
    for c in copies_in:
        c.start()

    barrier = pltpu.get_barrier_semaphore()
    for o in range(1, N_DAP):
        pl.semaphore_signal(barrier, inc=1, device_id=peer(o), device_id_type=MESH)
    pl.semaphore_wait(barrier, N_DAP - 1)

    def gather(stage, ref):
        return [
            pltpu.make_async_remote_copy(
                src_ref=ref, dst_ref=ref, send_sem=g_send.at[stage, o - 1], recv_sem=g_recv.at[stage, o - 1],
                device_id=peer(o), device_id_type=MESH)
            for o in range(1, N_DAP)
        ]

    def start(copies):
        for c in copies:
            c.start()

    def wait(copies):
        for c in copies:
            c.wait()

    def z_copy(stage, o, first, count, at=0, size=R):
        dest = lax.rem(me + o, N_DAP)
        return pltpu.make_async_remote_copy(
            src_ref=z_snd.at[min(stage, 1), pl.ds(first, count), pl.ds(pl.multiple_of(dest * R + at, H), size), :],
            dst_ref=z_rcv.at[min(stage, 1), pl.ds(me * R + first, count), pl.ds(at, size), :],
            send_sem=a_send.at[stage, o - 1], recv_sem=a_recv.at[stage, o - 1],
            device_id=(data, dest), device_id_type=MESH)

    copy_m.wait()
    g_in = gather(0, own_m)
    start(g_in)
    for c in copies_in:
        c.wait()

    e_c = eye_bf16(C)
    e_l = eye_bf16(L)

    def every(first, count, stride):
        return tmp[pl.ds(first, count, stride=stride), :]

    for b in range(2):
        tmp[:H, :] = w_row_bias[b].astype(F32)
        tmp[H:H + 4, :] = w_ts_bias[b].astype(F32)
        tmp[H + 4:S, :] = w_te_bias[b].astype(F32)
        w_bias[b] = tmp[:S, :].astype(BF16)
        wro_t[b] = mm_nt(e_c, w_row_out[b]).astype(BF16)
        tmp[:4 * C, :C] = w_col_in[b].astype(F32)
        wci_p[b] = subl([every(f * C + d, H, H) for f in range(4) for d in range(H)])[:, :C].astype(BF16)
        tmp[:C, :C] = w_col_out[b].astype(F32)
        wco_t[b] = mm_nt(e_c, subl([every(d, H, H) for d in range(H)])[:, :C].astype(BF16)).astype(BF16)

    def late_weights():
        for b in range(2):
            wtri_t[0, b] = mm_nt(e_l, w_ts_out[b]).astype(BF16)
            wtri_t[1, b] = mm_nt(e_l, w_te_out[b]).astype(BF16)
        tmp[...] = w_opm_out[0].astype(F32)
        woo_t[0] = mm_nt(e_l, subl([every(q, R, R) for q in range(R)]).astype(BF16)).astype(BF16)
        woo_t[1] = mm_nt(e_l, w_opm_out[1]).astype(BF16)
        src, lane = iota((4 * L, 4 * L), 0), iota((4 * L, 4 * L), 1)
        join[...] = ones_at((src // L == lane % L // R) & (src % L == lane // L * R + lane % R))

    def down(row):
        return jnp.transpose(jnp.broadcast_to(row, (L, L)))

    mask_f = msk[...].astype(F32)
    for s in range(S):
        cmask[s] = jnp.broadcast_to(mask_f[s:s + 1, :], (H, L))
    mask_t = jnp.transpose(subl([mask_f] * H)).astype(BF16)[:, :S]
    nrm[...] = 1.0 / (1e-3 + mm(mask_t, mask_f.astype(BF16)))
    key_row = rmsk[...].astype(F32)
    key_col = down(key_row)
    key_row2 = lanes([key_row, key_row])
    turned = jnp.transpose(subl([mask_f] * H))
    for s in range(S):
        kcols[s] = jnp.broadcast_to(turned[:, s:s + 1], (L, L))

    def iota(shape, axis):
        return lax.broadcasted_iota(jnp.int32, shape, axis)

    def ones_at(where):
        return jnp.where(where, 1.0, 0.0).astype(BF16)

    src, lane = iota((4 * L, L), 0), iota((4 * L, L), 1)
    pick[...] = ones_at((src // L == lane // R) & (src % L == me * R + lane % R))
    src, lane = iota((L, 8 * L), 0), iota((L, 8 * L), 1)
    spread[...] = ones_at(src == lane // L2 * R + lane % R)
    src, lane = iota((L, L), 0), iota((L, L), 1)
    own_mask = mm(mask_f.astype(BF16), ones_at(src == me * R + lane % R))
    for s in range(S):
        omask[s] = jnp.broadcast_to(own_mask[s:s + 1, :], (H, L))

    def bias_rows(bsc, ln_ref, b, group):
        def stage(t):
            n = t * 2
            rows = part(mm(w_bias[b], pair(ln_ref, n)), group, H)
            bsc[rows_at(n, H), :] = lo(rows)
            bsc[rows_at(n + 1, H), :] = hi(rows)
        return stage

    def pack_bias(bsc, ref, first, heads):
        for h in range(heads):
            ref[h, my_rows, :] = bsc[pl.ds(first + h, R, stride=H), :].astype(BF16)

    def normalise(t):
        for n in (t * 2, t * 2 + 1):
            ln_t[n] = layer_norm_t(z_t[n])

    def make_tri_bias(ref, by_key):
        for h in range(4):
            t = ref[h].astype(F32) * LOG2E
            t = t if by_key else jnp.transpose(t)
            bt_tri[:, cols(h)] = jnp.where(key_col > 0, t, NEG)

    def project_stages(w_in_ref):
        def project(t):
            n = t * 2
            ln2 = pair(ln_t, n)
            put_pair(p_q, n, mm(part(w_in_ref, 0, L), ln2).astype(BF16))
            k_s[...] = round_bf16(mm(part(w_in_ref, 1, L), ln2)) * key_row2
            put_pair(p_v, n, mm(part(w_in_ref, 2, L), ln2).astype(BF16))
            put_pair(p_sg, n, round_bf16(mm(part(w_in_ref, 3, L), ln2)))

        def turn(t):
            for r in range(2):
                p_kt[t * 2 + r] = jnp.transpose(k_s[:, cols(r)]).astype(BF16)
                p_sg[t * 2 + r] = sigmoid(p_sg[t * 2 + r])

        return [project, turn]

    def weigh(t):
        for k in range(4):
            for half in (cols(0), cols(1)):
                e = jnp.exp2(x_s[k, :, half] - m_s[k, :, half])
                w_s[k, :, half] = (e * (1.0 / jnp.sum(e, axis=0, keepdims=True))).astype(BF16)

    def put_score(k, x):
        x_s[k] = x
        m_s[k] = jnp.max(x, axis=0, keepdims=True)

    def attend_stages(w_out_t, finish):
        scale = R ** -0.5 * LOG2E

        def score(t):
            for r in range(2):
                q = p_q[t * 2 + r]
                kt = p_kt[t * 2 + r]
                for hp in range(2):
                    blocks = [only(part(q, h, R), h, R, 4) for h in (2 * hp, 2 * hp + 1)]
                    put_score(2 * r + hp, mm(kt, lanes(blocks)) * scale + bt_tri[:, cols(hp, L2)])

        def gather_values(t):
            for r in range(2):
                v = p_v[t * 2 + r]
                outs = []
                for hp in range(2):
                    o2 = mm(part(v, hp, C), w_s[2 * r + hp])
                    outs += [lo(part(o2, 0, R)), hi(part(o2, 1, R))]
                g_s[:, cols(r)] = (subl(outs) * p_sg[t * 2 + r]).astype(BF16)

        def project_out(t):
            finish[0](t, pair(z_t, t * 2).astype(F32) + mm(w_out_t[...], g_s[...]))

        return [score, weigh, gather_values, project_out] + finish[1:]

    def row_attention(b, load, store):
        scale = H ** -0.5 * LOG2E
        for t in range(4):
            proj = round_bf16(mm(w_row_in[b], layer_norm_t(load(t))))
            q, k, v, g = [part(proj, f, C) for f in range(4)]
            p_sg[4 + t, :C] = q
            mkt[t] = jnp.transpose(subl([k, k]))[:, :C].astype(BF16)
            mv[t] = v.astype(BF16)
            p_sg[t, :C] = sigmoid(g)

        def score(t):
            kt = mkt[t]
            kcol = kcols[4 * me + t]
            kcol2 = lanes([kcol, kcol])
            for hp in range(4):
                blocks = [only(p_sg[4 + t, cols(h, H)], h, H, H) for h in (2 * hp, 2 * hp + 1)]
                x = mm(kt, lanes(blocks).astype(BF16)) * scale + bt_row[:, cols(hp, L2)]
                put_score(hp, jnp.where(kcol2 > 0, x, NEG))

        def gather_values(t):
            outs = []
            for hp in range(4):
                o2 = mm(mv[t, cols(hp, S)], w_s[hp])
                outs += [lo(part(o2, 0, H)), hi(part(o2, 1, H))]
            g_s[:C, :L] = (subl(outs) * p_sg[t, :C]).astype(BF16)

        def project_out(t):
            store(t, (load(t).astype(F32) + mm(wro_t[b], g_s[:C, :L])).astype(BF16))

        pipeline([score, weigh, gather_values, project_out], 4)

    same_head = iota((C, L2), 0) // H == iota((C, L2), 1) // R
    block = iota((C, L), 1) // R

    def row_attention_own():
        scale = H ** -0.5 * LOG2E
        rows = subl([bsc_row[pl.ds(h, R, stride=H), :] for h in range(H)])
        bias = jnp.transpose(round_bf16(rows)) * LOG2E
        bt_row[:, :L2] = bias
        w_qg = subl([part(w_row_in[0], 0, C), part(w_row_in[0], 3, C)])

        def keys(t):
            ln2 = lanes([layer_norm_t(m_all[2 * t]), layer_norm_t(m_all[2 * t + 1])])
            kv = round_bf16(mm(w_row_in[0, C:3 * C], ln2))
            for s, x in ((2 * t, lo(kv)), (2 * t + 1, hi(kv))):
                mkt[s] = jnp.transpose(x)[:, :C].astype(BF16)
                mv[s] = part(x, 1, C).astype(BF16)

        def queries(t):
            own = mm(lanes([m_all[4 * t + k] for k in range(4)]), pick[...])
            m_own[t] = own.astype(BF16)
            qg = round_bf16(mm(w_qg, layer_norm_t(own)))
            p_sg[t, :C] = sigmoid(part(qg, 1, C))
            q = mm(part(qg, 0, C).astype(BF16), spread[...])
            for k in range(4):
                mq[4 * t + k] = jnp.where(same_head, q[:, cols(k, L2)], 0.0).astype(BF16)

        def score(t):
            for k in range(4):
                s = 4 * t + k
                x = mm(mkt[s], mq[s]) * scale + bt_row[:, :L2]
                put_score(k, jnp.where(lanes([kcols[s], kcols[s]]) > 0, x, NEG))

        def gather_values(t):
            out = jnp.zeros((C, L), F32)
            for k in range(4):
                o2 = jnp.where(same_head, mm(mv[4 * t + k], w_s[k]), 0.0)
                o = lo(o2) + hi(o2)
                o = o + pltpu.roll(o, C, 1)
                o = o + pltpu.roll(o, R, 1)
                out = jnp.where(block == k, o, out)
            g_s[:C, :L] = (out * p_sg[t, :C]).astype(BF16)

        def project_out(t):
            m_own[t] = (m_own[t].astype(F32) + mm(wro_t[0], g_s[:C, :L])).astype(BF16)

        wait(g_in)
        for t in range(4):
            queries(t)
        for t in range(S // 2):
            keys(t)
        pipeline([score, weigh, gather_values, project_out], 4)

    def attend_columns(steps, mask):
        scale = H ** -0.5 * LOG2E

        def attend(a, carry):
            def at(s, f, d):
                return ckv[s, cols(f * H + d, H)]

            q = [cq[a, cols(d, H)] for d in range(H)]
            logits = []
            for t in range(S):
                acc = functools.reduce(jnp.add, [q[d] * at(t, 0, d) for d in range(H)])
                logits.append(jnp.where(mask[t] > 0, acc * scale, NEG))
            top = functools.reduce(jnp.maximum, logits)
            e = [jnp.exp2(x - top) for x in logits]
            inv = 1.0 / functools.reduce(jnp.add, e)
            probs = [round_bf16(x * inv) for x in e]
            outs = [functools.reduce(jnp.add, [probs[t] * at(t, 1, d) for t in range(S)]) for d in range(H)]
            og[a] = (subl(outs) * part(cq[a], 1, C)).astype(BF16)
            return carry
        lax.fori_loop(0, steps, attend, 0)

    def col_attention_own():
        ln4 = lanes([layer_norm_t(m_own[t]) for t in range(4)])
        proj = round_bf16(mm(wci_p[0], ln4))
        for t in range(4):
            x = proj[:, cols(t)]
            cq[t] = subl([part(x, 0, C), sigmoid(part(x, 3, C))])
            kv = x[C:3 * C].astype(BF16)
            for k in range(4):
                ckv[4 * t + k] = mm(kv, spread[:, cols(2 * k)])
        attend_columns(4, omask)
        new = mm(wco_t[0], lanes([og[t] for t in range(4)]))
        for t in range(4):
            m_dev[me, t] = (m_own[t].astype(F32) + new[:, cols(t)]).astype(BF16)
        both = mm(w_opm_in[0], lanes([layer_norm_t(m_dev[me, t]) for t in range(4)]))
        for t in range(4):
            mask = omask[4 * t, :1]
            for k in range(1, 4):
                mask = jnp.where(block[:1] == k, omask[4 * t + k, :1], mask)
            x = (both[:, cols(t)] * mask).astype(BF16)
            c_dev[me, t] = part(x, 1, R)
            for k in range(4):
                acs[pl.ds((4 * t + k) * C, R), :] = mm(part(x, 0, R), spread[:, cols(2 * k)])

    def col_attention():
        def normalise_m(t):
            for s in (2 * t, 2 * t + 1):
                ln_m[s] = layer_norm_t(m_all[s])

        def project(t):
            proj = round_bf16(mm(wci_p[1], pair(ln_m, 2 * t)))
            put_pair(cq, 2 * t, subl([part(proj, 0, C), sigmoid(part(proj, 3, C))]))
            put_pair(ckv, 2 * t, proj[C:3 * C])
        pipeline([normalise_m, project], S // 2)
        attend_columns(S, cmask)

        def update(t):
            new = pair(m_all, 2 * t).astype(F32) + mm(wco_t[1], pair(og, 2 * t))
            put_pair(m_all, 2 * t, new.astype(BF16))
        return update

    def opm_halves(b, first):
        def normalise_m(t):
            for s in (2 * t, 2 * t + 1):
                ln_m[s] = layer_norm_t(m_all[s])

        def halves(t):
            both = mm(w_opm_in[b], pair(ln_m, 2 * t))
            for s, x in ((2 * t, lo(both)), (2 * t + 1, hi(both))):
                acs[rows_at(s, C), :] = x * msk[pl.ds(s, 1), :].astype(F32)
        pipeline(first + [normalise_m, halves], S // 2)

    row_id = lax.broadcasted_iota(jnp.int32, (S, L2), 0)
    lane_id = lax.broadcasted_iota(jnp.int32, (S, L2), 1)
    diag = row_id == lane_id // S

    def opm(b, finish):
        local, other = (0, R) if b == 0 else (R, 0)
        for q in range(R):
            r_all[q] = acs[pl.ds(other + q, S, stride=C), :].astype(BF16)
        for t in range(4):
            rows = subl([acs[pl.ds(local + H * t + p, S, stride=C), :] for p in range(H)])
            x_loc[:, cols(t)] = jnp.transpose(round_bf16(rows))

        def outer(t):
            left = []
            for k in range(4):
                row = x_loc[pl.ds(b * me * R + t * 4 + k, 1), :]
                for half in (cols(0, L2), cols(1, L2)):
                    left.append(jnp.where(diag, jnp.broadcast_to(row[:, half], (S, L2)), 0.0))
            left = subl(left).astype(BF16)
            for q in range(0, R, 2):
                put_pair(o_scr, q, mm(left, lanes([subl([r_all[q]] * S), subl([r_all[q + 1]] * S)])).astype(BF16))

        def contract(t):
            for k in range(2):
                blocks = [o_scr[:, cols(2 * k + j, R), :].reshape(R * R, L) for j in range(2)]
                n = t * 4 + 2 * k
                at = me * R + n
                norm = lanes([nrm[pl.ds(at, 1), :], nrm[pl.ds(at + 1, 1), :]])
                finish[0](n, mm(woo_t[b], lanes(blocks)) * norm)

        pipeline([outer, contract] + [
            lambda t, f=f: (f(2 * t), f(2 * t + 1)) for f in finish[1:]], R // 4)

    def put_z(t, z2):
        put_pair(z_t, 2 * t, z2.astype(BF16))

    def send_z(stage, b, size):
        def turn(t, z2):
            put_z(t, z2)
            z2 = round_bf16(z2)
            for r, x in ((0, lo(z2)), (1, hi(z2))):
                z_snd[stage, 2 * t + r] = jnp.transpose(x).astype(BF16)

        def send(t):
            for o in range(1, N_DAP):
                z_copy(stage, o, 2 * t, 2, 0, size).start()
            for n in (2 * t, 2 * t + 1):
                z_rcv[stage, me * R + n] = z_snd[stage, n, my_rows, :]
        send.early = True
        return [turn, send, normalise, bias_rows(bsc_tri, ln_t, b, 1)]

    def widen_z(stage, at, size):
        def widen(t):
            for r in range(4):
                n = t * 4 + r
                z_f[pl.ds(pl.multiple_of(n * (R + H) + at, H), size), :] = z_rcv[stage, n, pl.ds(at, size), :].astype(F32)
        pipeline([widen], R)

    def wait_z(stage, at, size):
        for o in range(1, N_DAP):
            z_copy(stage, o, 0, R, at, size).wait()

    def turn_z(t):
        for n in (2 * t, 2 * t + 1):
            z_t[n] = jnp.transpose(z_f[pl.ds(n, L, stride=R + H), :]).astype(BF16)

    def enter(t):
        for n in (2 * t, 2 * t + 1):
            z_t[n] = jnp.transpose(z_in[n].astype(F32)).astype(BF16)
    pipeline([enter, normalise, bias_rows(bsc_row, ln_t, 0, 0)], R // 2)
    row_attention_own()
    col_attention_own()
    g = gather(7, c_dev.at[me])
    start(g)
    g_m = gather(1, m_dev.at[me])
    start(g_m)
    late_weights()
    wait(g)
    for t in range(4):
        whole = mm(lanes([c_dev[d, t] for d in range(4)]), join[...])
        for k in range(4):
            acs[pl.ds((4 * t + k) * C + R, R), :] = whole[:, cols(k)]

    def add_first(n, update2):
        put_pair(z_t, n, (pair(z_t, n).astype(F32) + update2).astype(BF16))
    opm(0, [add_first, normalise, bias_rows(bsc_tri, ln_t, 0, 1)])
    pack_bias(bsc_tri, tb.at[0], 0, 4)
    g = gather(2, tb.at[0, :, my_rows, :])
    start(g)
    pipeline(project_stages(w_ts_in.at[0]), R // 2)
    wait(g)
    make_tri_bias(tb.at[0], False)
    pipeline(attend_stages(wtri_t.at[0, 0], send_z(0, 0, R)), R // 2)
    pack_bias(bsc_tri, tb.at[1], 4, 4)
    g = gather(3, tb.at[1, :, my_rows, :])
    start(g)

    wait(g_m)
    for t in range(4):
        whole = mm(lanes([m_dev[d, t] for d in range(4)]), join[...]).astype(BF16)
        for k in range(4):
            m_all[4 * t + k] = whole[:, cols(k)]
    opm_halves(1, [col_attention()])

    def keep_update(n, update2):
        put_pair(u_opm, n, update2)
    opm(1, [keep_update])

    def add_second(t):
        put_z(t, pair(z_t, 2 * t).astype(F32) + pair(u_opm, 2 * t))

    wait(g)
    make_tri_bias(tb.at[1], True)
    wait_z(0, 0, R)
    widen_z(0, 0, R)
    pipeline(
        [turn_z, normalise] + project_stages(w_te_in.at[0])
        + attend_stages(wtri_t.at[1, 0], [
            put_z, normalise, bias_rows(bsc_row, ln_t, 1, 0), add_second, normalise, bias_rows(bsc_tri, ln_t, 1, 1)]),
        R // 2)

    pack_bias(bsc_row, rb, 0, H)

    pack_bias(bsc_tri, tb.at[2], 4, 4)
    g = gather(5, tb.at[2, :, my_rows, :])
    start(g)
    g_row = gather(4, rb.at[:, my_rows, :])
    start(g_row)
    pipeline(project_stages(w_te_in.at[1]), R // 2)
    wait(g)
    make_tri_bias(tb.at[2], False)
    pipeline(attend_stages(wtri_t.at[1, 1], send_z(1, 1, FIRST)), R // 2)
    pack_bias(bsc_tri, tb.at[3], 0, 4)
    g = gather(6, tb.at[3, :, my_rows, :])
    start(g)
    for o in range(1, N_DAP):
        z_copy(2, o, 0, R, FIRST, R - FIRST).start()

    wait(g_row)
    for h in range(H):
        bt_row[:, cols(h)] = rb[h].astype(F32) * LOG2E

    def emit_m(s, value):
        m_own[s] = value
    row_attention(1, lambda s: m_all[4 * me + s], emit_m)
    m_done = pltpu.make_async_copy(m_own, m_out, in_sems.at[0])
    m_done.start()

    def last_bias():
        wait(g)
        make_tri_bias(tb.at[3], True)

    def emit_z(t, z2):
        for n, x in ((2 * t, lo(z2)), (2 * t + 1, hi(z2))):
            z_snd[0, n] = jnp.transpose(x).astype(BF16)

    def put_out(n, count):
        return pltpu.make_async_copy(z_snd.at[0, pl.ds(n, count)], z_out.at[pl.ds(n, count)], in_sems.at[1])

    def leave(t):
        put_out(2 * t, 2).start()

    def last_rows():
        wait_z(2, FIRST, R - FIRST)
        widen_z(1, FIRST, R - FIRST)
    wait_z(1, 0, FIRST)
    widen_z(1, 0, FIRST)
    pipeline(
        [turn_z, normalise] + project_stages(w_ts_in.at[1]) + attend_stages(wtri_t.at[0, 1], [emit_z, leave]),
        R // 2, {4: last_bias, FIRST // 2: last_rows})
    m_done.wait()
    put_out(0, R).wait()


def hand_out(m_new, z_new, m_out, z_out, m_v, z_v, sems):
    moves = [(m_new, m_v, m_out)]
    for k in range(4):
        moves.append([ref.at[pl.ds(k * H, H)] for ref in (z_new, z_v, z_out)])
    into = [pltpu.make_async_copy(src, mid, sems.at[0, k]) for k, (src, mid, _) in enumerate(moves)]
    out = [pltpu.make_async_copy(mid, dst, sems.at[1, k]) for k, (_, mid, dst) in enumerate(moves)]
    for c in into:
        c.start()
    for c, d in zip(into, out):
        c.wait()
        d.start()
    for d in out:
        d.wait()


def solution(mesh):
    def local_step(msa_act, pair_act, msa_mask, res_mask, w_row_bias, w_row_in, w_row_out, w_col_in, w_col_out, w_opm_in, w_opm_out, w_ts_bias, w_ts_in, w_ts_out, w_te_bias, w_te_in, w_te_out):
        def rows_first(w):
            w = jnp.moveaxis(w, 1, -1)
            return w.reshape(2, -1, w.shape[-1])

        def flat_out(w):
            return w.reshape(2, -1, w.shape[-1])

        w_bias = [jnp.swapaxes(w, 1, 2) for w in (w_row_bias, w_ts_bias, w_te_bias)]
        hbm = pl.BlockSpec(memory_space=pltpu.HBM)

        def wide(*shape):
            return pltpu.VMEM(shape, F32)

        def half(*shape):
            return pltpu.VMEM(shape, BF16)

        scratch = dict(
            z_t=half(R, L, L), ln_t=half(R, L, L), p_q=half(R, L, L), p_kt=half(R, L, L), p_v=half(R, L, L),
            p_sg=wide(R, L, L), k_s=wide(L, L2), bsc_row=wide(R * H, L), bsc_tri=wide(R * H, L),
            rb=half(H, L, L), tb=half(4, 4, L, L), bt_row=wide(L, H * L), bt_tri=wide(L, 4 * L),
            m_all=half(S, C, L), m_dev=half(4, 4, C, L), c_dev=half(4, 4, R, L), m_own=half(4, C, L), ln_m=half(S, C, L),
            cq=wide(S, L, L), ckv=wide(S, L, L), og=half(S, C, L),
            cmask=wide(S, H, L), omask=wide(S, H, L), kcols=wide(S, L, L),
            mq=half(S, C, L2), mkt=half(S, L, C), mv=half(S, C, L),
            pick=half(4 * L, L), spread=half(L, 8 * L), join=half(4 * L, 4 * L),
            acs=wide(S * C, L), r_all=half(R, S, L), x_loc=wide(L, R * S),
            o_scr=half(R, L, L), u_opm=wide(R, L, L), z_snd=half(2, R, L, L), z_rcv=half(2, L, R, L),
            z_f=wide(L * (R + H), L), nrm=wide(L, L), tmp=wide(R * R, L),
            wro_t=half(2, C, C), wci_p=half(2, 4 * C, C), wco_t=half(2, C, C), woo_t=half(2, L, R * R),
            wtri_t=half(2, 2, L, L), x_s=wide(4, L, L2), m_s=wide(4, 1, L2), w_s=half(4, L, L2), g_s=half(L, L2), w_bias=half(2, S, L),
        )
        sems = [pltpu.SemaphoreType.DMA((n, N_DAP - 1)) for n in (8, 8, 3, 3)]
        operands = (
            jnp.swapaxes(msa_act, 1, 2), pair_act, msa_mask, res_mask.reshape(1, L), *w_bias,
            rows_first(w_row_in), flat_out(w_row_out), rows_first(w_col_in), flat_out(w_col_out),
            rows_first(w_opm_in), flat_out(w_opm_out),
            rows_first(w_ts_in), flat_out(w_ts_out), rows_first(w_te_in), flat_out(w_te_out),
        )
        held = [pltpu.VMEM(x.shape, x.dtype) for x in operands[1:]] + [pltpu.SemaphoreType.DMA((N_IN,))]
        m_new, z_new = pl.pallas_call(
            body,
            out_shape=(jax.ShapeDtypeStruct((4, C, L), BF16), jax.ShapeDtypeStruct((R, L, L), BF16)),
            in_specs=[hbm] * N_IN,
            out_specs=(hbm, hbm),
            scratch_shapes=held + list(scratch.values()) + sems,
            compiler_params=pltpu.CompilerParams(collective_id=0, has_side_effects=True, vmem_limit_bytes=60 * 2 ** 20),
        )(*operands)
        m_new, z_new = pl.pallas_call(
            hand_out, in_specs=[hbm] * 2, out_specs=[hbm] * 2,
            out_shape=[jax.ShapeDtypeStruct(x.shape, x.dtype) for x in (m_new, z_new)],
            scratch_shapes=[half(4, C, L), half(R, L, L), pltpu.SemaphoreType.DMA((2, 5))],
        )(m_new, z_new)
        return jnp.swapaxes(m_new, 1, 2), z_new

    in_specs = (P(('data', 'dap')), P(('data', 'dap')), P('data'), P('data')) + (P(),) * 13
    out_specs = (P(('data', 'dap')), P(('data', 'dap')))
    return jax.shard_map(local_step, mesh=mesh, in_specs=in_specs, out_specs=out_specs, check_vma=False)
```
